32 devices in a mesh: dp: 1 (over z), stage: 32 (over y, x, core).
Axes of the slice: x: 4, y: 4, z: 1, core: 2. Of those that a mesh axis runs over, the one named last changes fastest.
The devices are a block of a 4x4x8 slice.
Arguments:
- x_in: bfloat16 [64, 64, 256], P('dp')
- y_target: bfloat16 [64, 64, 256], P('dp')
- w_up: bfloat16 [32, 256, 1024], P('stage')
- w_down: bfloat16 [32, 1024, 256], P('stage')
- norm_gain: float32 [32, 256], P('stage')
Outputs:
- output 1: float32 [32, 256, 1024], P(('dp', 'stage'))
- output 2: float32 [32, 1024, 256], P(('dp', 'stage'))
- output 3: float32 [32, 256], P(('dp', 'stage'))
- output 4: float32 [1], P('dp')
All inputs are finite; a program needn't handle non-finite values.
Results may differ from the reference program's by a relative error of at most 0.00668016.
Values are sent between devices in bfloat16 or wider.
A program may use at most 768 MiB of HBM per device.

```python
import jax
import jax.numpy as jnp
from jax import lax

D_MODEL = 256
FFN_DIM = 1024
TOKENS = 64
MICROBATCHES = 64
NUM_LAYERS = 32
NORM_EPS = 1e-6


def setup_inputs(seed: int = 0, part: int = 0) -> dict:
    part_key = jax.random.fold_in(jax.random.key(seed), part)
    key_x, key_y = jax.random.split(part_key, 2)
    key_up, key_down, key_gain = jax.random.split(jax.random.key(seed + 1), 3)
    act_shape = (MICROBATCHES, TOKENS, D_MODEL)
    x_in = jax.random.normal(key_x, act_shape, jnp.float32)
    y_target = 2.0 * jax.random.normal(key_y, act_shape, jnp.float32)
    w_up = jax.random.normal(key_up, (NUM_LAYERS, D_MODEL, FFN_DIM), jnp.float32) * D_MODEL ** -0.5
    w_down = jax.random.normal(key_down, (NUM_LAYERS, FFN_DIM, D_MODEL), jnp.float32) * FFN_DIM ** -0.5
    norm_gain = 1.0 + 0.25 * jax.random.normal(key_gain, (NUM_LAYERS, D_MODEL), jnp.float32)
    return {'x_in': x_in.astype(jnp.bfloat16), 'y_target': y_target.astype(jnp.bfloat16), 'w_up': w_up.astype(jnp.bfloat16), 'w_down': w_down.astype(jnp.bfloat16), 'norm_gain': norm_gain}


def rms_norm(x_act, gain_row):
    x_float = x_act.astype(jnp.float32)
    inv_rms = lax.rsqrt(jnp.mean(x_float * x_float, axis=-1, keepdims=True) + NORM_EPS)
    return x_float * inv_rms * gain_row


def layer_apply(x_act, w_up_l, w_down_l, gain_l):
    normed = rms_norm(x_act, gain_l).astype(jnp.bfloat16).astype(jnp.float32)
    hidden = jnp.dot(normed, w_up_l, preferred_element_type=jnp.float32)
    gelu_out = jax.nn.gelu(hidden, approximate=True).astype(jnp.bfloat16).astype(jnp.float32)
    mlp_out = jnp.dot(gelu_out, w_down_l, preferred_element_type=jnp.float32)
    return (x_act.astype(jnp.float32) + mlp_out).astype(jnp.bfloat16)


layer_ckpt = jax.checkpoint(layer_apply)


def micro_loss(weights, x_micro, y_micro):
    def layer_step(act_rows, layer_params):
        return layer_ckpt(act_rows, layer_params[0], layer_params[1], layer_params[2]), None
    scan_out = lax.scan(layer_step, x_micro, weights)
    error_val = scan_out[0].astype(jnp.float32) - y_micro.astype(jnp.float32)
    return jnp.sum(error_val * error_val) / (MICROBATCHES * TOKENS * D_MODEL)


def reference(x_in, y_target, w_up, w_down, norm_gain):
    weights = (w_up.astype(jnp.float32), w_down.astype(jnp.float32), norm_gain)
    grad_fn = jax.value_and_grad(micro_loss)

    def micro_step(totals, micro_pair):
        loss_val, grad_vals = grad_fn(weights, micro_pair[0], micro_pair[1])
        new_totals = (totals[0] + loss_val, totals[1] + grad_vals[0], totals[2] + grad_vals[1], totals[3] + grad_vals[2])
        return new_totals, None

    start_totals = (jnp.zeros((), jnp.float32), jnp.zeros_like(weights[0]), jnp.zeros_like(weights[1]), jnp.zeros_like(norm_gain))
    scan_out = lax.scan(micro_step, start_totals, (x_in, y_target))
    totals = scan_out[0]
    return totals[1], totals[2], totals[3], totals[0].reshape(1)
```

```python
import functools

import jax
import jax.numpy as jnp
from jax import lax
from jax.experimental import pallas as pl
from jax.experimental.pallas import tpu as pltpu
from jax.sharding import PartitionSpec as P

NORM_EPS = 1e-6
SEG = 8
N_CHUNKS = 4
GELU_C = 0.7978845608028654
GELU_A = 0.044715
MESH = pl.DeviceIdType.MESH
F32 = jnp.float32
BF16 = jnp.bfloat16


def dot_nn(lhs, rhs):
    return lax.dot_general(lhs, rhs, (((1,), (0,)), ((), ())), preferred_element_type=F32)


def dot_nt(lhs, rhs):
    return lax.dot_general(lhs, rhs, (((1,), (1,)), ((), ())), preferred_element_type=F32)


def dot_tn(lhs, rhs):
    return lax.dot_general(lhs, rhs, (((0,), (0,)), ((), ())), preferred_element_type=F32)


def gelu_parts(hidden):
    sq = hidden * hidden
    tanh_val = jnp.tanh(hidden * (GELU_C + (GELU_C * GELU_A) * sq))
    half = 0.5 * hidden
    value = half + half * tanh_val
    slope = (0.5 + 0.5 * tanh_val) + (half * (1.0 - tanh_val * tanh_val)) * (GELU_C + (3.0 * GELU_C * GELU_A) * sq)
    return value, slope


def inv_rms_of(x_float):
    return lax.rsqrt(jnp.mean(x_float * x_float, axis=-1, keepdims=True) + NORM_EPS)


def fold_rows(block):
    rows, cols = block.shape
    return jnp.sum(block.reshape(rows // 8, 8, cols), axis=0)


def step_kernel(n_stages, loss_scale,
                x_hbm, y_hbm, wu_hbm, wd_hbm, gain_ref,
                dwu_ref, dwd_ref, dgain_ref, loss_ref,
                wu, wd, gains, acts, grads, slopes, act_stash, grad_stash, targets, dwd_t,
                dg_part, dg_stash, loss_part, loss_stash, loss_total,
                load_sem, x_sem, y_sem, agu_send, agu_recv, agd_send, agd_recv, gain_send, gain_recv,
                as_send, as_recv, gs_send, gs_recv, fwd_send, fwd_recv, bwd_send, bwd_recv,
                dg_send, dg_recv, lrow_send, lrow_recv, lcol_send, lcol_recv):
    n_rows = n_stages // SEG
    n_chips = SEG // 2
    chunk = acts.shape[2]
    d_model = acts.shape[3]
    d_ff = wu.shape[2]
    me = lax.axis_index('stage')
    row = lax.div(me, SEG)
    r = lax.rem(me, SEG)
    chip = lax.div(r, 2)
    core = lax.rem(r, 2)
    row_base = row * SEG
    left = lax.rem(chip + n_chips - 1, n_chips) * 2 + core
    right = lax.rem(chip + 1, n_chips) * 2 + core
    across = lax.rem(chip + 2, n_chips) * 2 + core
    flip = 1 - 2 * core
    sib = r + flip

    def rcopy(src, dst, send_sem, recv_sem, dev):
        return pltpu.make_async_remote_copy(src_ref=src, dst_ref=dst, send_sem=send_sem, recv_sem=recv_sem,
                                            device_id={'stage': dev}, device_id_type=MESH)

    load_u = pltpu.make_async_copy(wu_hbm.at[0], wu.at[r], load_sem.at[0])
    load_d = pltpu.make_async_copy(wd_hbm.at[0], wd.at[r], load_sem.at[1])
    load_u.start()
    load_d.start()

    def x_load(k):
        first = pl.multiple_of((r * N_CHUNKS + k) * chunk, chunk)
        return pltpu.make_async_copy(x_hbm.at[pl.ds(first, chunk)], acts.at[0, k], x_sem.at[k])

    def y_load(k):
        first = pl.multiple_of((r * N_CHUNKS + k) * chunk, chunk)
        return pltpu.make_async_copy(y_hbm.at[pl.ds(first, chunk)], targets.at[k], y_sem.at[k])

    @pl.when(row == 0)
    def _():
        for k in range(N_CHUNKS):
            x_load(k).start()

    @pl.when(row == n_rows - 1)
    def _():
        for k in range(N_CHUNKS):
            y_load(k).start()

    gains[r] = jnp.broadcast_to(gain_ref[...], (8, d_model))
    dg_part[...] = jnp.zeros_like(dg_part)
    loss_part[...] = jnp.zeros_like(loss_part)

    barrier = pltpu.get_barrier_semaphore()
    for step in range(1, SEG):
        pl.semaphore_signal(barrier, inc=1, device_id={'stage': row_base + lax.rem(r + step, SEG)}, device_id_type=MESH)
    for step in range(1, n_rows):
        pl.semaphore_signal(barrier, inc=1, device_id={'stage': lax.rem(row + step, n_rows) * SEG + r}, device_id_type=MESH)
    pl.semaphore_wait(barrier, SEG - 1 + n_rows - 1)

    def u_copy(slot, dev):
        return rcopy(wu.at[slot], wu.at[slot], agu_send, agu_recv.at[slot], row_base + dev)

    def d_copy(slot, dev):
        return rcopy(wd.at[slot], wd.at[slot], agd_send, agd_recv.at[slot], row_base + dev)

    load_u.wait()
    load_d.wait()
    u_copy(r, right).start()
    d_copy(r, left).start()
    d_copy(r, right).start()
    u_copy(r, left).start()
    u_copy(r, sib).start()
    d_copy(r, sib).start()
    for step in range(1, SEG):
        rcopy(gains.at[r], gains.at[r], gain_send, gain_recv, row_base + lax.rem(r + step, SEG)).start()

    u_copy(left, r).wait_recv()
    u_copy(left, right).start()
    u_copy(left, sib).start()
    d_copy(right, r).wait_recv()
    d_copy(right, left).start()
    d_copy(right, sib).start()
    d_copy(left, r).wait_recv()
    d_copy(left, sib).start()
    u_copy(right, r).wait_recv()
    u_copy(right, sib).start()
    u_copy(across, r).wait_recv()
    u_copy(across, sib).start()
    d_copy(across, r).wait_recv()
    d_copy(across, sib).start()
    for slot in (sib, left + flip, right + flip, across + flip):
        u_copy(slot, r).wait_recv()
        d_copy(slot, r).wait_recv()
    rcopy(gains.at[pl.ds(0, SEG - 1)], gains.at[pl.ds(0, SEG - 1)], gain_send, gain_recv, me).wait_recv()

    def act_ship(layer, k):
        return rcopy(acts.at[layer, k], act_stash.at[r, k], as_send, as_recv, row_base + layer)

    def grad_ship(layer, k):
        return rcopy(grads.at[layer + 1, k], grad_stash.at[r, k], gs_send, gs_recv, row_base + layer)

    def fwd_layer(layer, k):
        x_float = acts[layer, k].astype(F32)
        normed = (x_float * inv_rms_of(x_float) * gains[layer, 0:1, :]).astype(BF16)
        hidden = dot_nn(normed, wu[layer])
        value, slope = gelu_parts(hidden)
        slopes[layer, k] = slope
        out = x_float + dot_nn(value.astype(BF16), wd[layer])
        acts[layer + 1, k] = out.astype(BF16)

        @pl.when(layer != r)
        def _():
            act_ship(layer, k).start()
        return k

    def fwd_chunk(k, carry):
        @pl.when(row == 0)
        def _():
            x_load(k).wait()

        @pl.when(row > 0)
        def _():
            rcopy(acts.at[0, k], acts.at[0, k], fwd_send, fwd_recv.at[k], me).wait_recv()

        lax.fori_loop(0, SEG, fwd_layer, k)

        @pl.when(row < n_rows - 1)
        def _():
            rcopy(acts.at[SEG, k], acts.at[0, k], fwd_send, fwd_recv.at[k], me + SEG).start()

        @pl.when(row == n_rows - 1)
        def _():
            y_load(k).wait()
            error_val = acts[SEG, k].astype(F32) - targets[k].astype(F32)
            loss_part[...] += fold_rows(error_val * error_val)
            grads[SEG, k] = ((2.0 * loss_scale) * error_val).astype(BF16)
        return carry

    lax.fori_loop(0, N_CHUNKS, fwd_chunk, 0)

    @pl.when(row == n_rows - 1)
    def _():
        loss_stash[r] = loss_part[...]
        for step in range(1, SEG):
            rcopy(loss_stash.at[r], loss_stash.at[r], lrow_send, lrow_recv, row_base + lax.rem(r + step, SEG)).start()

    def bwd_layer(step, k):
        layer = SEG - 1 - step
        grad_out = grads[layer + 1, k]

        @pl.when(layer != r)
        def _():
            grad_ship(layer, k).start()

        x_float = acts[layer, k].astype(F32)
        inv_rms = inv_rms_of(x_float)
        x_hat = x_float * inv_rms
        gain = gains[layer, 0:1, :]
        grad_gelu = dot_nt(grad_out, wd[layer]).astype(BF16).astype(F32)
        grad_hidden = (grad_gelu * slopes[layer, k]).astype(BF16)
        grad_normed = dot_nt(grad_hidden, wu[layer]).astype(BF16).astype(F32)
        dg_part[layer] += fold_rows(grad_normed * x_hat)
        grad_hat = grad_normed * gain
        mean_dot = jnp.mean(grad_hat * x_hat, axis=-1, keepdims=True)
        grad_x = inv_rms * (grad_hat - x_hat * mean_dot)
        grads[layer, k] = (grad_out.astype(F32) + grad_x).astype(BF16)
        return k

    def bwd_chunk(k, carry):
        @pl.when(row < n_rows - 1)
        def _():
            rcopy(grads.at[SEG, k], grads.at[SEG, k], bwd_send, bwd_recv.at[k], me).wait_recv()

        lax.fori_loop(0, SEG, bwd_layer, k)

        @pl.when(row > 0)
        def _():
            rcopy(grads.at[0, k], grads.at[SEG, k], bwd_send, bwd_recv.at[k], me - SEG).start()
        return carry

    lax.fori_loop(0, N_CHUNKS, bwd_chunk, 0)

    def dg_ship(layer):
        return rcopy(dg_part.at[layer], dg_stash.at[r], dg_send, dg_recv, row_base + layer)

    for step in range(1, SEG):
        dg_ship(lax.rem(r + step, SEG)).start()
    dg_stash[r] = dg_part[r]

    @pl.when(row == n_rows - 1)
    def _():
        rest = loss_stash.at[pl.ds(0, SEG - 1)]
        rcopy(rest, rest, lrow_send, lrow_recv, me).wait_recv()
        loss_total[...] = jnp.sum(loss_stash[...], axis=0)
        for step in range(1, n_rows):
            rcopy(loss_total, loss_total, lcol_send, lcol_recv, me - step * SEG).start()

    act_stash[r] = acts[r]
    grad_stash[r] = grads[r + 1]
    rest = act_stash.at[pl.ds(0, SEG - 1)]
    rcopy(rest, rest, as_send, as_recv, me).wait_recv()
    rcopy(rest, rest, gs_send, gs_recv, me).wait_recv()
    dwu_ref[...] = jnp.zeros_like(dwu_ref)
    dwd_t[...] = jnp.zeros_like(dwd_t)

    def weight_block(src, carry):
        rows = N_CHUNKS * chunk
        x_float = act_stash[src].reshape(rows, d_model).astype(F32)
        grad_out = grad_stash[src].reshape(rows, d_model)
        normed = (x_float * inv_rms_of(x_float) * gains[r, 0:1, :]).astype(BF16)
        value, slope = gelu_parts(dot_nn(normed, wu[r]))
        grad_gelu = dot_nt(grad_out, wd[r]).astype(BF16).astype(F32)
        grad_hidden = (grad_gelu * slope).astype(BF16)
        dwu_ref[0] += dot_tn(normed, grad_hidden)
        dwd_t[...] += dot_tn(grad_out, value.astype(BF16))
        return carry

    lax.fori_loop(0, SEG, weight_block, 0)
    dwd_ref[0] = dwd_t[...].T

    rest_dg = dg_stash.at[pl.ds(0, SEG - 1)]
    rcopy(rest_dg, rest_dg, dg_send, dg_recv, me).wait_recv()
    dgain_ref[...] = jnp.sum(jnp.sum(dg_stash[...], axis=0), axis=0, keepdims=True)

    @pl.when(row < n_rows - 1)
    def _():
        rcopy(loss_total, loss_total, lcol_send, lcol_recv, me).wait_recv()
    loss_ref[0] = jnp.sum(loss_total[...]) * loss_scale

    rest_u = wu.at[pl.ds(0, SEG - 1)]
    rest_d = wd.at[pl.ds(0, SEG - 1)]
    rcopy(rest_u, rest_u, agu_send, gain_recv, me).wait_send()
    rcopy(rest_d, rest_d, agd_send, gain_recv, me).wait_send()
    rest_gain = gains.at[pl.ds(0, SEG - 1)]
    rcopy(rest_gain, rest_gain, gain_send, gain_recv, me).wait_send()
    rcopy(rest, rest, as_send, as_recv, me).wait_send()
    rcopy(rest, rest, gs_send, gs_recv, me).wait_send()
    rcopy(rest_dg, rest_dg, dg_send, dg_recv, me).wait_send()

    @pl.when(row < n_rows - 1)
    def _():
        rcopy(acts.at[0], acts.at[0], fwd_send, dg_recv, me).wait_send()

    @pl.when(row > 0)
    def _():
        rcopy(grads.at[0], grads.at[0], bwd_send, dg_recv, me).wait_send()

    @pl.when(row == n_rows - 1)
    def _():
        rest_row = loss_stash.at[pl.ds(0, SEG - 1)]
        rcopy(rest_row, rest_row, lrow_send, lrow_recv, me).wait_send()
        for step in range(1, n_rows):
            rcopy(loss_total, loss_total, lcol_send, lcol_recv, me).wait_send()


def solution(mesh):
    n_stages = mesh.shape['stage']

    def stage_body(x_in, y_target, w_up, w_down, norm_gain):
        n_micro, n_tok, d_model = x_in.shape
        d_ff = w_up.shape[2]
        n_rows = n_micro * n_tok
        chunk = n_rows // SEG // N_CHUNKS
        loss_scale = 1.0 / (n_rows * d_model)
        sem = pltpu.SemaphoreType.DMA
        act_shape = (N_CHUNKS, chunk, d_model)
        scratch = [
            pltpu.VMEM((SEG, d_model, d_ff), BF16),
            pltpu.VMEM((SEG, d_ff, d_model), BF16),
            pltpu.VMEM((SEG, 8, d_model), F32),
            pltpu.VMEM((SEG + 1,) + act_shape, BF16),
            pltpu.VMEM((SEG + 1,) + act_shape, BF16),
            pltpu.VMEM((SEG, N_CHUNKS, chunk, d_ff), F32),
            pltpu.VMEM((SEG,) + act_shape, BF16),
            pltpu.VMEM((SEG,) + act_shape, BF16),
            pltpu.VMEM(act_shape, BF16),
            pltpu.VMEM((d_model, d_ff), F32),
            pltpu.VMEM((SEG, 8, d_model), F32),
            pltpu.VMEM((SEG, 8, d_model), F32),
            pltpu.VMEM((8, d_model), F32),
            pltpu.VMEM((SEG, 8, d_model), F32),
            pltpu.VMEM((8, d_model), F32),
            sem((2,)), sem((N_CHUNKS,)), sem((N_CHUNKS,)),
            sem, sem((SEG,)), sem, sem((SEG,)), sem, sem,
            sem, sem, sem, sem, sem, sem((N_CHUNKS,)), sem, sem((N_CHUNKS,)),
            sem, sem, sem, sem, sem, sem,
        ]
        any_spec = pl.BlockSpec(memory_space=pl.ANY)
        vmem_spec = pl.BlockSpec(memory_space=pltpu.VMEM)
        dw_up, dw_down, dgain, loss = pl.pallas_call(
            functools.partial(step_kernel, n_stages, loss_scale),
            out_shape=(jax.ShapeDtypeStruct(w_up.shape, F32), jax.ShapeDtypeStruct(w_down.shape, F32),
                       jax.ShapeDtypeStruct(norm_gain.shape, F32), jax.ShapeDtypeStruct((1,), F32)),
            in_specs=[any_spec, any_spec, any_spec, any_spec, vmem_spec],
            out_specs=(vmem_spec, vmem_spec, vmem_spec, pl.BlockSpec(memory_space=pltpu.SMEM)),
            scratch_shapes=scratch,
            compiler_params=pltpu.CompilerParams(collective_id=0, has_side_effects=True,
                                                 vmem_limit_bytes=60 * 1024 * 1024),
        )(x_in.reshape(n_rows, d_model), y_target.reshape(n_rows, d_model), w_up, w_down, norm_gain)
        return dw_up, dw_down, dgain, loss

    return jax.shard_map(stage_body, mesh=mesh,
                         in_specs=(P('dp'), P('dp'), P('stage'), P('stage'), P('stage')),
                         out_specs=(P(('dp', 'stage')), P(('dp', 'stage')), P(('dp', 'stage')), P('dp')),
                         check_vma=False)
```

```python
import functools

import jax
import jax.numpy as jnp
from jax import lax
from jax.experimental import pallas as pl
from jax.experimental.pallas import tpu as pltpu
from jax.sharding import PartitionSpec as P

NORM_EPS = 1e-6
SEG = 8
N_CHUNKS = 4
COLS = 256
HALF = SEG // 2
GELU_C = 0.7978845608028654
GELU_A = 0.044715
MESH = pl.DeviceIdType.MESH
F32 = jnp.float32
BF16 = jnp.bfloat16


def dot_nn(lhs, rhs):
    return lax.dot_general(lhs, rhs, (((1,), (0,)), ((), ())), preferred_element_type=F32)


def dot_nt(lhs, rhs):
    return lax.dot_general(lhs, rhs, (((1,), (1,)), ((), ())), preferred_element_type=F32)


def dot_tn(lhs, rhs):
    return lax.dot_general(lhs, rhs, (((0,), (0,)), ((), ())), preferred_element_type=F32)


def gelu_gate(hidden):
    sq = hidden * hidden
    gate = 0.5 + 0.5 * jnp.tanh(hidden * (GELU_C + (GELU_C * GELU_A) * sq))
    return gate, sq


def gelu_value(hidden):
    return hidden * gelu_gate(hidden)[0]


def gelu_slope(hidden, gate, sq):
    return gate + ((gate * (1.0 - gate)) * hidden) * (2.0 * GELU_C + (6.0 * GELU_C * GELU_A) * sq)


def inv_rms_of(x_float):
    return lax.rsqrt(jnp.mean(x_float * x_float, axis=-1, keepdims=True) + NORM_EPS)


def fold_rows(block):
    rows, cols = block.shape
    return jnp.sum(block.reshape(rows // 8, 8, cols), axis=0)


def step_kernel(n_stages, loss_scale,
                x_hbm, y_hbm, wu_hbm, wd_hbm, gain_ref,
                dwu_ref, dwd_ref, dgain_ref, loss_ref,
                wu, wd, gains, acts, grads, hiddens, act_stash, grad_stash, value_stash, slope_stash, targets, dwd_t,
                dg_part, dg_stash, loss_part, loss_stash, loss_total,
                load_sem, x_sem, y_sem, agu_send, agu_recv, agd_send, agd_recv, gain_send, gain_recv,
                as_send, as_recv, gs_send, gs_recv, fwd_send, fwd_recv, bwd_send, bwd_recv,
                dg_send, dg_recv, lrow_send, lrow_recv, lcol_send, lcol_recv):
    n_rows = n_stages // SEG
    n_chips = SEG // 2
    chunk = acts.shape[2]
    d_model = acts.shape[3]
    d_ff = wu.shape[2]
    me = lax.axis_index('stage')
    row = lax.div(me, SEG)
    r = lax.rem(me, SEG)
    chip = lax.div(r, 2)
    core = lax.rem(r, 2)
    row_base = row * SEG
    left = lax.rem(chip + n_chips - 1, n_chips) * 2 + core
    right = lax.rem(chip + 1, n_chips) * 2 + core
    across = lax.rem(chip + 2, n_chips) * 2 + core
    flip = 1 - 2 * core
    sib = r + flip

    def rcopy(src, dst, send_sem, recv_sem, dev):
        return pltpu.make_async_remote_copy(src_ref=src, dst_ref=dst, send_sem=send_sem, recv_sem=recv_sem,
                                            device_id={'stage': dev}, device_id_type=MESH)

    load_u = pltpu.make_async_copy(wu_hbm.at[0], wu.at[r], load_sem.at[0])
    load_d = pltpu.make_async_copy(wd_hbm.at[0], wd.at[r], load_sem.at[1])
    load_u.start()
    load_d.start()

    def x_load(k):
        first = pl.multiple_of((r * N_CHUNKS + k) * chunk, chunk)
        return pltpu.make_async_copy(x_hbm.at[pl.ds(first, chunk)], acts.at[0, k], x_sem.at[k])

    def y_load(k):
        first = pl.multiple_of((r * N_CHUNKS + k) * chunk, chunk)
        return pltpu.make_async_copy(y_hbm.at[pl.ds(first, chunk)], targets.at[k], y_sem.at[k])

    @pl.when(row == 0)
    def _():
        for k in range(N_CHUNKS):
            x_load(k).start()

    @pl.when(row == n_rows - 1)
    def _():
        for k in range(N_CHUNKS):
            y_load(k).start()

    gains[r] = jnp.broadcast_to(gain_ref[...], (8, d_model))
    dg_part[...] = jnp.zeros_like(dg_part)
    loss_part[...] = jnp.zeros_like(loss_part)

    with jax.named_scope('barrier'):
        barrier = pltpu.get_barrier_semaphore()
        for step in range(1, SEG):
            pl.semaphore_signal(barrier, inc=1, device_id={'stage': row_base + lax.rem(r + step, SEG)}, device_id_type=MESH)
        for step in range(1, n_rows):
            pl.semaphore_signal(barrier, inc=1, device_id={'stage': lax.rem(row + step, n_rows) * SEG + r}, device_id_type=MESH)
        pl.semaphore_wait(barrier, SEG - 1 + n_rows - 1)

    def u_copy(slot, dev):
        return rcopy(wu.at[slot], wu.at[slot], agu_send, agu_recv.at[slot], row_base + dev)

    def d_copy(slot, dev):
        return rcopy(wd.at[slot], wd.at[slot], agd_send, agd_recv.at[slot], row_base + dev)

    with jax.named_scope('w_load_u'):
        load_u.wait()
    with jax.named_scope('w_load_d'):
        load_d.wait()
    u_copy(r, right).start()
    d_copy(r, left).start()
    d_copy(r, right).start()
    u_copy(r, left).start()
    u_copy(r, sib).start()
    d_copy(r, sib).start()
    for step in range(1, SEG):
        rcopy(gains.at[r], gains.at[r], gain_send, gain_recv, row_base + lax.rem(r + step, SEG)).start()

    with jax.named_scope('ag_u_left'):
        u_copy(left, r).wait_recv()
    u_copy(left, right).start()
    u_copy(left, sib).start()
    with jax.named_scope('ag_d_right'):
        d_copy(right, r).wait_recv()
    d_copy(right, left).start()
    d_copy(right, sib).start()
    with jax.named_scope('ag_d_left'):
        d_copy(left, r).wait_recv()
    d_copy(left, sib).start()
    with jax.named_scope('ag_u_right'):
        u_copy(right, r).wait_recv()
    u_copy(right, sib).start()
    with jax.named_scope('ag_u_across'):
        u_copy(across, r).wait_recv()
    u_copy(across, sib).start()
    with jax.named_scope('ag_d_across'):
        d_copy(across, r).wait_recv()
    d_copy(across, sib).start()
    with jax.named_scope('ag_sib'):
        for slot in (sib, left + flip, right + flip, across + flip):
            u_copy(slot, r).wait_recv()
            d_copy(slot, r).wait_recv()
    rcopy(gains.at[pl.ds(0, SEG - 1)], gains.at[pl.ds(0, SEG - 1)], gain_send, gain_recv, me).wait_recv()

    def act_ship(layer, k):
        return rcopy(acts.at[layer, k], act_stash.at[k, r], as_send, as_recv, row_base + layer)

    def grad_ship(layer, k):
        return rcopy(grads.at[layer + 1, k], grad_stash.at[k, r], gs_send, gs_recv.at[k], row_base + layer)

    def fwd_layer(layer, k):
        x_float = acts[layer, k].astype(F32)
        normed = (x_float * inv_rms_of(x_float) * gains[layer, 0:1, :]).astype(BF16)
        out = x_float
        for part in range(0, d_ff, COLS):
            cols = slice(part, part + COLS)
            hidden = dot_nn(normed, wu[layer, :, cols])
            hiddens[layer, k, :, cols] = hidden
            out += dot_nn(gelu_value(hidden).astype(BF16), wd[layer, cols, :])
        acts[layer + 1, k] = out.astype(BF16)

        @pl.when(layer != r)
        def _():
            act_ship(layer, k).start()
        return k

    def fwd_chunk(k, carry):
        @pl.when(row == 0)
        def _():
            x_load(k).wait()

        @pl.when(row > 0)
        def _():
            with jax.named_scope('fwd_wait'):
                rcopy(acts.at[0, k], acts.at[0, k], fwd_send, fwd_recv.at[k], me).wait_recv()

        with jax.named_scope('fwd_layers'):
            lax.fori_loop(0, SEG, fwd_layer, k)

        @pl.when(row < n_rows - 1)
        def _():
            rcopy(acts.at[SEG, k], acts.at[0, k], fwd_send, fwd_recv.at[k], me + SEG).start()

        @pl.when(row == n_rows - 1)
        def _():
            y_load(k).wait()
            error_val = acts[SEG, k].astype(F32) - targets[k].astype(F32)
            loss_part[...] += fold_rows(error_val * error_val)
            grads[SEG, k] = ((2.0 * loss_scale) * error_val).astype(BF16)
        return carry

    lax.fori_loop(0, N_CHUNKS, fwd_chunk, 0)

    @pl.when(row == n_rows - 1)
    def _():
        loss_stash[r] = loss_part[...]
        for step in range(1, SEG):
            rcopy(loss_stash.at[r], loss_stash.at[r], lrow_send, lrow_recv, row_base + lax.rem(r + step, SEG)).start()

    rest = act_stash.at[0, pl.ds(0, SEG - 1)]
    all_rest = acts.at[pl.ds(0, SEG - 1)]

    def owner_block(index):
        return lax.div(index, 2), pl.ds(lax.rem(index, 2) * HALF, HALF)

    def value_block(index, carry):
        k, srcs = owner_block(index)
        x_float = act_stash[k, srcs].reshape(HALF * chunk, d_model).astype(F32)
        normed = (x_float * inv_rms_of(x_float) * gains[r, 0:1, :]).astype(BF16)
        act_stash[k, srcs] = normed.reshape(HALF, chunk, d_model)
        for part in range(0, d_ff, COLS):
            cols = slice(part, part + COLS)
            hidden = dot_nn(normed, wu[r, :, cols])
            gate, sq = gelu_gate(hidden)
            value_stash[k, srcs, :, cols] = (hidden * gate).astype(BF16).reshape(HALF, chunk, COLS)
            slope_stash[k, srcs, :, cols] = gelu_slope(hidden, gate, sq).reshape(HALF, chunk, COLS)
        return carry

    def value_phase():
        with jax.named_scope('as_wait'):
            rcopy(all_rest, all_rest, as_send, as_recv, me).wait_recv()
        for k in range(N_CHUNKS):
            act_stash[k, r] = acts[r, k]
        dwu_ref[...] = jnp.zeros_like(dwu_ref)
        dwd_t[...] = jnp.zeros_like(dwd_t)
        with jax.named_scope('value_blocks'):
            lax.fori_loop(0, 2 * N_CHUNKS, value_block, 0)

    @pl.when(row < n_rows - 1)
    def _():
        value_phase()

    def bwd_layer(step, k):
        layer = SEG - 1 - step
        grad_out = grads[layer + 1, k]

        @pl.when(layer != r)
        def _():
            grad_ship(layer, k).start()

        x_float = acts[layer, k].astype(F32)
        inv_rms = inv_rms_of(x_float)
        x_hat = x_float * inv_rms
        gain = gains[layer, 0:1, :]
        grad_normed = 0.0
        for part in range(0, d_ff, COLS):
            cols = slice(part, part + COLS)
            hidden = hiddens[layer, k, :, cols]
            slope = gelu_slope(hidden, *gelu_gate(hidden))
            grad_gelu = dot_nt(grad_out, wd[layer, cols, :]).astype(BF16).astype(F32)
            grad_hidden = (grad_gelu * slope).astype(BF16)
            grad_normed += dot_nt(grad_hidden, wu[layer, :, cols])
        grad_normed = grad_normed.astype(BF16).astype(F32)
        dg_part[layer] += fold_rows(grad_normed * x_hat)
        grad_hat = grad_normed * gain
        mean_dot = jnp.mean(grad_hat * x_hat, axis=-1, keepdims=True)
        grad_x = inv_rms * (grad_hat - x_hat * mean_dot)
        grads[layer, k] = (grad_out.astype(F32) + grad_x).astype(BF16)
        return k

    def bwd_chunk(k, carry):
        @pl.when(row < n_rows - 1)
        def _():
            with jax.named_scope('bwd_wait'):
                rcopy(grads.at[SEG, k], grads.at[SEG, k], bwd_send, bwd_recv.at[k], me).wait_recv()

        with jax.named_scope('bwd_layers'):
            lax.fori_loop(0, SEG, bwd_layer, k)

        @pl.when(row > 0)
        def _():
            rcopy(grads.at[0, k], grads.at[SEG, k], bwd_send, bwd_recv.at[k], me - SEG).start()
        return carry

    lax.fori_loop(0, N_CHUNKS, bwd_chunk, 0)

    def dg_ship(layer):
        return rcopy(dg_part.at[layer], dg_stash.at[r], dg_send, dg_recv, row_base + layer)

    for step in range(1, SEG):
        dg_ship(lax.rem(r + step, SEG)).start()
    dg_stash[r] = dg_part[r]

    @pl.when(row == n_rows - 1)
    def _():
        rest = loss_stash.at[pl.ds(0, SEG - 1)]
        rcopy(rest, rest, lrow_send, lrow_recv, me).wait_recv()
        loss_total[...] = jnp.sum(loss_stash[...], axis=0)
        for step in range(1, n_rows):
            rcopy(loss_total, loss_total, lcol_send, lcol_recv, me - step * SEG).start()

    @pl.when(row == n_rows - 1)
    def _():
        value_phase()

    for k in range(N_CHUNKS):
        grad_stash[k, r] = grads[r + 1, k]

    def weight_block(index, carry):
        k, srcs = owner_block(index)
        rows = HALF * chunk

        @pl.when(lax.rem(index, 2) == 0)
        def _():
            with jax.named_scope('gs_wait'):
                rcopy(rest, rest, gs_send, gs_recv.at[k], me).wait_recv()
        normed = act_stash[k, srcs].reshape(rows, d_model)
        grad_out = grad_stash[k, srcs].reshape(rows, d_model)
        for part in range(0, d_ff, COLS):
            cols = slice(part, part + COLS)
            grad_gelu = dot_nt(grad_out, wd[r, cols, :]).astype(BF16).astype(F32)
            grad_hidden = (grad_gelu * slope_stash[k, srcs, :, cols].reshape(rows, COLS)).astype(BF16)
            dwu_ref[0, :, cols] += dot_tn(normed, grad_hidden)
            dwd_t[:, cols] += dot_tn(grad_out, value_stash[k, srcs, :, cols].reshape(rows, COLS))
        return carry

    with jax.named_scope('weight_blocks'):
        lax.fori_loop(0, 2 * N_CHUNKS, weight_block, 0)
    with jax.named_scope('turn'):
        dwd_ref[0] = dwd_t[...].T

    rest_dg = dg_stash.at[pl.ds(0, SEG - 1)]
    with jax.named_scope('dg_wait'):
        rcopy(rest_dg, rest_dg, dg_send, dg_recv, me).wait_recv()
    dgain_ref[...] = jnp.sum(jnp.sum(dg_stash[...], axis=0), axis=0, keepdims=True)

    @pl.when(row < n_rows - 1)
    def _():
        rcopy(loss_total, loss_total, lcol_send, lcol_recv, me).wait_recv()
    loss_ref[0] = jnp.sum(loss_total[...]) * loss_scale

    rest_u = wu.at[pl.ds(0, SEG - 1)]
    rest_d = wd.at[pl.ds(0, SEG - 1)]
    rcopy(rest_u, rest_u, agu_send, gain_recv, me).wait_send()
    rcopy(rest_d, rest_d, agd_send, gain_recv, me).wait_send()
    rest_gain = gains.at[pl.ds(0, SEG - 1)]
    rcopy(rest_gain, rest_gain, gain_send, gain_recv, me).wait_send()
    rcopy(all_rest, all_rest, as_send, dg_recv, me).wait_send()
    rcopy(all_rest, all_rest, gs_send, dg_recv, me).wait_send()
    rcopy(rest_dg, rest_dg, dg_send, dg_recv, me).wait_send()

    @pl.when(row < n_rows - 1)
    def _():
        rcopy(acts.at[0], acts.at[0], fwd_send, dg_recv, me).wait_send()

    @pl.when(row > 0)
    def _():
        rcopy(grads.at[0], grads.at[0], bwd_send, dg_recv, me).wait_send()

    @pl.when(row == n_rows - 1)
    def _():
        rest_row = loss_stash.at[pl.ds(0, SEG - 1)]
        rcopy(rest_row, rest_row, lrow_send, lrow_recv, me).wait_send()
        for step in range(1, n_rows):
            rcopy(loss_total, loss_total, lcol_send, lcol_recv, me).wait_send()


def solution(mesh):
    n_stages = mesh.shape['stage']

    def stage_body(x_in, y_target, w_up, w_down, norm_gain):
        n_micro, n_tok, d_model = x_in.shape
        d_ff = w_up.shape[2]
        n_rows = n_micro * n_tok
        chunk = n_rows // SEG // N_CHUNKS
        loss_scale = 1.0 / (n_rows * d_model)
        sem = pltpu.SemaphoreType.DMA
        act_shape = (N_CHUNKS, chunk, d_model)
        scratch = [
            pltpu.VMEM((SEG, d_model, d_ff), BF16),
            pltpu.VMEM((SEG, d_ff, d_model), BF16),
            pltpu.VMEM((SEG, 8, d_model), F32),
            pltpu.VMEM((SEG + 1,) + act_shape, BF16),
            pltpu.VMEM((SEG + 1,) + act_shape, BF16),
            pltpu.VMEM((SEG, N_CHUNKS, chunk, d_ff), F32),
            pltpu.VMEM((N_CHUNKS, SEG, chunk, d_model), BF16),
            pltpu.VMEM((N_CHUNKS, SEG, chunk, d_model), BF16),
            pltpu.VMEM((N_CHUNKS, SEG, chunk, d_ff), BF16),
            pltpu.VMEM((N_CHUNKS, SEG, chunk, d_ff), F32),
            pltpu.VMEM(act_shape, BF16),
            pltpu.VMEM((d_model, d_ff), F32),
            pltpu.VMEM((SEG, 8, d_model), F32),
            pltpu.VMEM((SEG, 8, d_model), F32),
            pltpu.VMEM((8, d_model), F32),
            pltpu.VMEM((SEG, 8, d_model), F32),
            pltpu.VMEM((8, d_model), F32),
            sem((2,)), sem((N_CHUNKS,)), sem((N_CHUNKS,)),
            sem, sem((SEG,)), sem, sem((SEG,)), sem, sem,
            sem, sem, sem, sem((N_CHUNKS,)), sem, sem((N_CHUNKS,)), sem, sem((N_CHUNKS,)),
            sem, sem, sem, sem, sem, sem,
        ]
        any_spec = pl.BlockSpec(memory_space=pl.ANY)
        vmem_spec = pl.BlockSpec(memory_space=pltpu.VMEM)
        dw_up, dw_down, dgain, loss = pl.pallas_call(
            functools.partial(step_kernel, n_stages, loss_scale),
            out_shape=(jax.ShapeDtypeStruct(w_up.shape, F32), jax.ShapeDtypeStruct(w_down.shape, F32),
                       jax.ShapeDtypeStruct(norm_gain.shape, F32), jax.ShapeDtypeStruct((1,), F32)),
            in_specs=[any_spec, any_spec, any_spec, any_spec, vmem_spec],
            out_specs=(vmem_spec, vmem_spec, vmem_spec, pl.BlockSpec(memory_space=pltpu.SMEM)),
            scratch_shapes=scratch,
            compiler_params=pltpu.CompilerParams(collective_id=0, has_side_effects=True,
                                                 vmem_limit_bytes=67043328),
        )(x_in.reshape(n_rows, d_model), y_target.reshape(n_rows, d_model), w_up, w_down, norm_gain)
        return dw_up, dw_down, dgain, loss

    return jax.shard_map(stage_body, mesh=mesh,
                         in_specs=(P('dp'), P('dp'), P('stage'), P('stage'), P('stage')),
                         out_specs=(P(('dp', 'stage')), P(('dp', 'stage')), P(('dp', 'stage')), P('dp')),
                         check_vma=False)
```

```python
import functools

import jax
import jax.numpy as jnp
from jax import lax
from jax.experimental import pallas as pl
from jax.experimental.pallas import tpu as pltpu
from jax.sharding import PartitionSpec as P

NORM_EPS = 1e-6
SEG = 8
N_CHUNKS = 4
COLS = 256
HALF = SEG // 2
UNROLL = 4
BOTH_UNROLL = 2
GELU_C = 0.7978845608028654
GELU_A = 0.044715
MESH = pl.DeviceIdType.MESH
F32 = jnp.float32
BF16 = jnp.bfloat16


def dot_nn(lhs, rhs):
    return lax.dot_general(lhs, rhs, (((1,), (0,)), ((), ())), preferred_element_type=F32)


def dot_nt(lhs, rhs):
    return lax.dot_general(lhs, rhs, (((1,), (1,)), ((), ())), preferred_element_type=F32)


def dot_tn(lhs, rhs):
    return lax.dot_general(lhs, rhs, (((0,), (0,)), ((), ())), preferred_element_type=F32)


def gelu_gate(hidden):
    sq = hidden * hidden
    gate = 0.5 + 0.5 * jnp.tanh(hidden * (GELU_C + (GELU_C * GELU_A) * sq))
    return gate, sq


def gelu_value(hidden):
    return hidden * gelu_gate(hidden)[0]


def gelu_slope(hidden, gate, sq):
    return gate + ((gate * (1.0 - gate)) * hidden) * (2.0 * GELU_C + (6.0 * GELU_C * GELU_A) * sq)


def inv_rms_of(x_float):
    return lax.rsqrt(jnp.mean(x_float * x_float, axis=-1, keepdims=True) + NORM_EPS)


def fold_rows(block):
    rows, cols = block.shape
    return jnp.sum(block.reshape(rows // 8, 8, cols), axis=0)


def step_kernel(n_stages, loss_scale,
                x_hbm, y_hbm, wu_hbm, wd_hbm, gain_ref,
                dwu_ref, dwd_ref, dgain_ref, loss_ref,
                wu, wd, gains, acts, grads, hiddens, act_stash, grad_stash, value_stash, slope_stash, targets, dwd_t,
                dg_part, dg_stash, loss_part, loss_stash, loss_total,
                load_sem, x_sem, y_sem, agu_send, agu_recv, agd_send, agd_recv, gain_send, gain_recv,
                as_send, as_recv, gs_send, gs_recv, fwd_send, fwd_recv, bwd_send, bwd_recv,
                dg_send, dg_recv, lrow_send, lrow_recv, lcol_send, lcol_recv):
    n_rows = n_stages // SEG
    n_chips = SEG // 2
    chunk = acts.shape[2]
    d_model = acts.shape[3]
    d_ff = wu.shape[2]
    me = lax.axis_index('stage')
    row = lax.div(me, SEG)
    r = lax.rem(me, SEG)
    chip = lax.div(r, 2)
    core = lax.rem(r, 2)
    row_base = row * SEG
    left = lax.rem(chip + n_chips - 1, n_chips) * 2 + core
    right = lax.rem(chip + 1, n_chips) * 2 + core
    across = lax.rem(chip + 2, n_chips) * 2 + core
    flip = 1 - 2 * core
    sib = r + flip

    def rcopy(src, dst, send_sem, recv_sem, dev):
        return pltpu.make_async_remote_copy(src_ref=src, dst_ref=dst, send_sem=send_sem, recv_sem=recv_sem,
                                            device_id={'stage': dev}, device_id_type=MESH)

    load_u = pltpu.make_async_copy(wu_hbm.at[0], wu.at[r], load_sem.at[0])
    load_d = pltpu.make_async_copy(wd_hbm.at[0], wd.at[r], load_sem.at[1])
    load_u.start()
    load_d.start()

    def x_load(k):
        first = pl.multiple_of((r * N_CHUNKS + k) * chunk, chunk)
        return pltpu.make_async_copy(x_hbm.at[pl.ds(first, chunk)], acts.at[0, k], x_sem.at[k])

    def y_load(k):
        first = pl.multiple_of((r * N_CHUNKS + k) * chunk, chunk)
        return pltpu.make_async_copy(y_hbm.at[pl.ds(first, chunk)], targets.at[k], y_sem.at[k])

    @pl.when(row == 0)
    def _():
        for k in range(N_CHUNKS):
            x_load(k).start()

    @pl.when(row == n_rows - 1)
    def _():
        for k in range(N_CHUNKS):
            y_load(k).start()

    gains[r] = jnp.broadcast_to(gain_ref[...], (8, d_model))
    dg_part[...] = jnp.zeros_like(dg_part)
    loss_part[...] = jnp.zeros_like(loss_part)

    with jax.named_scope('barrier'):
        barrier = pltpu.get_barrier_semaphore()
        for step in range(1, SEG):
            pl.semaphore_signal(barrier, inc=1, device_id={'stage': row_base + lax.rem(r + step, SEG)}, device_id_type=MESH)
        for step in range(1, n_rows):
            pl.semaphore_signal(barrier, inc=1, device_id={'stage': lax.rem(row + step, n_rows) * SEG + r}, device_id_type=MESH)
        pl.semaphore_wait(barrier, SEG - 1 + n_rows - 1)

    def u_copy(slot, dev):
        return rcopy(wu.at[slot], wu.at[slot], agu_send, agu_recv.at[slot], row_base + dev)

    def d_copy(slot, dev):
        return rcopy(wd.at[slot], wd.at[slot], agd_send, agd_recv.at[slot], row_base + dev)

    with jax.named_scope('w_load_u'):
        load_u.wait()
    with jax.named_scope('w_load_d'):
        load_d.wait()
    u_copy(r, right).start()
    d_copy(r, left).start()
    d_copy(r, right).start()
    u_copy(r, left).start()
    u_copy(r, sib).start()
    d_copy(r, sib).start()
    for step in range(1, SEG):
        rcopy(gains.at[r], gains.at[r], gain_send, gain_recv, row_base + lax.rem(r + step, SEG)).start()

    with jax.named_scope('ag_u_left'):
        u_copy(left, r).wait_recv()
    u_copy(left, right).start()
    u_copy(left, sib).start()
    with jax.named_scope('ag_d_right'):
        d_copy(right, r).wait_recv()
    d_copy(right, left).start()
    d_copy(right, sib).start()
    with jax.named_scope('ag_d_left'):
        d_copy(left, r).wait_recv()
    d_copy(left, sib).start()
    with jax.named_scope('ag_u_right'):
        u_copy(right, r).wait_recv()
    u_copy(right, sib).start()
    with jax.named_scope('ag_u_across'):
        u_copy(across, r).wait_recv()
    u_copy(across, sib).start()
    with jax.named_scope('ag_d_across'):
        d_copy(across, r).wait_recv()
    d_copy(across, sib).start()
    with jax.named_scope('ag_sib'):
        for slot in (sib, left + flip, right + flip, across + flip):
            u_copy(slot, r).wait_recv()
            d_copy(slot, r).wait_recv()
    rcopy(gains.at[pl.ds(0, SEG - 1)], gains.at[pl.ds(0, SEG - 1)], gain_send, gain_recv, me).wait_recv()

    def act_ship(layer, k):
        mine = layer == r
        return rcopy(acts.at[layer, k], act_stash.at[k, jnp.where(mine, SEG, r)], as_send, as_recv,
                     row_base + jnp.where(mine, sib, layer))

    def grad_ship(layer, k):
        mine = layer == r
        return rcopy(grads.at[layer + 1, k], grad_stash.at[k, jnp.where(mine, SEG, r)], gs_send, gs_recv.at[k],
                     row_base + jnp.where(mine, sib, layer))

    def fwd_layer(layer, k):
        x_float = acts[layer, k].astype(F32)
        normed = (x_float * inv_rms_of(x_float) * gains[layer, 0:1, :]).astype(BF16)
        out = x_float
        for part in range(0, d_ff, COLS):
            cols = slice(part, part + COLS)
            hidden = dot_nn(normed, wu[layer, :, cols])
            hiddens[layer, k, :, cols] = hidden
            out += dot_nn(gelu_value(hidden).astype(BF16), wd[layer, cols, :])
        acts[layer + 1, k] = out.astype(BF16)
        return k

    def fwd_input_wait(k):
        @pl.when(row == 0)
        def _():
            x_load(k).wait()

        @pl.when(row > 0)
        def _():
            with jax.named_scope('fwd_wait'):
                rcopy(acts.at[0, k], acts.at[0, k], fwd_send, fwd_recv.at[k], me).wait_recv()

    def top_grad(k):
        y_load(k).wait()
        error_val = acts[SEG, k].astype(F32) - targets[k].astype(F32)
        loss_part[...] += fold_rows(error_val * error_val)
        grads[SEG, k] = ((2.0 * loss_scale) * error_val).astype(BF16)

    def fwd_chunk(k, carry):
        fwd_input_wait(k)
        with jax.named_scope('fwd_layers'):
            lax.fori_loop(0, SEG, fwd_layer, k, unroll=UNROLL)

        @pl.when(row < n_rows - 1)
        def _():
            rcopy(acts.at[SEG, k], acts.at[0, k], fwd_send, fwd_recv.at[k], me + SEG).start()
        for layer in range(SEG):
            act_ship(layer, k).start()

        @pl.when(row == n_rows - 1)
        def _():
            top_grad(k)
        return carry

    lax.fori_loop(0, jnp.where(row == n_rows - 1, 1, N_CHUNKS), fwd_chunk, 0)

    def bwd_layer(step, k):
        layer = SEG - 1 - step
        grad_out = grads[layer + 1, k]
        x_float = acts[layer, k].astype(F32)
        inv_rms = inv_rms_of(x_float)
        x_hat = x_float * inv_rms
        gain = gains[layer, 0:1, :]
        grad_normed = 0.0
        for part in range(0, d_ff, COLS):
            cols = slice(part, part + COLS)
            hidden = hiddens[layer, k, :, cols]
            slope = gelu_slope(hidden, *gelu_gate(hidden))
            grad_gelu = dot_nt(grad_out, wd[layer, cols, :]).astype(BF16).astype(F32)
            grad_hidden = (grad_gelu * slope).astype(BF16)
            grad_normed += dot_nt(grad_hidden, wu[layer, :, cols])
        grad_normed = grad_normed.astype(BF16).astype(F32)
        dg_part[layer] += fold_rows(grad_normed * x_hat)
        grad_hat = grad_normed * gain
        mean_dot = jnp.mean(grad_hat * x_hat, axis=-1, keepdims=True)
        grad_x = inv_rms * (grad_hat - x_hat * mean_dot)
        grads[layer, k] = (grad_out.astype(F32) + grad_x).astype(BF16)
        return k

    def bwd_output(k):
        @pl.when(row > 0)
        def _():
            rcopy(grads.at[0, k], grads.at[SEG, k], bwd_send, bwd_recv.at[k], me - SEG).start()
        for layer in range(SEG):
            grad_ship(layer, k).start()

    def both_layers(step, k):
        fwd_layer(step, k)
        bwd_layer(step, k - 1)
        return k

    def both_chunks(k, carry):
        fwd_input_wait(k)
        with jax.named_scope('both_layers'):
            lax.fori_loop(0, SEG, both_layers, k, unroll=BOTH_UNROLL)
        bwd_output(k - 1)
        top_grad(k)
        for layer in range(SEG):
            act_ship(layer, k).start()
        return carry

    @pl.when(row == n_rows - 1)
    def _():
        lax.fori_loop(1, N_CHUNKS, both_chunks, 0)
        loss_stash[r] = loss_part[...]
        for step in range(1, SEG):
            rcopy(loss_stash.at[r], loss_stash.at[r], lrow_send, lrow_recv, row_base + lax.rem(r + step, SEG)).start()

    rest = act_stash.at[0, pl.ds(0, SEG)]
    all_rest = acts.at[pl.ds(0, SEG)]

    def owner_block(index):
        return lax.div(index, 2), pl.ds(lax.rem(index, 2) * HALF, HALF)

    def value_block(index, carry):
        k, srcs = owner_block(index)
        x_float = act_stash[k, srcs].reshape(HALF * chunk, d_model).astype(F32)
        normed = (x_float * inv_rms_of(x_float) * gains[r, 0:1, :]).astype(BF16)
        act_stash[k, srcs] = normed.reshape(HALF, chunk, d_model)
        for part in range(0, d_ff, COLS):
            cols = slice(part, part + COLS)
            hidden = dot_nn(normed, wu[r, :, cols])
            gate, sq = gelu_gate(hidden)
            value_stash[k, srcs, :, cols] = (hidden * gate).astype(BF16).reshape(HALF, chunk, COLS)
            slope_stash[k, srcs, :, cols] = gelu_slope(hidden, gate, sq).reshape(HALF, chunk, COLS)
        return carry

    def value_phase():
        with jax.named_scope('as_wait'):
            rcopy(all_rest, all_rest, as_send, as_recv, me).wait_recv()
        for k in range(N_CHUNKS):
            act_stash[k, r] = acts[r, k]
        dwu_ref[...] = jnp.zeros_like(dwu_ref)
        dwd_t[...] = jnp.zeros_like(dwd_t)
        with jax.named_scope('value_blocks'):
            lax.fori_loop(0, 2 * N_CHUNKS, value_block, 0)

    @pl.when(row < n_rows - 1)
    def _():
        value_phase()

    def bwd_chunk(k, carry):
        @pl.when(row < n_rows - 1)
        def _():
            with jax.named_scope('bwd_wait'):
                rcopy(grads.at[SEG, k], grads.at[SEG, k], bwd_send, bwd_recv.at[k], me).wait_recv()

        with jax.named_scope('bwd_layers'):
            lax.fori_loop(0, SEG, bwd_layer, k, unroll=UNROLL)
        bwd_output(k)
        return carry

    lax.fori_loop(jnp.where(row == n_rows - 1, N_CHUNKS - 1, 0), N_CHUNKS, bwd_chunk, 0)

    def dg_ship(layer):
        return rcopy(dg_part.at[layer], dg_stash.at[r], dg_send, dg_recv, row_base + layer)

    for step in range(1, SEG):
        dg_ship(lax.rem(r + step, SEG)).start()
    dg_stash[r] = dg_part[r]

    @pl.when(row == n_rows - 1)
    def _():
        rest = loss_stash.at[pl.ds(0, SEG - 1)]
        rcopy(rest, rest, lrow_send, lrow_recv, me).wait_recv()
        loss_total[...] = jnp.sum(loss_stash[...], axis=0)
        for step in range(1, n_rows):
            rcopy(loss_total, loss_total, lcol_send, lcol_recv, me - step * SEG).start()

    @pl.when(row == n_rows - 1)
    def _():
        value_phase()

    for k in range(N_CHUNKS):
        grad_stash[k, r] = grads[r + 1, k]

    def weight_block(k, carry):
        rows = SEG * chunk
        with jax.named_scope('gs_wait'):
            rcopy(rest, rest, gs_send, gs_recv.at[k], me).wait_recv()
        normed = act_stash[k, pl.ds(0, SEG)].reshape(rows, d_model)
        grad_out = grad_stash[k, pl.ds(0, SEG)].reshape(rows, d_model)
        for part in range(0, d_ff, COLS):
            cols = slice(part, part + COLS)
            grad_gelu = dot_nt(grad_out, wd[r, cols, :]).astype(BF16).astype(F32)
            grad_hidden = (grad_gelu * slope_stash[k, :, :, cols].reshape(rows, COLS)).astype(BF16)
            dwu_ref[0, :, cols] += dot_tn(normed, grad_hidden)
            dwd_t[:, cols] += dot_tn(grad_out, value_stash[k, :, :, cols].reshape(rows, COLS))
        return carry

    with jax.named_scope('weight_blocks'):
        lax.fori_loop(0, N_CHUNKS, weight_block, 0)
    with jax.named_scope('turn'):
        dwd_ref[0] = dwd_t[...].T

    rest_dg = dg_stash.at[pl.ds(0, SEG - 1)]
    with jax.named_scope('dg_wait'):
        rcopy(rest_dg, rest_dg, dg_send, dg_recv, me).wait_recv()
    dgain_ref[...] = jnp.sum(jnp.sum(dg_stash[...], axis=0), axis=0, keepdims=True)

    @pl.when(row < n_rows - 1)
    def _():
        rcopy(loss_total, loss_total, lcol_send, lcol_recv, me).wait_recv()
    loss_ref[0] = jnp.sum(loss_total[...]) * loss_scale

    rest_u = wu.at[pl.ds(0, SEG - 1)]
    rest_d = wd.at[pl.ds(0, SEG - 1)]
    rcopy(rest_u, rest_u, agu_send, gain_recv, me).wait_send()
    rcopy(rest_d, rest_d, agd_send, gain_recv, me).wait_send()
    rest_gain = gains.at[pl.ds(0, SEG - 1)]
    rcopy(rest_gain, rest_gain, gain_send, gain_recv, me).wait_send()
    rcopy(all_rest, all_rest, as_send, dg_recv, me).wait_send()
    rcopy(all_rest, all_rest, gs_send, dg_recv, me).wait_send()
    rcopy(rest_dg, rest_dg, dg_send, dg_recv, me).wait_send()

    @pl.when(row < n_rows - 1)
    def _():
        rcopy(acts.at[0], acts.at[0], fwd_send, dg_recv, me).wait_send()

    @pl.when(row > 0)
    def _():
        rcopy(grads.at[0], grads.at[0], bwd_send, dg_recv, me).wait_send()

    @pl.when(row == n_rows - 1)
    def _():
        rest_row = loss_stash.at[pl.ds(0, SEG - 1)]
        rcopy(rest_row, rest_row, lrow_send, lrow_recv, me).wait_send()
        for step in range(1, n_rows):
            rcopy(loss_total, loss_total, lcol_send, lcol_recv, me).wait_send()


def solution(mesh):
    n_stages = mesh.shape['stage']

    def stage_body(x_in, y_target, w_up, w_down, norm_gain):
        n_micro, n_tok, d_model = x_in.shape
        d_ff = w_up.shape[2]
        n_rows = n_micro * n_tok
        chunk = n_rows // SEG // N_CHUNKS
        loss_scale = 1.0 / (n_rows * d_model)
        sem = pltpu.SemaphoreType.DMA
        act_shape = (N_CHUNKS, chunk, d_model)
        scratch = [
            pltpu.VMEM((SEG, d_model, d_ff), BF16),
            pltpu.VMEM((SEG, d_ff, d_model), BF16),
            pltpu.VMEM((SEG, 8, d_model), F32),
            pltpu.VMEM((SEG + 1,) + act_shape, BF16),
            pltpu.VMEM((SEG + 1,) + act_shape, BF16),
            pltpu.VMEM((SEG, N_CHUNKS, chunk, d_ff), F32),
            pltpu.VMEM((N_CHUNKS, SEG + 1, chunk, d_model), BF16),
            pltpu.VMEM((N_CHUNKS, SEG + 1, chunk, d_model), BF16),
            pltpu.VMEM((N_CHUNKS, SEG, chunk, d_ff), BF16),
            pltpu.VMEM((N_CHUNKS, SEG, chunk, d_ff), F32),
            pltpu.VMEM(act_shape, BF16),
            pltpu.VMEM((d_model, d_ff), F32),
            pltpu.VMEM((SEG, 8, d_model), F32),
            pltpu.VMEM((SEG, 8, d_model), F32),
            pltpu.VMEM((8, d_model), F32),
            pltpu.VMEM((SEG, 8, d_model), F32),
            pltpu.VMEM((8, d_model), F32),
            sem((2,)), sem((N_CHUNKS,)), sem((N_CHUNKS,)),
            sem, sem((SEG,)), sem, sem((SEG,)), sem, sem,
            sem, sem, sem, sem((N_CHUNKS,)), sem, sem((N_CHUNKS,)), sem, sem((N_CHUNKS,)),
            sem, sem, sem, sem, sem, sem,
        ]
        any_spec = pl.BlockSpec(memory_space=pl.ANY)
        vmem_spec = pl.BlockSpec(memory_space=pltpu.VMEM)
        dw_up, dw_down, dgain, loss = pl.pallas_call(
            functools.partial(step_kernel, n_stages, loss_scale),
            out_shape=(jax.ShapeDtypeStruct(w_up.shape, F32), jax.ShapeDtypeStruct(w_down.shape, F32),
                       jax.ShapeDtypeStruct(norm_gain.shape, F32), jax.ShapeDtypeStruct((1,), F32)),
            in_specs=[any_spec, any_spec, any_spec, any_spec, vmem_spec],
            out_specs=(vmem_spec, vmem_spec, vmem_spec, pl.BlockSpec(memory_space=pltpu.SMEM)),
            scratch_shapes=scratch,
            compiler_params=pltpu.CompilerParams(collective_id=0, has_side_effects=True,
                                                 vmem_limit_bytes=67043328),
        )(x_in.reshape(n_rows, d_model), y_target.reshape(n_rows, d_model), w_up, w_down, norm_gain)
        return dw_up, dw_down, dgain, loss

    return jax.shard_map(stage_body, mesh=mesh,
                         in_specs=(P('dp'), P('dp'), P('stage'), P('stage'), P('stage')),
                         out_specs=(P(('dp', 'stage')), P(('dp', 'stage')), P(('dp', 'stage')), P('dp')),
                         check_vma=False)
```

```python
import functools

import jax
import jax.numpy as jnp
from jax import lax
from jax.experimental import pallas as pl
from jax.experimental.pallas import tpu as pltpu
from jax.sharding import PartitionSpec as P

NORM_EPS = 1e-6
SEG = 8
N_CHUNKS = 4
COLS = 256
HALF = SEG // 2
GROUP = 4
LATE_ROWS = 2
GELU_C = 0.7978845608028654
GELU_A = 0.044715
MESH = pl.DeviceIdType.MESH
F32 = jnp.float32
BF16 = jnp.bfloat16


def dot_nn(lhs, rhs):
    return lax.dot_general(lhs, rhs, (((1,), (0,)), ((), ())), preferred_element_type=F32)


def dot_nt(lhs, rhs):
    return lax.dot_general(lhs, rhs, (((1,), (1,)), ((), ())), preferred_element_type=F32)


def dot_tn(lhs, rhs):
    return lax.dot_general(lhs, rhs, (((0,), (0,)), ((), ())), preferred_element_type=F32)


def gelu_gate(hidden):
    sq = hidden * hidden
    gate = 0.5 + 0.5 * jnp.tanh(hidden * (GELU_C + (GELU_C * GELU_A) * sq))
    return gate, sq


def gelu_value(hidden):
    return hidden * gelu_gate(hidden)[0]


def gelu_slope(hidden, gate, sq):
    return gate + ((gate * (1.0 - gate)) * hidden) * (2.0 * GELU_C + (6.0 * GELU_C * GELU_A) * sq)


def inv_rms_of(x_float):
    return lax.rsqrt(jnp.mean(x_float * x_float, axis=-1, keepdims=True) + NORM_EPS)


def fold_rows(block):
    rows, cols = block.shape
    return jnp.sum(block.reshape(rows // 8, 8, cols), axis=0)


def step_kernel(n_stages, loss_scale,
                x_hbm, y_hbm, wu_hbm, wd_hbm, gain_ref,
                dwu_ref, dwd_ref, dgain_ref, loss_ref,
                wu, wd, gains, acts, grads, hiddens, act_stash, grad_stash, value_stash, slope_stash, targets, dwd_t,
                dg_part, dg_stash, loss_part, loss_stash, loss_total,
                load_sem, x_sem, y_sem, agu_send, agu_recv, agd_send, agd_recv, gain_send, gain_recv,
                as_send, as_recv, gs_send, gs_recv, fwd_send, fwd_recv, bwd_send, bwd_recv,
                dg_send, dg_recv, lrow_send, lrow_recv, lcol_send, lcol_recv):
    n_rows = n_stages // SEG
    n_chips = SEG // 2
    chunk = acts.shape[2]
    d_model = acts.shape[3]
    d_ff = wu.shape[2]
    me = lax.axis_index('stage')
    row = lax.div(me, SEG)
    r = lax.rem(me, SEG)
    chip = lax.div(r, 2)
    core = lax.rem(r, 2)
    row_base = row * SEG
    left = lax.rem(chip + n_chips - 1, n_chips) * 2 + core
    right = lax.rem(chip + 1, n_chips) * 2 + core
    across = lax.rem(chip + 2, n_chips) * 2 + core
    flip = 1 - 2 * core
    sib = r + flip

    def rcopy(src, dst, send_sem, recv_sem, dev):
        return pltpu.make_async_remote_copy(src_ref=src, dst_ref=dst, send_sem=send_sem, recv_sem=recv_sem,
                                            device_id={'stage': dev}, device_id_type=MESH)

    load_u = pltpu.make_async_copy(wu_hbm.at[0], wu.at[r], load_sem.at[0])
    load_d = pltpu.make_async_copy(wd_hbm.at[0], wd.at[r], load_sem.at[1])
    load_u.start()
    load_d.start()

    def x_load(k):
        first = pl.multiple_of((r * N_CHUNKS + k) * chunk, chunk)
        return pltpu.make_async_copy(x_hbm.at[pl.ds(first, chunk)], acts.at[0, k], x_sem.at[k])

    def y_load(k):
        first = pl.multiple_of((r * N_CHUNKS + k) * chunk, chunk)
        return pltpu.make_async_copy(y_hbm.at[pl.ds(first, chunk)], targets.at[k], y_sem.at[k])

    @pl.when(row == 0)
    def _():
        for k in range(N_CHUNKS):
            x_load(k).start()

    @pl.when(row == n_rows - 1)
    def _():
        for k in range(N_CHUNKS):
            y_load(k).start()

    gains[r] = jnp.broadcast_to(gain_ref[...], (8, d_model))
    dg_part[...] = jnp.zeros_like(dg_part)
    loss_part[...] = jnp.zeros_like(loss_part)

    with jax.named_scope('barrier'):
        barrier = pltpu.get_barrier_semaphore()
        for step in range(1, SEG):
            pl.semaphore_signal(barrier, inc=1, device_id={'stage': row_base + lax.rem(r + step, SEG)}, device_id_type=MESH)
        for step in range(1, n_rows):
            pl.semaphore_signal(barrier, inc=1, device_id={'stage': lax.rem(row + step, n_rows) * SEG + r}, device_id_type=MESH)
        pl.semaphore_wait(barrier, SEG - 1 + n_rows - 1)

    def u_copy(slot, dev):
        return rcopy(wu.at[slot], wu.at[slot], agu_send, agu_recv.at[slot], row_base + dev)

    def d_copy(slot, dev):
        return rcopy(wd.at[slot], wd.at[slot], agd_send, agd_recv.at[slot], row_base + dev)

    with jax.named_scope('w_load_u'):
        load_u.wait()
    with jax.named_scope('w_load_d'):
        load_d.wait()
    u_copy(r, right).start()
    d_copy(r, left).start()
    d_copy(r, right).start()
    u_copy(r, left).start()
    u_copy(r, sib).start()
    d_copy(r, sib).start()
    for step in range(1, SEG):
        rcopy(gains.at[r], gains.at[r], gain_send, gain_recv, row_base + lax.rem(r + step, SEG)).start()

    with jax.named_scope('ag_u_left'):
        u_copy(left, r).wait_recv()
    u_copy(left, right).start()
    u_copy(left, sib).start()
    with jax.named_scope('ag_d_right'):
        d_copy(right, r).wait_recv()
    d_copy(right, left).start()
    d_copy(right, sib).start()
    with jax.named_scope('ag_d_left'):
        d_copy(left, r).wait_recv()
    d_copy(left, sib).start()
    with jax.named_scope('ag_u_right'):
        u_copy(right, r).wait_recv()
    u_copy(right, sib).start()
    with jax.named_scope('ag_u_across'):
        u_copy(across, r).wait_recv()
    u_copy(across, sib).start()
    with jax.named_scope('ag_d_across'):
        d_copy(across, r).wait_recv()
    d_copy(across, sib).start()
    with jax.named_scope('ag_sib'):
        for slot in (sib, left + flip, right + flip, across + flip):
            u_copy(slot, r).wait_recv()
            d_copy(slot, r).wait_recv()
    rcopy(gains.at[pl.ds(0, SEG - 1)], gains.at[pl.ds(0, SEG - 1)], gain_send, gain_recv, me).wait_recv()

    def act_ship(layer, k):
        mine = layer == r
        return rcopy(acts.at[layer, k], act_stash.at[k, jnp.where(mine, SEG, r)], as_send, as_recv,
                     row_base + jnp.where(mine, sib, layer))

    def grad_ship(layer, k):
        mine = layer == r
        return rcopy(grads.at[layer + 1, k], grad_stash.at[k, jnp.where(mine, SEG, r)], gs_send, gs_recv.at[k],
                     row_base + jnp.where(mine, sib, layer))

    def fwd_layer(layer, k):
        x_float = acts[layer, k].astype(F32)
        normed = (x_float * inv_rms_of(x_float) * gains[layer, 0:1, :]).astype(BF16)
        out = x_float
        for part in range(0, d_ff, COLS):
            cols = slice(part, part + COLS)
            hidden = dot_nn(normed, wu[layer, :, cols])
            hiddens[layer, k, :, cols] = hidden
            out += dot_nn(gelu_value(hidden).astype(BF16), wd[layer, cols, :])
        acts[layer + 1, k] = out.astype(BF16)

    def fwd_input_wait(k):
        @pl.when(row == 0)
        def _():
            x_load(k).wait()

        @pl.when(row > 0)
        def _():
            with jax.named_scope('fwd_wait'):
                rcopy(acts.at[0, k], acts.at[0, k], fwd_send, fwd_recv.at[k], me).wait_recv()

    def top_grad(k):
        y_load(k).wait()
        error_val = acts[SEG, k].astype(F32) - targets[k].astype(F32)
        loss_part[...] += fold_rows(error_val * error_val)
        grads[SEG, k] = ((2.0 * loss_scale) * error_val).astype(BF16)

    def fwd_group(group, k):
        for step in range(GROUP):
            fwd_layer(group * GROUP + step, k)
        return k

    def fwd_chunk(k, carry):
        fwd_input_wait(k)
        with jax.named_scope('fwd_layers'):
            lax.fori_loop(0, SEG // GROUP, fwd_group, k)

        @pl.when(row < n_rows - 1)
        def _():
            rcopy(acts.at[SEG, k], acts.at[0, k], fwd_send, fwd_recv.at[k], me + SEG).start()
        for layer in range(SEG):
            act_ship(layer, k).start()

        @pl.when(row == n_rows - 1)
        def _():
            top_grad(k)
        return carry

    lax.fori_loop(0, jnp.where(row == n_rows - 1, 1, N_CHUNKS), fwd_chunk, 0)

    def bwd_layer(step, k):
        layer = SEG - 1 - step
        grad_out = grads[layer + 1, k]
        x_float = acts[layer, k].astype(F32)
        inv_rms = inv_rms_of(x_float)
        x_hat = x_float * inv_rms
        gain = gains[layer, 0:1, :]
        grad_normed = 0.0
        for part in range(0, d_ff, COLS):
            cols = slice(part, part + COLS)
            hidden = hiddens[layer, k, :, cols]
            slope = gelu_slope(hidden, *gelu_gate(hidden))
            grad_gelu = dot_nt(grad_out, wd[layer, cols, :]).astype(BF16).astype(F32)
            grad_hidden = (grad_gelu * slope).astype(BF16)
            grad_normed += dot_nt(grad_hidden, wu[layer, :, cols])
        grad_normed = grad_normed.astype(BF16).astype(F32)
        dg_part[layer] += fold_rows(grad_normed * x_hat)
        grad_hat = grad_normed * gain
        mean_dot = jnp.mean(grad_hat * x_hat, axis=-1, keepdims=True)
        grad_x = inv_rms * (grad_hat - x_hat * mean_dot)
        grads[layer, k] = (grad_out.astype(F32) + grad_x).astype(BF16)

    def bwd_group(group, k):
        for step in range(GROUP):
            bwd_layer(group * GROUP + step, k)

        @pl.when((row > 0) & (group == SEG // GROUP - 1))
        def _():
            rcopy(grads.at[0, k], grads.at[SEG, k], bwd_send, bwd_recv.at[k], me - SEG).start()
        for step in range(GROUP):
            grad_ship(SEG - 1 - group * GROUP - step, k).start()
        return k

    def both_group(group, k):
        for step in range(GROUP):
            fwd_layer(group * GROUP + step, k)
            bwd_layer(group * GROUP + step, k - 1)

        @pl.when((row > 0) & (group == SEG // GROUP - 1))
        def _():
            rcopy(grads.at[0, k - 1], grads.at[SEG, k - 1], bwd_send, bwd_recv.at[k - 1], me - SEG).start()
        for step in range(GROUP):
            grad_ship(SEG - 1 - group * GROUP - step, k - 1).start()
        return k

    def both_chunks(k, carry):
        fwd_input_wait(k)
        with jax.named_scope('both_layers'):
            lax.fori_loop(0, SEG // GROUP, both_group, k)
        top_grad(k)
        for layer in range(SEG):
            act_ship(layer, k).start()
        return carry

    @pl.when(row == n_rows - 1)
    def _():
        lax.fori_loop(1, N_CHUNKS, both_chunks, 0)
        loss_stash[r] = loss_part[...]
        for step in range(1, SEG):
            rcopy(loss_stash.at[r], loss_stash.at[r], lrow_send, lrow_recv, row_base + lax.rem(r + step, SEG)).start()

    rest = act_stash.at[0, pl.ds(0, SEG)]
    all_rest = acts.at[pl.ds(0, SEG)]

    def owner_block(index):
        return lax.div(index, 2), pl.ds(lax.rem(index, 2) * HALF, HALF)

    def value_block(index, carry):
        k, srcs = owner_block(index)
        x_float = act_stash[k, srcs].reshape(HALF * chunk, d_model).astype(F32)
        normed = (x_float * inv_rms_of(x_float) * gains[r, 0:1, :]).astype(BF16)
        act_stash[k, srcs] = normed.reshape(HALF, chunk, d_model)
        for part in range(0, d_ff, COLS):
            cols = slice(part, part + COLS)
            hidden = dot_nn(normed, wu[r, :, cols])
            gate, sq = gelu_gate(hidden)
            value_stash[k, srcs, :, cols] = (hidden * gate).astype(BF16).reshape(HALF, chunk, COLS)
            slope_stash[k, srcs, :, cols] = gelu_slope(hidden, gate, sq).reshape(HALF, chunk, COLS)
        return carry

    def value_phase():
        with jax.named_scope('as_wait'):
            rcopy(all_rest, all_rest, as_send, as_recv, me).wait_recv()
        for k in range(N_CHUNKS):
            act_stash[k, r] = acts[r, k]
        dwu_ref[...] = jnp.zeros_like(dwu_ref)
        dwd_t[...] = jnp.zeros_like(dwd_t)
        with jax.named_scope('value_blocks'):
            lax.fori_loop(0, 2 * N_CHUNKS, value_block, 0)

    @pl.when(row < n_rows - LATE_ROWS)
    def _():
        value_phase()

    def weight_block(k, carry):
        rows = SEG * chunk
        with jax.named_scope('gs_wait'):
            rcopy(rest, rest, gs_send, gs_recv.at[k], me).wait_recv()
        grad_stash[k, r] = grads[r + 1, k]
        normed = act_stash[k, pl.ds(0, SEG)].reshape(rows, d_model)
        grad_out = grad_stash[k, pl.ds(0, SEG)].reshape(rows, d_model)
        for part in range(0, d_ff, COLS):
            cols = slice(part, part + COLS)
            grad_gelu = dot_nt(grad_out, wd[r, cols, :]).astype(BF16).astype(F32)
            grad_hidden = (grad_gelu * slope_stash[k, :, :, cols].reshape(rows, COLS)).astype(BF16)
            dwu_ref[0, :, cols] += dot_tn(normed, grad_hidden)
            dwd_t[:, cols] += dot_tn(grad_out, value_stash[k, :, :, cols].reshape(rows, COLS))
        return carry

    def bwd_chunk(k, carry):
        @pl.when(row < n_rows - 1)
        def _():
            with jax.named_scope('bwd_wait'):
                rcopy(grads.at[SEG, k], grads.at[SEG, k], bwd_send, bwd_recv.at[k], me).wait_recv()

        with jax.named_scope('bwd_layers'):
            lax.fori_loop(0, SEG // GROUP, bwd_group, k)

        @pl.when((row < n_rows - LATE_ROWS) & (k > 0) & (k < N_CHUNKS - 1))
        def _():
            weight_block(k - 1, 0)
        return carry

    lax.fori_loop(jnp.where(row == n_rows - 1, N_CHUNKS - 1, 0), N_CHUNKS, bwd_chunk, 0)

    def dg_ship(layer):
        return rcopy(dg_part.at[layer], dg_stash.at[r], dg_send, dg_recv, row_base + layer)

    for step in range(1, SEG):
        dg_ship(lax.rem(r + step, SEG)).start()
    dg_stash[r] = dg_part[r]

    @pl.when(row >= n_rows - LATE_ROWS)
    def _():
        value_phase()

    with jax.named_scope('weight_blocks'):
        lax.fori_loop(jnp.where(row < n_rows - LATE_ROWS, N_CHUNKS - 2, 0), N_CHUNKS, weight_block, 0)
    @pl.when(row == n_rows - 1)
    def _():
        rest_row = loss_stash.at[pl.ds(0, SEG - 1)]
        rcopy(rest_row, rest_row, lrow_send, lrow_recv, me).wait_recv()
        loss_total[...] = jnp.sum(loss_stash[...], axis=0)
        for step in range(1, n_rows):
            rcopy(loss_total, loss_total, lcol_send, lcol_recv, me - step * SEG).start()

    with jax.named_scope('turn'):
        dwd_ref[0] = dwd_t[...].T

    rest_dg = dg_stash.at[pl.ds(0, SEG - 1)]
    with jax.named_scope('dg_wait'):
        rcopy(rest_dg, rest_dg, dg_send, dg_recv, me).wait_recv()
    dgain_ref[...] = jnp.sum(jnp.sum(dg_stash[...], axis=0), axis=0, keepdims=True)

    @pl.when(row < n_rows - 1)
    def _():
        rcopy(loss_total, loss_total, lcol_send, lcol_recv, me).wait_recv()
    loss_ref[0] = jnp.sum(loss_total[...]) * loss_scale

    rest_u = wu.at[pl.ds(0, SEG - 1)]
    rest_d = wd.at[pl.ds(0, SEG - 1)]
    rcopy(rest_u, rest_u, agu_send, gain_recv, me).wait_send()
    rcopy(rest_d, rest_d, agd_send, gain_recv, me).wait_send()
    rest_gain = gains.at[pl.ds(0, SEG - 1)]
    rcopy(rest_gain, rest_gain, gain_send, gain_recv, me).wait_send()
    rcopy(all_rest, all_rest, as_send, dg_recv, me).wait_send()
    rcopy(all_rest, all_rest, gs_send, dg_recv, me).wait_send()
    rcopy(rest_dg, rest_dg, dg_send, dg_recv, me).wait_send()

    @pl.when(row < n_rows - 1)
    def _():
        rcopy(acts.at[0], acts.at[0], fwd_send, dg_recv, me).wait_send()

    @pl.when(row > 0)
    def _():
        rcopy(grads.at[0], grads.at[0], bwd_send, dg_recv, me).wait_send()

    @pl.when(row == n_rows - 1)
    def _():
        rest_row = loss_stash.at[pl.ds(0, SEG - 1)]
        rcopy(rest_row, rest_row, lrow_send, lrow_recv, me).wait_send()
        for step in range(1, n_rows):
            rcopy(loss_total, loss_total, lcol_send, lcol_recv, me).wait_send()


def solution(mesh):
    n_stages = mesh.shape['stage']

    def stage_body(x_in, y_target, w_up, w_down, norm_gain):
        n_micro, n_tok, d_model = x_in.shape
        d_ff = w_up.shape[2]
        n_rows = n_micro * n_tok
        chunk = n_rows // SEG // N_CHUNKS
        loss_scale = 1.0 / (n_rows * d_model)
        sem = pltpu.SemaphoreType.DMA
        act_shape = (N_CHUNKS, chunk, d_model)
        scratch = [
            pltpu.VMEM((SEG, d_model, d_ff), BF16),
            pltpu.VMEM((SEG, d_ff, d_model), BF16),
            pltpu.VMEM((SEG, 8, d_model), F32),
            pltpu.VMEM((SEG + 1,) + act_shape, BF16),
            pltpu.VMEM((SEG + 1,) + act_shape, BF16),
            pltpu.VMEM((SEG, N_CHUNKS, chunk, d_ff), F32),
            pltpu.VMEM((N_CHUNKS, SEG + 1, chunk, d_model), BF16),
            pltpu.VMEM((N_CHUNKS, SEG + 1, chunk, d_model), BF16),
            pltpu.VMEM((N_CHUNKS, SEG, chunk, d_ff), BF16),
            pltpu.VMEM((N_CHUNKS, SEG, chunk, d_ff), F32),
            pltpu.VMEM(act_shape, BF16),
            pltpu.VMEM((d_model, d_ff), F32),
            pltpu.VMEM((SEG, 8, d_model), F32),
            pltpu.VMEM((SEG, 8, d_model), F32),
            pltpu.VMEM((8, d_model), F32),
            pltpu.VMEM((SEG, 8, d_model), F32),
            pltpu.VMEM((8, d_model), F32),
            sem((2,)), sem((N_CHUNKS,)), sem((N_CHUNKS,)),
            sem, sem((SEG,)), sem, sem((SEG,)), sem, sem,
            sem, sem, sem, sem((N_CHUNKS,)), sem, sem((N_CHUNKS,)), sem, sem((N_CHUNKS,)),
            sem, sem, sem, sem, sem, sem,
        ]
        any_spec = pl.BlockSpec(memory_space=pl.ANY)
        vmem_spec = pl.BlockSpec(memory_space=pltpu.VMEM)
        dw_up, dw_down, dgain, loss = pl.pallas_call(
            functools.partial(step_kernel, n_stages, loss_scale),
            out_shape=(jax.ShapeDtypeStruct(w_up.shape, F32), jax.ShapeDtypeStruct(w_down.shape, F32),
                       jax.ShapeDtypeStruct(norm_gain.shape, F32), jax.ShapeDtypeStruct((1,), F32)),
            in_specs=[any_spec, any_spec, any_spec, any_spec, vmem_spec],
            out_specs=(vmem_spec, vmem_spec, vmem_spec, pl.BlockSpec(memory_space=pltpu.SMEM)),
            scratch_shapes=scratch,
            compiler_params=pltpu.CompilerParams(collective_id=0, has_side_effects=True,
                                                 vmem_limit_bytes=67043328),
        )(x_in.reshape(n_rows, d_model), y_target.reshape(n_rows, d_model), w_up, w_down, norm_gain)
        return dw_up, dw_down, dgain, loss

    return jax.shard_map(stage_body, mesh=mesh,
                         in_specs=(P('dp'), P('dp'), P('stage'), P('stage'), P('stage')),
                         out_specs=(P(('dp', 'stage')), P(('dp', 'stage')), P(('dp', 'stage')), P('dp')),
                         check_vma=False)
```

```python
import functools

import jax
import jax.numpy as jnp
from jax import lax
from jax.experimental import pallas as pl
from jax.experimental.pallas import tpu as pltpu
from jax.sharding import PartitionSpec as P

NORM_EPS = 1e-6
SEG = 8
N_CHUNKS = 4
PIECES = 4
COLS = 256
HALF = SEG // 2
GROUP = 4
LATE_ROWS = 2
GELU_C = 0.7978845608028654
GELU_A = 0.044715
MESH = pl.DeviceIdType.MESH
F32 = jnp.float32
BF16 = jnp.bfloat16


def dot_nn(lhs, rhs):
    return lax.dot_general(lhs, rhs, (((1,), (0,)), ((), ())), preferred_element_type=F32)


def dot_nt(lhs, rhs):
    return lax.dot_general(lhs, rhs, (((1,), (1,)), ((), ())), preferred_element_type=F32)


def dot_tn(lhs, rhs):
    return lax.dot_general(lhs, rhs, (((0,), (0,)), ((), ())), preferred_element_type=F32)


def gelu_gate(hidden):
    sq = hidden * hidden
    gate = 0.5 + 0.5 * jnp.tanh(hidden * (GELU_C + (GELU_C * GELU_A) * sq))
    return gate, sq


def gelu_value(hidden):
    return hidden * gelu_gate(hidden)[0]


def gelu_slope(hidden, gate, sq):
    return gate + ((gate * (1.0 - gate)) * hidden) * (2.0 * GELU_C + (6.0 * GELU_C * GELU_A) * sq)


def inv_rms_of(x_float):
    return lax.rsqrt(jnp.mean(x_float * x_float, axis=-1, keepdims=True) + NORM_EPS)


def fold_rows(block):
    rows, cols = block.shape
    return jnp.sum(block.reshape(rows // 8, 8, cols), axis=0)


def step_kernel(n_stages, loss_scale,
                x_hbm, y_hbm, wu_hbm, wd_hbm, gain_ref,
                dwu_ref, dwd_ref, dgain_ref, loss_ref,
                wu, wd, gains, acts, grads, hiddens, act_stash, grad_stash, value_stash, slope_stash, targets, dwd_t,
                dg_part, dg_stash, loss_part, loss_stash, loss_total,
                load_sem, x_sem, y_sem, agu_send, agu_recv, agd_send, agd_recv, gain_send, gain_recv,
                as_send, as_recv, gs_send, gs_recv, fwd_send, fwd_recv, bwd_send, bwd_recv,
                dg_send, dg_recv, lrow_send, lrow_recv, lcol_send, lcol_recv):
    n_rows = n_stages // SEG
    n_chips = SEG // 2
    chunk = acts.shape[2]
    d_model = acts.shape[3]
    d_ff = wu.shape[2]
    me = lax.axis_index('stage')
    row = lax.div(me, SEG)
    r = lax.rem(me, SEG)
    chip = lax.div(r, 2)
    core = lax.rem(r, 2)
    row_base = row * SEG
    left = lax.rem(chip + n_chips - 1, n_chips) * 2 + core
    right = lax.rem(chip + 1, n_chips) * 2 + core
    across = lax.rem(chip + 2, n_chips) * 2 + core
    flip = 1 - 2 * core
    sib = r + flip

    def rcopy(src, dst, send_sem, recv_sem, dev):
        return pltpu.make_async_remote_copy(src_ref=src, dst_ref=dst, send_sem=send_sem, recv_sem=recv_sem,
                                            device_id={'stage': dev}, device_id_type=MESH)

    load_u = pltpu.make_async_copy(wu_hbm.at[0], wu.at[r], load_sem.at[0])
    load_d = pltpu.make_async_copy(wd_hbm.at[0], wd.at[r], load_sem.at[1])
    load_u.start()
    load_d.start()

    def x_load(k):
        first = pl.multiple_of((r * N_CHUNKS + k) * chunk, chunk)
        return pltpu.make_async_copy(x_hbm.at[pl.ds(first, chunk)], acts.at[0, k], x_sem.at[k])

    def y_load(k):
        first = pl.multiple_of((r * N_CHUNKS + k) * chunk, chunk)
        return pltpu.make_async_copy(y_hbm.at[pl.ds(first, chunk)], targets.at[k], y_sem.at[k])

    @pl.when(row == 0)
    def _():
        for k in range(N_CHUNKS):
            x_load(k).start()

    @pl.when(row == n_rows - 1)
    def _():
        for k in range(N_CHUNKS):
            y_load(k).start()

    gains[r] = jnp.broadcast_to(gain_ref[...], (8, d_model))
    dg_part[...] = jnp.zeros_like(dg_part)
    loss_part[...] = jnp.zeros_like(loss_part)

    with jax.named_scope('barrier'):
        barrier = pltpu.get_barrier_semaphore()
        for step in range(1, SEG):
            pl.semaphore_signal(barrier, inc=1, device_id={'stage': row_base + lax.rem(r + step, SEG)}, device_id_type=MESH)
        for step in range(1, n_rows):
            pl.semaphore_signal(barrier, inc=1, device_id={'stage': lax.rem(row + step, n_rows) * SEG + r}, device_id_type=MESH)
        pl.semaphore_wait(barrier, SEG - 1 + n_rows - 1)

    u_rows = d_model // PIECES
    d_rows = d_ff // PIECES

    def u_copy(slot, piece, dev):
        part = wu.at[slot, pl.ds(piece * u_rows, u_rows)]
        return rcopy(part, part, agu_send, agu_recv.at[slot, piece], row_base + dev)

    def d_copy(slot, piece, dev):
        part = wd.at[slot, pl.ds(piece * d_rows, d_rows)]
        return rcopy(part, part, agd_send, agd_recv.at[slot, piece], row_base + dev)

    with jax.named_scope('w_load_u'):
        load_u.wait()
    with jax.named_scope('w_load_d'):
        load_d.wait()
    for piece in range(PIECES):
        u_copy(r, piece, right).start()
        d_copy(r, piece, left).start()
    for piece in range(PIECES):
        d_copy(r, piece, right).start()
        u_copy(r, piece, left).start()
    for piece in range(PIECES):
        u_copy(r, piece, sib).start()
        d_copy(r, piece, sib).start()
    for step in range(1, SEG):
        rcopy(gains.at[r], gains.at[r], gain_send, gain_recv, row_base + lax.rem(r + step, SEG)).start()

    with jax.named_scope('ag_first'):
        for piece in range(PIECES):
            u_copy(left, piece, r).wait_recv()
            u_copy(left, piece, right).start()
            u_copy(left, piece, sib).start()
            d_copy(right, piece, r).wait_recv()
            d_copy(right, piece, left).start()
            d_copy(right, piece, sib).start()
    with jax.named_scope('ag_second'):
        for piece in range(PIECES):
            d_copy(left, piece, r).wait_recv()
            d_copy(left, piece, sib).start()
            u_copy(right, piece, r).wait_recv()
            u_copy(right, piece, sib).start()
    with jax.named_scope('ag_across'):
        for piece in range(PIECES):
            u_copy(across, piece, r).wait_recv()
            u_copy(across, piece, sib).start()
            d_copy(across, piece, r).wait_recv()
            d_copy(across, piece, sib).start()
    with jax.named_scope('ag_sib'):
        for slot in (sib, left + flip, right + flip, across + flip):
            for piece in range(PIECES):
                u_copy(slot, piece, r).wait_recv()
                d_copy(slot, piece, r).wait_recv()
    rcopy(gains.at[pl.ds(0, SEG - 1)], gains.at[pl.ds(0, SEG - 1)], gain_send, gain_recv, me).wait_recv()

    def act_ship(layer, k):
        mine = layer == r
        return rcopy(acts.at[layer, k], act_stash.at[k, jnp.where(mine, SEG, r)], as_send, as_recv,
                     row_base + jnp.where(mine, sib, layer))

    def grad_ship(layer, k):
        mine = layer == r
        return rcopy(grads.at[layer + 1, k], grad_stash.at[k, jnp.where(mine, SEG, r)], gs_send, gs_recv.at[k],
                     row_base + jnp.where(mine, sib, layer))

    def fwd_layer(layer, k):
        x_float = acts[layer, k].astype(F32)
        normed = (x_float * inv_rms_of(x_float) * gains[layer, 0:1, :]).astype(BF16)
        out = x_float
        for part in range(0, d_ff, COLS):
            cols = slice(part, part + COLS)
            hidden = dot_nn(normed, wu[layer, :, cols])
            hiddens[layer, k, :, cols] = hidden
            out += dot_nn(gelu_value(hidden).astype(BF16), wd[layer, cols, :])
        acts[layer + 1, k] = out.astype(BF16)

    def fwd_input_wait(k):
        @pl.when(row == 0)
        def _():
            x_load(k).wait()

        @pl.when(row > 0)
        def _():
            with jax.named_scope('fwd_wait'):
                rcopy(acts.at[0, k], acts.at[0, k], fwd_send, fwd_recv.at[k], me).wait_recv()

    def top_grad(k):
        y_load(k).wait()
        error_val = acts[SEG, k].astype(F32) - targets[k].astype(F32)
        loss_part[...] += fold_rows(error_val * error_val)
        grads[SEG, k] = ((2.0 * loss_scale) * error_val).astype(BF16)

    def fwd_group(group, k):
        for step in range(GROUP):
            fwd_layer(group * GROUP + step, k)
        return k

    def fwd_chunk(k, carry):
        fwd_input_wait(k)
        with jax.named_scope('fwd_layers'):
            lax.fori_loop(0, SEG // GROUP, fwd_group, k)

        @pl.when(row < n_rows - 1)
        def _():
            rcopy(acts.at[SEG, k], acts.at[0, k], fwd_send, fwd_recv.at[k], me + SEG).start()
        for layer in range(SEG):
            act_ship(layer, k).start()

        @pl.when(row == n_rows - 1)
        def _():
            top_grad(k)
        return carry

    lax.fori_loop(0, jnp.where(row == n_rows - 1, 1, N_CHUNKS), fwd_chunk, 0)

    def bwd_layer(step, k):
        layer = SEG - 1 - step
        grad_out = grads[layer + 1, k]
        x_float = acts[layer, k].astype(F32)
        inv_rms = inv_rms_of(x_float)
        x_hat = x_float * inv_rms
        gain = gains[layer, 0:1, :]
        grad_normed = 0.0
        for part in range(0, d_ff, COLS):
            cols = slice(part, part + COLS)
            hidden = hiddens[layer, k, :, cols]
            slope = gelu_slope(hidden, *gelu_gate(hidden))
            grad_gelu = dot_nt(grad_out, wd[layer, cols, :]).astype(BF16).astype(F32)
            grad_hidden = (grad_gelu * slope).astype(BF16)
            grad_normed += dot_nt(grad_hidden, wu[layer, :, cols])
        grad_normed = grad_normed.astype(BF16).astype(F32)
        dg_part[layer] += fold_rows(grad_normed * x_hat)
        grad_hat = grad_normed * gain
        mean_dot = jnp.mean(grad_hat * x_hat, axis=-1, keepdims=True)
        grad_x = inv_rms * (grad_hat - x_hat * mean_dot)
        grads[layer, k] = (grad_out.astype(F32) + grad_x).astype(BF16)

    def bwd_group(group, k):
        for step in range(GROUP):
            bwd_layer(group * GROUP + step, k)

        @pl.when((row > 0) & (group == SEG // GROUP - 1))
        def _():
            rcopy(grads.at[0, k], grads.at[SEG, k], bwd_send, bwd_recv.at[k], me - SEG).start()
        for step in range(GROUP):
            grad_ship(SEG - 1 - group * GROUP - step, k).start()
        return k

    def both_group(group, k):
        for step in range(GROUP):
            fwd_layer(group * GROUP + step, k)
            bwd_layer(group * GROUP + step, k - 1)

        @pl.when((row > 0) & (group == SEG // GROUP - 1))
        def _():
            rcopy(grads.at[0, k - 1], grads.at[SEG, k - 1], bwd_send, bwd_recv.at[k - 1], me - SEG).start()
        for step in range(GROUP):
            grad_ship(SEG - 1 - group * GROUP - step, k - 1).start()
        return k

    def both_chunks(k, carry):
        fwd_input_wait(k)
        with jax.named_scope('both_layers'):
            lax.fori_loop(0, SEG // GROUP, both_group, k)
        top_grad(k)
        for layer in range(SEG):
            act_ship(layer, k).start()
        return carry

    @pl.when(row == n_rows - 1)
    def _():
        lax.fori_loop(1, N_CHUNKS, both_chunks, 0)
        loss_stash[r] = loss_part[...]
        for step in range(1, SEG):
            rcopy(loss_stash.at[r], loss_stash.at[r], lrow_send, lrow_recv, row_base + lax.rem(r + step, SEG)).start()

    rest = act_stash.at[0, pl.ds(0, SEG)]
    all_rest = acts.at[pl.ds(0, SEG)]

    def owner_block(index):
        return lax.div(index, 2), pl.ds(lax.rem(index, 2) * HALF, HALF)

    def value_block(index, carry):
        k, srcs = owner_block(index)
        x_float = act_stash[k, srcs].reshape(HALF * chunk, d_model).astype(F32)
        normed = (x_float * inv_rms_of(x_float) * gains[r, 0:1, :]).astype(BF16)
        act_stash[k, srcs] = normed.reshape(HALF, chunk, d_model)
        for part in range(0, d_ff, COLS):
            cols = slice(part, part + COLS)
            hidden = dot_nn(normed, wu[r, :, cols])
            gate, sq = gelu_gate(hidden)
            value_stash[k, srcs, :, cols] = (hidden * gate).astype(BF16).reshape(HALF, chunk, COLS)
            slope_stash[k, srcs, :, cols] = gelu_slope(hidden, gate, sq).reshape(HALF, chunk, COLS)
        return carry

    def value_phase():
        with jax.named_scope('as_wait'):
            rcopy(all_rest, all_rest, as_send, as_recv, me).wait_recv()
        for k in range(N_CHUNKS):
            act_stash[k, r] = acts[r, k]
        dwu_ref[...] = jnp.zeros_like(dwu_ref)
        dwd_t[...] = jnp.zeros_like(dwd_t)
        with jax.named_scope('value_blocks'):
            lax.fori_loop(0, 2 * N_CHUNKS, value_block, 0)

    @pl.when(row < n_rows - LATE_ROWS)
    def _():
        value_phase()

    def weight_block(k, carry):
        rows = SEG * chunk
        with jax.named_scope('gs_wait'):
            rcopy(rest, rest, gs_send, gs_recv.at[k], me).wait_recv()
        grad_stash[k, r] = grads[r + 1, k]
        normed = act_stash[k, pl.ds(0, SEG)].reshape(rows, d_model)
        grad_out = grad_stash[k, pl.ds(0, SEG)].reshape(rows, d_model)
        for part in range(0, d_ff, COLS):
            cols = slice(part, part + COLS)
            grad_gelu = dot_nt(grad_out, wd[r, cols, :]).astype(BF16).astype(F32)
            grad_hidden = (grad_gelu * slope_stash[k, :, :, cols].reshape(rows, COLS)).astype(BF16)
            dwu_ref[0, :, cols] += dot_tn(normed, grad_hidden)
            dwd_t[:, cols] += dot_tn(grad_out, value_stash[k, :, :, cols].reshape(rows, COLS))
        return carry

    def bwd_chunk(k, carry):
        @pl.when(row < n_rows - 1)
        def _():
            with jax.named_scope('bwd_wait'):
                rcopy(grads.at[SEG, k], grads.at[SEG, k], bwd_send, bwd_recv.at[k], me).wait_recv()

        with jax.named_scope('bwd_layers'):
            lax.fori_loop(0, SEG // GROUP, bwd_group, k)

        @pl.when((row < n_rows - LATE_ROWS) & (k > 0) & (k < N_CHUNKS - 1))
        def _():
            weight_block(k - 1, 0)
        return carry

    lax.fori_loop(jnp.where(row == n_rows - 1, N_CHUNKS - 1, 0), N_CHUNKS, bwd_chunk, 0)

    def dg_ship(layer):
        return rcopy(dg_part.at[layer], dg_stash.at[r], dg_send, dg_recv, row_base + layer)

    for step in range(1, SEG):
        dg_ship(lax.rem(r + step, SEG)).start()
    dg_stash[r] = dg_part[r]

    @pl.when(row >= n_rows - LATE_ROWS)
    def _():
        value_phase()

    with jax.named_scope('weight_blocks'):
        lax.fori_loop(jnp.where(row < n_rows - LATE_ROWS, N_CHUNKS - 2, 0), N_CHUNKS, weight_block, 0)
    @pl.when(row == n_rows - 1)
    def _():
        rest_row = loss_stash.at[pl.ds(0, SEG - 1)]
        rcopy(rest_row, rest_row, lrow_send, lrow_recv, me).wait_recv()
        loss_total[...] = jnp.sum(loss_stash[...], axis=0)
        for step in range(1, n_rows):
            rcopy(loss_total, loss_total, lcol_send, lcol_recv, me - step * SEG).start()

    with jax.named_scope('turn'):
        dwd_ref[0] = dwd_t[...].T

    rest_dg = dg_stash.at[pl.ds(0, SEG - 1)]
    with jax.named_scope('dg_wait'):
        rcopy(rest_dg, rest_dg, dg_send, dg_recv, me).wait_recv()
    dgain_ref[...] = jnp.sum(jnp.sum(dg_stash[...], axis=0), axis=0, keepdims=True)

    @pl.when(row < n_rows - 1)
    def _():
        rcopy(loss_total, loss_total, lcol_send, lcol_recv, me).wait_recv()
    loss_ref[0] = jnp.sum(loss_total[...]) * loss_scale

    rest_u = wu.at[pl.ds(0, SEG - 1)]
    rest_d = wd.at[pl.ds(0, SEG - 1)]
    rcopy(rest_u, rest_u, agu_send, gain_recv, me).wait_send()
    rcopy(rest_d, rest_d, agd_send, gain_recv, me).wait_send()
    rest_gain = gains.at[pl.ds(0, SEG - 1)]
    rcopy(rest_gain, rest_gain, gain_send, gain_recv, me).wait_send()
    rcopy(all_rest, all_rest, as_send, dg_recv, me).wait_send()
    rcopy(all_rest, all_rest, gs_send, dg_recv, me).wait_send()
    rcopy(rest_dg, rest_dg, dg_send, dg_recv, me).wait_send()

    @pl.when(row < n_rows - 1)
    def _():
        rcopy(acts.at[0], acts.at[0], fwd_send, dg_recv, me).wait_send()

    @pl.when(row > 0)
    def _():
        rcopy(grads.at[0], grads.at[0], bwd_send, dg_recv, me).wait_send()

    @pl.when(row == n_rows - 1)
    def _():
        rest_row = loss_stash.at[pl.ds(0, SEG - 1)]
        rcopy(rest_row, rest_row, lrow_send, lrow_recv, me).wait_send()
        for step in range(1, n_rows):
            rcopy(loss_total, loss_total, lcol_send, lcol_recv, me).wait_send()


def solution(mesh):
    n_stages = mesh.shape['stage']

    def stage_body(x_in, y_target, w_up, w_down, norm_gain):
        n_micro, n_tok, d_model = x_in.shape
        d_ff = w_up.shape[2]
        n_rows = n_micro * n_tok
        chunk = n_rows // SEG // N_CHUNKS
        loss_scale = 1.0 / (n_rows * d_model)
        sem = pltpu.SemaphoreType.DMA
        act_shape = (N_CHUNKS, chunk, d_model)
        scratch = [
            pltpu.VMEM((SEG, d_model, d_ff), BF16),
            pltpu.VMEM((SEG, d_ff, d_model), BF16),
            pltpu.VMEM((SEG, 8, d_model), F32),
            pltpu.VMEM((SEG + 1,) + act_shape, BF16),
            pltpu.VMEM((SEG + 1,) + act_shape, BF16),
            pltpu.VMEM((SEG, N_CHUNKS, chunk, d_ff), F32),
            pltpu.VMEM((N_CHUNKS, SEG + 1, chunk, d_model), BF16),
            pltpu.VMEM((N_CHUNKS, SEG + 1, chunk, d_model), BF16),
            pltpu.VMEM((N_CHUNKS, SEG, chunk, d_ff), BF16),
            pltpu.VMEM((N_CHUNKS, SEG, chunk, d_ff), F32),
            pltpu.VMEM(act_shape, BF16),
            pltpu.VMEM((d_model, d_ff), F32),
            pltpu.VMEM((SEG, 8, d_model), F32),
            pltpu.VMEM((SEG, 8, d_model), F32),
            pltpu.VMEM((8, d_model), F32),
            pltpu.VMEM((SEG, 8, d_model), F32),
            pltpu.VMEM((8, d_model), F32),
            sem((2,)), sem((N_CHUNKS,)), sem((N_CHUNKS,)),
            sem, sem((SEG, PIECES)), sem, sem((SEG, PIECES)), sem, sem,
            sem, sem, sem, sem((N_CHUNKS,)), sem, sem((N_CHUNKS,)), sem, sem((N_CHUNKS,)),
            sem, sem, sem, sem, sem, sem,
        ]
        any_spec = pl.BlockSpec(memory_space=pl.ANY)
        vmem_spec = pl.BlockSpec(memory_space=pltpu.VMEM)
        dw_up, dw_down, dgain, loss = pl.pallas_call(
            functools.partial(step_kernel, n_stages, loss_scale),
            out_shape=(jax.ShapeDtypeStruct(w_up.shape, F32), jax.ShapeDtypeStruct(w_down.shape, F32),
                       jax.ShapeDtypeStruct(norm_gain.shape, F32), jax.ShapeDtypeStruct((1,), F32)),
            in_specs=[any_spec, any_spec, any_spec, any_spec, vmem_spec],
            out_specs=(vmem_spec, vmem_spec, vmem_spec, pl.BlockSpec(memory_space=pltpu.SMEM)),
            scratch_shapes=scratch,
            compiler_params=pltpu.CompilerParams(collective_id=0, has_side_effects=True,
                                                 vmem_limit_bytes=67043328),
        )(x_in.reshape(n_rows, d_model), y_target.reshape(n_rows, d_model), w_up, w_down, norm_gain)
        return dw_up, dw_down, dgain, loss

    return jax.shard_map(stage_body, mesh=mesh,
                         in_specs=(P('dp'), P('dp'), P('stage'), P('stage'), P('stage')),
                         out_specs=(P(('dp', 'stage')), P(('dp', 'stage')), P(('dp', 'stage')), P('dp')),
                         check_vma=False)
```

```python
import functools

import jax
import jax.numpy as jnp
from jax import lax
from jax.experimental import pallas as pl
from jax.experimental.pallas import tpu as pltpu
from jax.sharding import PartitionSpec as P

NORM_EPS = 1e-6
SEG = 8
N_CHUNKS = 4
PIECES = 4
COLS = 256
HALF = SEG // 2
GROUP = 4
LATE_ROWS = 2
GELU_C = 0.7978845608028654
GELU_A = 0.044715
MESH = pl.DeviceIdType.MESH
F32 = jnp.float32
BF16 = jnp.bfloat16


def dot_nn(lhs, rhs):
    return lax.dot_general(lhs, rhs, (((1,), (0,)), ((), ())), preferred_element_type=F32)


def dot_nt(lhs, rhs):
    return lax.dot_general(lhs, rhs, (((1,), (1,)), ((), ())), preferred_element_type=F32)


def dot_tn(lhs, rhs):
    return lax.dot_general(lhs, rhs, (((0,), (0,)), ((), ())), preferred_element_type=F32)


def gelu_gate(hidden):
    sq = hidden * hidden
    gate = 0.5 + 0.5 * jnp.tanh(hidden * (GELU_C + (GELU_C * GELU_A) * sq))
    return gate, sq


def gelu_value(hidden):
    return hidden * gelu_gate(hidden)[0]


def gelu_slope(hidden, gate, sq):
    return gate + ((gate * (1.0 - gate)) * hidden) * (2.0 * GELU_C + (6.0 * GELU_C * GELU_A) * sq)


def inv_rms_of(x_float):
    return lax.rsqrt(jnp.mean(x_float * x_float, axis=-1, keepdims=True) + NORM_EPS)


def fold_rows(block):
    rows, cols = block.shape
    return jnp.sum(block.reshape(rows // 8, 8, cols), axis=0)


def step_kernel(n_stages, loss_scale,
                x_hbm, y_hbm, wu_hbm, wd_hbm, gain_ref,
                dwu_ref, dwd_ref, dgain_ref, loss_ref,
                wu, wd, gains, acts, grads, hiddens, act_stash, grad_stash, value_stash, slope_stash, targets, dwd_t,
                dg_part, dg_stash, loss_part, loss_stash, loss_total,
                load_sem, x_sem, y_sem, agu_send, agu_recv, agd_send, agd_recv, gain_send, gain_recv,
                as_send, as_recv, gs_send, gs_recv, fwd_send, fwd_recv, bwd_send, bwd_recv,
                dg_send, dg_recv, lrow_send, lrow_recv, lcol_send, lcol_recv):
    n_rows = n_stages // SEG
    n_chips = SEG // 2
    chunk = acts.shape[2]
    d_model = acts.shape[3]
    d_ff = wu.shape[2]
    me = lax.axis_index('stage')
    row = lax.div(me, SEG)
    r = lax.rem(me, SEG)
    chip = lax.div(r, 2)
    core = lax.rem(r, 2)
    row_base = row * SEG
    left = lax.rem(chip + n_chips - 1, n_chips) * 2 + core
    right = lax.rem(chip + 1, n_chips) * 2 + core
    across = lax.rem(chip + 2, n_chips) * 2 + core
    flip = 1 - 2 * core
    sib = r + flip

    def rcopy(src, dst, send_sem, recv_sem, dev):
        return pltpu.make_async_remote_copy(src_ref=src, dst_ref=dst, send_sem=send_sem, recv_sem=recv_sem,
                                            device_id={'stage': dev}, device_id_type=MESH)

    load_u = pltpu.make_async_copy(wu_hbm.at[0], wu.at[r], load_sem.at[0])
    load_d = pltpu.make_async_copy(wd_hbm.at[0], wd.at[r], load_sem.at[1])
    load_u.start()
    load_d.start()

    def x_load(k):
        first = pl.multiple_of((r * N_CHUNKS + k) * chunk, chunk)
        return pltpu.make_async_copy(x_hbm.at[pl.ds(first, chunk)], acts.at[0, k], x_sem.at[k])

    def y_load(k):
        first = pl.multiple_of((r * N_CHUNKS + k) * chunk, chunk)
        return pltpu.make_async_copy(y_hbm.at[pl.ds(first, chunk)], targets.at[k], y_sem.at[k])

    @pl.when(row == 0)
    def _():
        for k in range(N_CHUNKS):
            x_load(k).start()

    @pl.when(row == n_rows - 1)
    def _():
        for k in range(N_CHUNKS):
            y_load(k).start()

    gains[r] = jnp.broadcast_to(gain_ref[...], (8, d_model))
    dg_part[...] = jnp.zeros_like(dg_part)
    loss_part[...] = jnp.zeros_like(loss_part)

    with jax.named_scope('barrier'):
        barrier = pltpu.get_barrier_semaphore()
        for step in range(1, SEG):
            pl.semaphore_signal(barrier, inc=1, device_id={'stage': row_base + lax.rem(r + step, SEG)}, device_id_type=MESH)
        for step in range(1, n_rows):
            pl.semaphore_signal(barrier, inc=1, device_id={'stage': lax.rem(row + step, n_rows) * SEG + r}, device_id_type=MESH)
        pl.semaphore_wait(barrier, SEG - 1 + n_rows - 1)

    u_rows = d_model // PIECES
    d_rows = d_ff // PIECES

    def u_copy(slot, piece, dev):
        part = wu.at[slot, pl.ds(piece * u_rows, u_rows)]
        return rcopy(part, part, agu_send, agu_recv.at[slot, piece], row_base + dev)

    def d_copy(slot, piece, dev):
        part = wd.at[slot, pl.ds(piece * d_rows, d_rows)]
        return rcopy(part, part, agd_send, agd_recv.at[slot, piece], row_base + dev)

    with jax.named_scope('w_load_u'):
        load_u.wait()
    with jax.named_scope('w_load_d'):
        load_d.wait()
    for piece in range(PIECES):
        u_copy(r, piece, right).start()
        d_copy(r, piece, left).start()
    for piece in range(PIECES):
        d_copy(r, piece, right).start()
        u_copy(r, piece, left).start()
    for piece in range(PIECES):
        u_copy(r, piece, sib).start()
        d_copy(r, piece, sib).start()
    for step in range(1, SEG):
        rcopy(gains.at[r], gains.at[r], gain_send, gain_recv, row_base + lax.rem(r + step, SEG)).start()

    with jax.named_scope('ag_first'):
        for piece in range(PIECES):
            u_copy(left, piece, r).wait_recv()
            u_copy(left, piece, right).start()
            u_copy(left, piece, sib).start()
            d_copy(right, piece, r).wait_recv()
            d_copy(right, piece, left).start()
            d_copy(right, piece, sib).start()
    with jax.named_scope('ag_second'):
        for piece in range(PIECES):
            d_copy(left, piece, r).wait_recv()
            d_copy(left, piece, sib).start()
            u_copy(right, piece, r).wait_recv()
            u_copy(right, piece, sib).start()
    with jax.named_scope('ag_across'):
        for piece in range(PIECES):
            u_copy(across, piece, r).wait_recv()
            u_copy(across, piece, sib).start()
            d_copy(across, piece, r).wait_recv()
            d_copy(across, piece, sib).start()
    with jax.named_scope('ag_sib'):
        for slot in (sib, left + flip, right + flip, across + flip):
            for piece in range(PIECES):
                u_copy(slot, piece, r).wait_recv()
                d_copy(slot, piece, r).wait_recv()
    rcopy(gains.at[pl.ds(0, SEG - 1)], gains.at[pl.ds(0, SEG - 1)], gain_send, gain_recv, me).wait_recv()

    def act_ship(layer, k):
        mine = layer == r
        return rcopy(acts.at[layer, k], act_stash.at[k, jnp.where(mine, SEG, r)], as_send, as_recv.at[k],
                     row_base + jnp.where(mine, sib, layer))

    def grad_ship(layer, k):
        mine = layer == r
        return rcopy(grads.at[layer + 1, k], grad_stash.at[k, jnp.where(mine, SEG, r)], gs_send, gs_recv.at[k],
                     row_base + jnp.where(mine, sib, layer))

    def fwd_layer(layer, k):
        x_float = acts[layer, k].astype(F32)
        normed = (x_float * inv_rms_of(x_float) * gains[layer, 0:1, :]).astype(BF16)
        out = x_float
        for part in range(0, d_ff, COLS):
            cols = slice(part, part + COLS)
            hidden = dot_nn(normed, wu[layer, :, cols])
            hiddens[layer, k, :, cols] = hidden
            out += dot_nn(gelu_value(hidden).astype(BF16), wd[layer, cols, :])
        acts[layer + 1, k] = out.astype(BF16)

    def fwd_input_wait(k):
        @pl.when(row == 0)
        def _():
            x_load(k).wait()

        @pl.when(row > 0)
        def _():
            with jax.named_scope('fwd_wait'):
                rcopy(acts.at[0, k], acts.at[0, k], fwd_send, fwd_recv.at[k], me).wait_recv()

    def top_grad(k):
        y_load(k).wait()
        error_val = acts[SEG, k].astype(F32) - targets[k].astype(F32)
        loss_part[...] += fold_rows(error_val * error_val)
        grads[SEG, k] = ((2.0 * loss_scale) * error_val).astype(BF16)

    def fwd_group(group, k):
        for step in range(GROUP):
            fwd_layer(group * GROUP + step, k)
        return k

    def fwd_chunk(k, carry):
        fwd_input_wait(k)
        with jax.named_scope('fwd_layers'):
            lax.fori_loop(0, SEG // GROUP, fwd_group, k)

        @pl.when(row < n_rows - 1)
        def _():
            rcopy(acts.at[SEG, k], acts.at[0, k], fwd_send, fwd_recv.at[k], me + SEG).start()
        for layer in range(SEG):
            act_ship(layer, k).start()

        @pl.when(row == n_rows - 1)
        def _():
            top_grad(k)
        return carry

    lax.fori_loop(0, jnp.where(row == n_rows - 1, 1, N_CHUNKS), fwd_chunk, 0)

    def bwd_layer(step, k):
        layer = SEG - 1 - step
        grad_out = grads[layer + 1, k]
        x_float = acts[layer, k].astype(F32)
        inv_rms = inv_rms_of(x_float)
        x_hat = x_float * inv_rms
        gain = gains[layer, 0:1, :]
        grad_normed = 0.0
        for part in range(0, d_ff, COLS):
            cols = slice(part, part + COLS)
            hidden = hiddens[layer, k, :, cols]
            slope = gelu_slope(hidden, *gelu_gate(hidden))
            grad_gelu = dot_nt(grad_out, wd[layer, cols, :]).astype(BF16).astype(F32)
            grad_hidden = (grad_gelu * slope).astype(BF16)
            grad_normed += dot_nt(grad_hidden, wu[layer, :, cols])
        grad_normed = grad_normed.astype(BF16).astype(F32)
        dg_part[layer] += fold_rows(grad_normed * x_hat)
        grad_hat = grad_normed * gain
        mean_dot = jnp.mean(grad_hat * x_hat, axis=-1, keepdims=True)
        grad_x = inv_rms * (grad_hat - x_hat * mean_dot)
        grads[layer, k] = (grad_out.astype(F32) + grad_x).astype(BF16)

    def bwd_group(group, k):
        for step in range(GROUP):
            bwd_layer(group * GROUP + step, k)

        @pl.when((row > 0) & (group == SEG // GROUP - 1))
        def _():
            rcopy(grads.at[0, k], grads.at[SEG, k], bwd_send, bwd_recv.at[k], me - SEG).start()
        for step in range(GROUP):
            grad_ship(SEG - 1 - group * GROUP - step, k).start()
        return k

    def both_group(group, k):
        for step in range(GROUP):
            fwd_layer(group * GROUP + step, k)
            bwd_layer(group * GROUP + step, k - 1)

        @pl.when((row > 0) & (group == SEG // GROUP - 1))
        def _():
            rcopy(grads.at[0, k - 1], grads.at[SEG, k - 1], bwd_send, bwd_recv.at[k - 1], me - SEG).start()
        for step in range(GROUP):
            grad_ship(SEG - 1 - group * GROUP - step, k - 1).start()
        return k

    def both_chunks(k, carry):
        fwd_input_wait(k)
        with jax.named_scope('both_layers'):
            lax.fori_loop(0, SEG // GROUP, both_group, k)
        top_grad(k)
        for layer in range(SEG):
            act_ship(layer, k).start()
        return carry

    @pl.when(row == n_rows - 1)
    def _():
        lax.fori_loop(1, N_CHUNKS, both_chunks, 0)
        loss_stash[r] = loss_part[...]
        for step in range(1, SEG):
            rcopy(loss_stash.at[r], loss_stash.at[r], lrow_send, lrow_recv, row_base + lax.rem(r + step, SEG)).start()

    rest = act_stash.at[0, pl.ds(0, SEG)]
    all_rest = acts.at[pl.ds(0, SEG)]

    def owner_block(index):
        return lax.div(index, 2), pl.ds(lax.rem(index, 2) * HALF, HALF)

    def value_block(index, carry):
        k, srcs = owner_block(index)

        @pl.when(lax.rem(index, 2) == 0)
        def _():
            with jax.named_scope('as_wait'):
                rcopy(rest, rest, as_send, as_recv.at[k], me).wait_recv()
            act_stash[k, r] = acts[r, k]
        x_float = act_stash[k, srcs].reshape(HALF * chunk, d_model).astype(F32)
        normed = (x_float * inv_rms_of(x_float) * gains[r, 0:1, :]).astype(BF16)
        act_stash[k, srcs] = normed.reshape(HALF, chunk, d_model)
        for part in range(0, d_ff, COLS):
            cols = slice(part, part + COLS)
            hidden = dot_nn(normed, wu[r, :, cols])
            gate, sq = gelu_gate(hidden)
            value_stash[k, srcs, :, cols] = (hidden * gate).astype(BF16).reshape(HALF, chunk, COLS)
            slope_stash[k, srcs, :, cols] = gelu_slope(hidden, gate, sq).reshape(HALF, chunk, COLS)
        return carry

    def value_phase():
        dwu_ref[...] = jnp.zeros_like(dwu_ref)
        dwd_t[...] = jnp.zeros_like(dwd_t)
        with jax.named_scope('value_blocks'):
            lax.fori_loop(0, 2 * N_CHUNKS, value_block, 0)

    @pl.when(row < n_rows - LATE_ROWS)
    def _():
        value_phase()

    def weight_block(k, carry):
        rows = SEG * chunk
        with jax.named_scope('gs_wait'):
            rcopy(rest, rest, gs_send, gs_recv.at[k], me).wait_recv()
        grad_stash[k, r] = grads[r + 1, k]
        normed = act_stash[k, pl.ds(0, SEG)].reshape(rows, d_model)
        grad_out = grad_stash[k, pl.ds(0, SEG)].reshape(rows, d_model)
        for part in range(0, d_ff, COLS):
            cols = slice(part, part + COLS)
            grad_gelu = dot_nt(grad_out, wd[r, cols, :]).astype(BF16).astype(F32)
            grad_hidden = (grad_gelu * slope_stash[k, :, :, cols].reshape(rows, COLS)).astype(BF16)
            dwu_ref[0, :, cols] += dot_tn(normed, grad_hidden)
            dwd_t[:, cols] += dot_tn(grad_out, value_stash[k, :, :, cols].reshape(rows, COLS))
        return carry

    def bwd_chunk(k, carry):
        @pl.when(row < n_rows - 1)
        def _():
            with jax.named_scope('bwd_wait'):
                rcopy(grads.at[SEG, k], grads.at[SEG, k], bwd_send, bwd_recv.at[k], me).wait_recv()

        with jax.named_scope('bwd_layers'):
            lax.fori_loop(0, SEG // GROUP, bwd_group, k)
        return carry

    lax.fori_loop(jnp.where(row == n_rows - 1, N_CHUNKS - 1, 0), N_CHUNKS, bwd_chunk, 0)

    def dg_ship(layer):
        return rcopy(dg_part.at[layer], dg_stash.at[r], dg_send, dg_recv, row_base + layer)

    for step in range(1, SEG):
        dg_ship(lax.rem(r + step, SEG)).start()
    dg_stash[r] = dg_part[r]

    @pl.when(row >= n_rows - LATE_ROWS)
    def _():
        value_phase()

    with jax.named_scope('weight_blocks'):
        lax.fori_loop(0, N_CHUNKS, weight_block, 0)
    @pl.when(row == n_rows - 1)
    def _():
        rest_row = loss_stash.at[pl.ds(0, SEG - 1)]
        rcopy(rest_row, rest_row, lrow_send, lrow_recv, me).wait_recv()
        loss_total[...] = jnp.sum(loss_stash[...], axis=0)
        for step in range(1, n_rows):
            rcopy(loss_total, loss_total, lcol_send, lcol_recv, me - step * SEG).start()

    with jax.named_scope('turn'):
        dwd_ref[0] = dwd_t[...].T

    rest_dg = dg_stash.at[pl.ds(0, SEG - 1)]
    with jax.named_scope('dg_wait'):
        rcopy(rest_dg, rest_dg, dg_send, dg_recv, me).wait_recv()
    dgain_ref[...] = jnp.sum(jnp.sum(dg_stash[...], axis=0), axis=0, keepdims=True)

    @pl.when(row < n_rows - 1)
    def _():
        rcopy(loss_total, loss_total, lcol_send, lcol_recv, me).wait_recv()
    loss_ref[0] = jnp.sum(loss_total[...]) * loss_scale

    rest_u = wu.at[pl.ds(0, SEG - 1)]
    rest_d = wd.at[pl.ds(0, SEG - 1)]
    rcopy(rest_u, rest_u, agu_send, gain_recv, me).wait_send()
    rcopy(rest_d, rest_d, agd_send, gain_recv, me).wait_send()
    rest_gain = gains.at[pl.ds(0, SEG - 1)]
    rcopy(rest_gain, rest_gain, gain_send, gain_recv, me).wait_send()
    rcopy(all_rest, all_rest, as_send, dg_recv, me).wait_send()
    rcopy(all_rest, all_rest, gs_send, dg_recv, me).wait_send()
    rcopy(rest_dg, rest_dg, dg_send, dg_recv, me).wait_send()

    @pl.when(row < n_rows - 1)
    def _():
        rcopy(acts.at[0], acts.at[0], fwd_send, dg_recv, me).wait_send()

    @pl.when(row > 0)
    def _():
        rcopy(grads.at[0], grads.at[0], bwd_send, dg_recv, me).wait_send()

    @pl.when(row == n_rows - 1)
    def _():
        rest_row = loss_stash.at[pl.ds(0, SEG - 1)]
        rcopy(rest_row, rest_row, lrow_send, lrow_recv, me).wait_send()
        for step in range(1, n_rows):
            rcopy(loss_total, loss_total, lcol_send, lcol_recv, me).wait_send()


def solution(mesh):
    n_stages = mesh.shape['stage']

    def stage_body(x_in, y_target, w_up, w_down, norm_gain):
        n_micro, n_tok, d_model = x_in.shape
        d_ff = w_up.shape[2]
        n_rows = n_micro * n_tok
        chunk = n_rows // SEG // N_CHUNKS
        loss_scale = 1.0 / (n_rows * d_model)
        sem = pltpu.SemaphoreType.DMA
        act_shape = (N_CHUNKS, chunk, d_model)
        scratch = [
            pltpu.VMEM((SEG, d_model, d_ff), BF16),
            pltpu.VMEM((SEG, d_ff, d_model), BF16),
            pltpu.VMEM((SEG, 8, d_model), F32),
            pltpu.VMEM((SEG + 1,) + act_shape, BF16),
            pltpu.VMEM((SEG + 1,) + act_shape, BF16),
            pltpu.VMEM((SEG, N_CHUNKS, chunk, d_ff), F32),
            pltpu.VMEM((N_CHUNKS, SEG + 1, chunk, d_model), BF16),
            pltpu.VMEM((N_CHUNKS, SEG + 1, chunk, d_model), BF16),
            pltpu.VMEM((N_CHUNKS, SEG, chunk, d_ff), BF16),
            pltpu.VMEM((N_CHUNKS, SEG, chunk, d_ff), F32),
            pltpu.VMEM(act_shape, BF16),
            pltpu.VMEM((d_model, d_ff), F32),
            pltpu.VMEM((SEG, 8, d_model), F32),
            pltpu.VMEM((SEG, 8, d_model), F32),
            pltpu.VMEM((8, d_model), F32),
            pltpu.VMEM((SEG, 8, d_model), F32),
            pltpu.VMEM((8, d_model), F32),
            sem((2,)), sem((N_CHUNKS,)), sem((N_CHUNKS,)),
            sem, sem((SEG, PIECES)), sem, sem((SEG, PIECES)), sem, sem,
            sem, sem((N_CHUNKS,)), sem, sem((N_CHUNKS,)), sem, sem((N_CHUNKS,)), sem, sem((N_CHUNKS,)),
            sem, sem, sem, sem, sem, sem,
        ]
        any_spec = pl.BlockSpec(memory_space=pl.ANY)
        vmem_spec = pl.BlockSpec(memory_space=pltpu.VMEM)
        dw_up, dw_down, dgain, loss = pl.pallas_call(
            functools.partial(step_kernel, n_stages, loss_scale),
            out_shape=(jax.ShapeDtypeStruct(w_up.shape, F32), jax.ShapeDtypeStruct(w_down.shape, F32),
                       jax.ShapeDtypeStruct(norm_gain.shape, F32), jax.ShapeDtypeStruct((1,), F32)),
            in_specs=[any_spec, any_spec, any_spec, any_spec, vmem_spec],
            out_specs=(vmem_spec, vmem_spec, vmem_spec, pl.BlockSpec(memory_space=pltpu.SMEM)),
            scratch_shapes=scratch,
            compiler_params=pltpu.CompilerParams(collective_id=0, has_side_effects=True,
                                                 vmem_limit_bytes=67043328),
        )(x_in.reshape(n_rows, d_model), y_target.reshape(n_rows, d_model), w_up, w_down, norm_gain)
        return dw_up, dw_down, dgain, loss

    return jax.shard_map(stage_body, mesh=mesh,
                         in_specs=(P('dp'), P('dp'), P('stage'), P('stage'), P('stage')),
                         out_specs=(P(('dp', 'stage')), P(('dp', 'stage')), P(('dp', 'stage')), P('dp')),
                         check_vma=False)
```

```python
import functools

import jax
import jax.numpy as jnp
from jax import lax
from jax.experimental import pallas as pl
from jax.experimental.pallas import tpu as pltpu
from jax.sharding import PartitionSpec as P

NORM_EPS = 1e-6
SEG = 8
N_CHUNKS = 4
PIECES = 8
HELP = 2
COLS = 256
HALF = SEG // 2
GROUP = 4
LATE_ROWS = 2
WRITE_PARTS = 4
GELU_C = 0.7978845608028654
GELU_A = 0.044715
MESH = pl.DeviceIdType.MESH
F32 = jnp.float32
BF16 = jnp.bfloat16


def dot_nn(lhs, rhs):
    return lax.dot_general(lhs, rhs, (((1,), (0,)), ((), ())), preferred_element_type=F32)


def dot_nt(lhs, rhs):
    return lax.dot_general(lhs, rhs, (((1,), (1,)), ((), ())), preferred_element_type=F32)


def dot_tn(lhs, rhs):
    return lax.dot_general(lhs, rhs, (((0,), (0,)), ((), ())), preferred_element_type=F32)


def gelu_gate(hidden):
    sq = hidden * hidden
    gate = 0.5 + 0.5 * jnp.tanh(hidden * (GELU_C + (GELU_C * GELU_A) * sq))
    return gate, sq


def gelu_value(hidden):
    return hidden * gelu_gate(hidden)[0]


def gelu_slope(hidden, gate, sq):
    return gate + ((gate * (1.0 - gate)) * hidden) * (2.0 * GELU_C + (6.0 * GELU_C * GELU_A) * sq)


def inv_rms_of(x_float):
    return lax.rsqrt(jnp.mean(x_float * x_float, axis=-1, keepdims=True) + NORM_EPS)


def fold_rows(block):
    rows, cols = block.shape
    return jnp.sum(block.reshape(rows // 8, 8, cols), axis=0)


def step_kernel(n_stages, loss_scale,
                x_hbm, y_hbm, wu_hbm, wd_hbm, gain_ref,
                dwu_ref, dwd_ref, dgain_ref, loss_ref,
                wu, wd, help_u, help_d, gains, acts, grads, hiddens, act_stash, grad_stash, value_stash, slope_stash, targets, dwd_t,
                dg_part, dg_stash, loss_part, loss_stash, loss_total,
                load_sem, x_sem, y_sem, agu_send, agu_recv, agd_send, agd_recv, hu_send, hu_recv, hd_send, hd_recv, gain_send, gain_recv,
                as_send, as_recv, gs_send, gs_recv, fwd_send, fwd_recv, bwd_send, bwd_recv,
                dg_send, dg_recv, lrow_send, lrow_recv, lcol_send, lcol_recv):
    n_rows = n_stages // SEG
    n_chips = SEG // 2
    chunk = acts.shape[2]
    d_model = acts.shape[3]
    d_ff = wu.shape[2]
    me = lax.axis_index('stage')
    row = lax.div(me, SEG)
    r = lax.rem(me, SEG)
    chip = lax.div(r, 2)
    core = lax.rem(r, 2)
    row_base = row * SEG
    left = lax.rem(chip + n_chips - 1, n_chips) * 2 + core
    right = lax.rem(chip + 1, n_chips) * 2 + core
    across = lax.rem(chip + 2, n_chips) * 2 + core
    flip = 1 - 2 * core
    sib = r + flip

    def rcopy(src, dst, send_sem, recv_sem, dev):
        return pltpu.make_async_remote_copy(src_ref=src, dst_ref=dst, send_sem=send_sem, recv_sem=recv_sem,
                                            device_id={'stage': dev}, device_id_type=MESH)

    load_u = pltpu.make_async_copy(wu_hbm.at[0], wu.at[r], load_sem.at[0])
    load_d = pltpu.make_async_copy(wd_hbm.at[0], wd.at[r], load_sem.at[1])
    load_u.start()
    load_d.start()

    def x_load(k):
        first = pl.multiple_of((r * N_CHUNKS + k) * chunk, chunk)
        return pltpu.make_async_copy(x_hbm.at[pl.ds(first, chunk)], acts.at[0, k], x_sem.at[k])

    def y_load(k):
        first = pl.multiple_of((r * N_CHUNKS + k) * chunk, chunk)
        return pltpu.make_async_copy(y_hbm.at[pl.ds(first, chunk)], targets.at[k], y_sem.at[k])

    @pl.when(row == 0)
    def _():
        for k in range(N_CHUNKS):
            x_load(k).start()

    @pl.when(row == n_rows - 1)
    def _():
        for k in range(N_CHUNKS):
            y_load(k).start()

    gains[r] = jnp.broadcast_to(gain_ref[...], (8, d_model))
    dg_part[...] = jnp.zeros_like(dg_part)
    loss_part[...] = jnp.zeros_like(loss_part)

    with jax.named_scope('barrier'):
        barrier = pltpu.get_barrier_semaphore()
        for step in range(1, SEG):
            pl.semaphore_signal(barrier, inc=1, device_id={'stage': row_base + lax.rem(r + step, SEG)}, device_id_type=MESH)
        for step in range(1, n_rows):
            pl.semaphore_signal(barrier, inc=1, device_id={'stage': lax.rem(row + step, n_rows) * SEG + r}, device_id_type=MESH)
        pl.semaphore_wait(barrier, SEG - 1 + n_rows - 1)

    u_rows = d_model // PIECES
    d_rows = d_ff // PIECES
    helped = row < n_rows // 2
    partner = (n_rows - 1 - row) * SEG + r
    n_help = jnp.where((row == 0) | (row == n_rows - 1), HELP, HELP - 1)
    n_direct = PIECES - n_help
    n_ring = jnp.where(helped, n_direct, PIECES)
    chip_left, chip_right, chip_across = lax.div(left, 2), lax.div(right, 2), lax.div(across, 2)

    def each_piece(first, last, fn):
        def body(piece, carry):
            fn(piece)
            return carry
        lax.fori_loop(first, last, body, 0)

    def u_part(slot, piece):
        return wu.at[slot, pl.ds(pl.multiple_of(piece * u_rows, u_rows), u_rows)]

    def d_part(slot, piece):
        return wd.at[slot, pl.ds(pl.multiple_of(piece * d_rows, d_rows), d_rows)]

    def u_copy(slot, piece, dev):
        part = u_part(slot, piece)
        return rcopy(part, part, agu_send, agu_recv.at[slot, piece], row_base + dev)

    def d_copy(slot, piece, dev):
        part = d_part(slot, piece)
        return rcopy(part, part, agd_send, agd_recv.at[slot, piece], row_base + dev)

    def hu_copy(place, piece, dev):
        part = help_u.at[place, piece]
        return rcopy(part, part, hu_send, hu_recv.at[place, piece], row_base + dev)

    def hd_copy(place, piece, dev):
        part = help_d.at[place, piece]
        return rcopy(part, part, hd_send, hd_recv.at[place, piece], row_base + dev)

    def hu_give(piece):
        rcopy(u_part(r, n_direct + piece), help_u.at[chip, piece], agu_send, hu_recv.at[chip, piece], partner).start()

    def hd_give(piece):
        rcopy(d_part(r, n_direct + piece), help_d.at[chip, piece], agd_send, hd_recv.at[chip, piece], partner).start()

    def hu_return(place, piece):
        slot = place * 2 + core
        rcopy(help_u.at[place, piece], u_part(slot, n_direct + piece), hu_send, agu_recv.at[slot, n_direct + piece], partner).start()

    def hd_return(place, piece):
        slot = place * 2 + core
        rcopy(help_d.at[place, piece], d_part(slot, n_direct + piece), hd_send, agd_recv.at[slot, n_direct + piece], partner).start()

    with jax.named_scope('w_load_u'):
        load_u.wait()
    with jax.named_scope('w_load_d'):
        load_d.wait()
    def ring_first(piece):
        u_copy(r, piece, right).start()
        d_copy(r, piece, left).start()

    def ring_second(piece):
        d_copy(r, piece, right).start()
        u_copy(r, piece, left).start()

    def give(piece):
        hu_give(piece)
        hd_give(piece)

    @pl.when(helped)
    def _():
        each_piece(0, n_help, give)
        each_piece(0, n_direct, ring_first)
        each_piece(0, n_direct, ring_second)

    @pl.when(jnp.logical_not(helped))
    def _():
        each_piece(0, PIECES // 2, ring_first)

    def own_to_sib(piece):
        u_copy(r, piece, sib).start()
        d_copy(r, piece, sib).start()
    each_piece(0, PIECES, own_to_sib)
    for step in range(1, SEG):
        rcopy(gains.at[r], gains.at[r], gain_send, gain_recv, row_base + lax.rem(r + step, SEG)).start()

    @pl.when(jnp.logical_not(helped))
    def _():
        def spread(piece):
            hu_copy(chip, piece, r).wait_recv()
            hu_copy(chip, piece, right).start()
            hu_copy(chip, piece, left).start()
            hd_copy(chip, piece, r).wait_recv()
            hd_copy(chip, piece, left).start()
            hd_copy(chip, piece, right).start()

        def relay(piece):
            hu_copy(chip_left, piece, r).wait_recv()
            hu_copy(chip_left, piece, right).start()
            hu_return(chip_left, piece)
            hd_copy(chip_right, piece, r).wait_recv()
            hd_copy(chip_right, piece, left).start()
            hd_return(chip_right, piece)

        def near(piece):
            hd_copy(chip_left, piece, r).wait_recv()
            hd_return(chip_left, piece)
            hu_copy(chip_right, piece, r).wait_recv()
            hu_return(chip_right, piece)

        def far(piece):
            hu_copy(chip_across, piece, r).wait_recv()
            hu_return(chip_across, piece)
            hd_copy(chip_across, piece, r).wait_recv()
            hd_return(chip_across, piece)

        with jax.named_scope('help'):
            each_piece(0, n_help, spread)
            each_piece(0, n_help, relay)
            each_piece(PIECES // 2, PIECES, ring_first)
            each_piece(0, PIECES, ring_second)
            each_piece(0, n_help, near)
            each_piece(0, n_help, far)

    def relay_near(piece):
        u_copy(left, piece, r).wait_recv()
        u_copy(left, piece, right).start()
        u_copy(left, piece, sib).start()
        d_copy(right, piece, r).wait_recv()
        d_copy(right, piece, left).start()
        d_copy(right, piece, sib).start()

    def take_near(piece):
        d_copy(left, piece, r).wait_recv()
        d_copy(left, piece, sib).start()
        u_copy(right, piece, r).wait_recv()
        u_copy(right, piece, sib).start()

    def take_across(piece):
        u_copy(across, piece, r).wait_recv()
        u_copy(across, piece, sib).start()
        d_copy(across, piece, r).wait_recv()
        d_copy(across, piece, sib).start()

    def take_help(piece):
        for slot in (left, right, across):
            u_copy(slot, piece, r).wait_recv()
            u_copy(slot, piece, sib).start()
            d_copy(slot, piece, r).wait_recv()
            d_copy(slot, piece, sib).start()

    def take_sib(piece):
        for slot in (sib, left + flip, right + flip, across + flip):
            u_copy(slot, piece, r).wait_recv()
            d_copy(slot, piece, r).wait_recv()

    with jax.named_scope('ag_first'):
        each_piece(0, n_ring, relay_near)
    with jax.named_scope('ag_second'):
        each_piece(0, n_ring, take_near)
    with jax.named_scope('ag_across'):
        each_piece(0, n_ring, take_across)
    with jax.named_scope('ag_help'):
        each_piece(n_ring, PIECES, take_help)
    with jax.named_scope('ag_sib'):
        each_piece(0, PIECES, take_sib)
    rcopy(gains.at[pl.ds(0, SEG - 1)], gains.at[pl.ds(0, SEG - 1)], gain_send, gain_recv, me).wait_recv()

    def act_ship(layer, k):
        mine = layer == r
        return rcopy(acts.at[layer, k], act_stash.at[k, jnp.where(mine, SEG, r)], as_send, as_recv.at[k],
                     row_base + jnp.where(mine, sib, layer))

    def grad_ship(layer, k):
        mine = layer == r
        return rcopy(grads.at[layer + 1, k], grad_stash.at[k, jnp.where(mine, SEG, r)], gs_send, gs_recv.at[k],
                     row_base + jnp.where(mine, sib, layer))

    def fwd_layer(layer, k):
        x_float = acts[layer, k].astype(F32)
        normed = (x_float * inv_rms_of(x_float) * gains[layer, 0:1, :]).astype(BF16)
        out = x_float
        for part in range(0, d_ff, COLS):
            cols = slice(part, part + COLS)
            hidden = dot_nn(normed, wu[layer, :, cols])
            hiddens[layer, k, :, cols] = hidden
            out += dot_nn(gelu_value(hidden).astype(BF16), wd[layer, cols, :])
        acts[layer + 1, k] = out.astype(BF16)

    def fwd_input_wait(k):
        @pl.when(row == 0)
        def _():
            x_load(k).wait()

        @pl.when(row > 0)
        def _():
            with jax.named_scope('fwd_wait'):
                rcopy(acts.at[0, k], acts.at[0, k], fwd_send, fwd_recv.at[k], me).wait_recv()

    def top_grad(k):
        y_load(k).wait()
        error_val = acts[SEG, k].astype(F32) - targets[k].astype(F32)
        loss_part[...] += fold_rows(error_val * error_val)
        grads[SEG, k] = ((2.0 * loss_scale) * error_val).astype(BF16)

    def fwd_group(group, k):
        for step in range(GROUP):
            fwd_layer(group * GROUP + step, k)
        return k

    def fwd_chunk(k, carry):
        fwd_input_wait(k)
        with jax.named_scope('fwd_layers'):
            lax.fori_loop(0, SEG // GROUP, fwd_group, k)

        @pl.when(row < n_rows - 1)
        def _():
            rcopy(acts.at[SEG, k], acts.at[0, k], fwd_send, fwd_recv.at[k], me + SEG).start()
        for layer in range(SEG):
            act_ship(layer, k).start()

        @pl.when(row == n_rows - 1)
        def _():
            top_grad(k)
        return carry

    lax.fori_loop(0, jnp.where(row == n_rows - 1, 1, N_CHUNKS), fwd_chunk, 0)

    def bwd_layer(step, k):
        layer = SEG - 1 - step
        grad_out = grads[layer + 1, k]
        x_float = acts[layer, k].astype(F32)
        inv_rms = inv_rms_of(x_float)
        x_hat = x_float * inv_rms
        gain = gains[layer, 0:1, :]
        grad_normed = 0.0
        for part in range(0, d_ff, COLS):
            cols = slice(part, part + COLS)
            hidden = hiddens[layer, k, :, cols]
            slope = gelu_slope(hidden, *gelu_gate(hidden))
            grad_gelu = dot_nt(grad_out, wd[layer, cols, :]).astype(BF16).astype(F32)
            grad_hidden = (grad_gelu * slope).astype(BF16)
            grad_normed += dot_nt(grad_hidden, wu[layer, :, cols])
        grad_normed = grad_normed.astype(BF16).astype(F32)
        dg_part[layer] += fold_rows(grad_normed * x_hat)
        grad_hat = grad_normed * gain
        mean_dot = jnp.mean(grad_hat * x_hat, axis=-1, keepdims=True)
        grad_x = inv_rms * (grad_hat - x_hat * mean_dot)
        grads[layer, k] = (grad_out.astype(F32) + grad_x).astype(BF16)

    def bwd_group(group, k):
        for step in range(GROUP):
            bwd_layer(group * GROUP + step, k)

        @pl.when((row > 0) & (group == SEG // GROUP - 1))
        def _():
            rcopy(grads.at[0, k], grads.at[SEG, k], bwd_send, bwd_recv.at[k], me - SEG).start()
        for step in range(GROUP):
            grad_ship(SEG - 1 - group * GROUP - step, k).start()
        return k

    def both_group(group, k):
        for step in range(GROUP):
            fwd_layer(group * GROUP + step, k)
            bwd_layer(group * GROUP + step, k - 1)

        @pl.when((row > 0) & (group == SEG // GROUP - 1))
        def _():
            rcopy(grads.at[0, k - 1], grads.at[SEG, k - 1], bwd_send, bwd_recv.at[k - 1], me - SEG).start()
        for step in range(GROUP):
            grad_ship(SEG - 1 - group * GROUP - step, k - 1).start()
        return k

    def both_chunks(k, carry):
        fwd_input_wait(k)
        with jax.named_scope('both_layers'):
            lax.fori_loop(0, SEG // GROUP, both_group, k)
        top_grad(k)
        for layer in range(SEG):
            act_ship(layer, k).start()
        return carry

    @pl.when(row == n_rows - 1)
    def _():
        lax.fori_loop(1, N_CHUNKS, both_chunks, 0)
        loss_stash[r] = loss_part[...]
        for step in range(1, SEG):
            rcopy(loss_stash.at[r], loss_stash.at[r], lrow_send, lrow_recv, row_base + lax.rem(r + step, SEG)).start()

    rest = act_stash.at[0, pl.ds(0, SEG)]
    all_rest = acts.at[pl.ds(0, SEG)]

    def owner_block(index):
        return lax.div(index, 2), pl.ds(lax.rem(index, 2) * HALF, HALF)

    def value_block(index, carry):
        k, srcs = owner_block(index)

        @pl.when(lax.rem(index, 2) == 0)
        def _():
            with jax.named_scope('as_wait'):
                rcopy(rest, rest, as_send, as_recv.at[k], me).wait_recv()
            act_stash[k, r] = acts[r, k]
        x_float = act_stash[k, srcs].reshape(HALF * chunk, d_model).astype(F32)
        normed = (x_float * inv_rms_of(x_float) * gains[r, 0:1, :]).astype(BF16)
        act_stash[k, srcs] = normed.reshape(HALF, chunk, d_model)
        for part in range(0, d_ff, COLS):
            cols = slice(part, part + COLS)
            hidden = dot_nn(normed, wu[r, :, cols])
            gate, sq = gelu_gate(hidden)
            value_stash[k, srcs, :, cols] = (hidden * gate).astype(BF16).reshape(HALF, chunk, COLS)
            slope_stash[k, srcs, :, cols] = gelu_slope(hidden, gate, sq).reshape(HALF, chunk, COLS)
        return carry

    def value_phase():
        dwu_ref[...] = jnp.zeros_like(dwu_ref)
        dwd_t[...] = jnp.zeros_like(dwd_t)
        with jax.named_scope('value_blocks'):
            lax.fori_loop(0, 2 * N_CHUNKS, value_block, 0)

    @pl.when(row < n_rows - LATE_ROWS)
    def _():
        value_phase()

    def weight_block(k, carry):
        rows = SEG * chunk
        with jax.named_scope('gs_wait'):
            rcopy(rest, rest, gs_send, gs_recv.at[k], me).wait_recv()
        grad_stash[k, r] = grads[r + 1, k]
        normed = act_stash[k, pl.ds(0, SEG)].reshape(rows, d_model)
        grad_out = grad_stash[k, pl.ds(0, SEG)].reshape(rows, d_model)
        for part in range(0, d_ff, COLS):
            cols = slice(part, part + COLS)
            grad_gelu = dot_nt(grad_out, wd[r, cols, :]).astype(BF16).astype(F32)
            grad_hidden = (grad_gelu * slope_stash[k, :, :, cols].reshape(rows, COLS)).astype(BF16)
            dwu_ref[0, :, cols] += dot_tn(normed, grad_hidden)
            dwd_t[:, cols] += dot_tn(grad_out, value_stash[k, :, :, cols].reshape(rows, COLS))
        return carry

    def bwd_chunk(k, carry):
        @pl.when(row < n_rows - 1)
        def _():
            with jax.named_scope('bwd_wait'):
                rcopy(grads.at[SEG, k], grads.at[SEG, k], bwd_send, bwd_recv.at[k], me).wait_recv()

        with jax.named_scope('bwd_layers'):
            lax.fori_loop(0, SEG // GROUP, bwd_group, k)
        return carry

    lax.fori_loop(jnp.where(row == n_rows - 1, N_CHUNKS - 1, 0), N_CHUNKS, bwd_chunk, 0)

    def dg_ship(layer):
        return rcopy(dg_part.at[layer], dg_stash.at[r], dg_send, dg_recv, row_base + layer)

    for step in range(1, SEG):
        dg_ship(lax.rem(r + step, SEG)).start()
    dg_stash[r] = dg_part[r]

    @pl.when(row >= n_rows - LATE_ROWS)
    def _():
        value_phase()

    with jax.named_scope('weight_blocks'):
        lax.fori_loop(0, N_CHUNKS, weight_block, 0)
    @pl.when(row == n_rows - 1)
    def _():
        rest_row = loss_stash.at[pl.ds(0, SEG - 1)]
        rcopy(rest_row, rest_row, lrow_send, lrow_recv, me).wait_recv()
        loss_total[...] = jnp.sum(loss_stash[...], axis=0)
        for step in range(1, n_rows):
            rcopy(loss_total, loss_total, lcol_send, lcol_recv, me - step * SEG).start()

    with jax.named_scope('turn'):
        dwd_ref[0] = dwd_t[...].T

    rest_dg = dg_stash.at[pl.ds(0, SEG - 1)]
    with jax.named_scope('dg_wait'):
        rcopy(rest_dg, rest_dg, dg_send, dg_recv, me).wait_recv()
    dgain_ref[...] = jnp.sum(jnp.sum(dg_stash[...], axis=0), axis=0, keepdims=True)

    @pl.when(row < n_rows - 1)
    def _():
        rcopy(loss_total, loss_total, lcol_send, lcol_recv, me).wait_recv()
    loss_ref[0] = jnp.sum(loss_total[...]) * loss_scale

    def sent_own(piece):
        rcopy(u_part(r, 0), u_part(r, 0), agu_send, gain_recv, me).wait_send()
        rcopy(d_part(r, 0), d_part(r, 0), agd_send, gain_recv, me).wait_send()
    each_piece(0, jnp.where(helped, 3 * n_direct + n_help + 4 * PIECES, 7 * PIECES), sent_own)

    def sent_help(piece):
        rcopy(help_u.at[0, 0], help_u.at[0, 0], hu_send, gain_recv, me).wait_send()
        rcopy(help_d.at[0, 0], help_d.at[0, 0], hd_send, gain_recv, me).wait_send()
    each_piece(0, jnp.where(helped, 0, 6 * n_help), sent_help)
    rest_gain = gains.at[pl.ds(0, SEG - 1)]
    rcopy(rest_gain, rest_gain, gain_send, gain_recv, me).wait_send()
    rcopy(all_rest, all_rest, as_send, dg_recv, me).wait_send()
    rcopy(all_rest, all_rest, gs_send, dg_recv, me).wait_send()
    rcopy(rest_dg, rest_dg, dg_send, dg_recv, me).wait_send()

    @pl.when(row < n_rows - 1)
    def _():
        rcopy(acts.at[0], acts.at[0], fwd_send, dg_recv, me).wait_send()

    @pl.when(row > 0)
    def _():
        rcopy(grads.at[0], grads.at[0], bwd_send, dg_recv, me).wait_send()

    @pl.when(row == n_rows - 1)
    def _():
        rest_row = loss_stash.at[pl.ds(0, SEG - 1)]
        rcopy(rest_row, rest_row, lrow_send, lrow_recv, me).wait_send()
        for step in range(1, n_rows):
            rcopy(loss_total, loss_total, lcol_send, lcol_recv, me).wait_send()


def write_kernel(n_parts, up_hbm, down_hbm, gain_ref, loss_ref, up_out, down_out, gain_out, loss_out,
                 up_buf, down_buf, in_sem, out_sem):
    pairs = ((up_hbm, up_buf, up_out), (down_hbm, down_buf, down_out))

    def part(ref, index):
        rows = ref.shape[0] // n_parts
        return ref.at[pl.ds(index * rows, rows)]

    reads, writes = [], []
    for side, (src, buf, dst) in enumerate(pairs):
        for index in range(n_parts):
            reads.append(pltpu.make_async_copy(part(src.at[0], index), part(buf, index), in_sem.at[side, index]))
            writes.append(pltpu.make_async_copy(part(buf, index), part(dst.at[0], index), out_sem.at[side, index]))
    for read in reads:
        read.start()
    gain_out[...] = gain_ref[...]
    loss_out[0] = loss_ref[0]
    for read, write in zip(reads, writes):
        read.wait()
        write.start()
    for write in writes:
        write.wait()


def solution(mesh):
    n_stages = mesh.shape['stage']

    def stage_body(x_in, y_target, w_up, w_down, norm_gain):
        n_micro, n_tok, d_model = x_in.shape
        d_ff = w_up.shape[2]
        n_rows = n_micro * n_tok
        chunk = n_rows // SEG // N_CHUNKS
        loss_scale = 1.0 / (n_rows * d_model)
        sem = pltpu.SemaphoreType.DMA
        act_shape = (N_CHUNKS, chunk, d_model)
        scratch = [
            pltpu.VMEM((SEG, d_model, d_ff), BF16),
            pltpu.VMEM((SEG, d_ff, d_model), BF16),
            pltpu.VMEM((SEG // 2, HELP, d_model // PIECES, d_ff), BF16),
            pltpu.VMEM((SEG // 2, HELP, d_ff // PIECES, d_model), BF16),
            pltpu.VMEM((SEG, 8, d_model), F32),
            pltpu.VMEM((SEG + 1,) + act_shape, BF16),
            pltpu.VMEM((SEG + 1,) + act_shape, BF16),
            pltpu.VMEM((SEG, N_CHUNKS, chunk, d_ff), F32),
            pltpu.VMEM((N_CHUNKS, SEG + 1, chunk, d_model), BF16),
            pltpu.VMEM((N_CHUNKS, SEG + 1, chunk, d_model), BF16),
            pltpu.VMEM((N_CHUNKS, SEG, chunk, d_ff), BF16),
            pltpu.VMEM((N_CHUNKS, SEG, chunk, d_ff), F32),
            pltpu.VMEM(act_shape, BF16),
            pltpu.VMEM((d_model, d_ff), F32),
            pltpu.VMEM((SEG, 8, d_model), F32),
            pltpu.VMEM((SEG, 8, d_model), F32),
            pltpu.VMEM((8, d_model), F32),
            pltpu.VMEM((SEG, 8, d_model), F32),
            pltpu.VMEM((8, d_model), F32),
            sem((2,)), sem((N_CHUNKS,)), sem((N_CHUNKS,)),
            sem, sem((SEG, PIECES)), sem, sem((SEG, PIECES)), sem, sem((SEG // 2, HELP)), sem, sem((SEG // 2, HELP)), sem, sem,
            sem, sem((N_CHUNKS,)), sem, sem((N_CHUNKS,)), sem, sem((N_CHUNKS,)), sem, sem((N_CHUNKS,)),
            sem, sem, sem, sem, sem, sem,
        ]
        any_spec = pl.BlockSpec(memory_space=pl.ANY)
        vmem_spec = pl.BlockSpec(memory_space=pltpu.VMEM)
        dw_up, dw_down, dgain, loss = pl.pallas_call(
            functools.partial(step_kernel, n_stages, loss_scale),
            out_shape=(jax.ShapeDtypeStruct(w_up.shape, F32), jax.ShapeDtypeStruct(w_down.shape, F32),
                       jax.ShapeDtypeStruct(norm_gain.shape, F32), jax.ShapeDtypeStruct((1,), F32)),
            in_specs=[any_spec, any_spec, any_spec, any_spec, vmem_spec],
            out_specs=(vmem_spec, vmem_spec, vmem_spec, pl.BlockSpec(memory_space=pltpu.SMEM)),
            scratch_shapes=scratch,
            compiler_params=pltpu.CompilerParams(collective_id=0, has_side_effects=True,
                                                 vmem_limit_bytes=67043328),
        )(x_in.reshape(n_rows, d_model), y_target.reshape(n_rows, d_model), w_up, w_down, norm_gain)
        smem_spec = pl.BlockSpec(memory_space=pltpu.SMEM)
        return pl.pallas_call(
            functools.partial(write_kernel, WRITE_PARTS),
            out_shape=(jax.ShapeDtypeStruct(w_up.shape, F32), jax.ShapeDtypeStruct(w_down.shape, F32),
                       jax.ShapeDtypeStruct(norm_gain.shape, F32), jax.ShapeDtypeStruct((1,), F32)),
            in_specs=[any_spec, any_spec, vmem_spec, smem_spec],
            out_specs=(any_spec, any_spec, vmem_spec, smem_spec),
            scratch_shapes=[pltpu.VMEM(w_up.shape[1:], F32), pltpu.VMEM(w_down.shape[1:], F32),
                            sem((2, WRITE_PARTS)), sem((2, WRITE_PARTS))],
        )(dw_up, dw_down, dgain, loss)

    return jax.shard_map(stage_body, mesh=mesh,
                         in_specs=(P('dp'), P('dp'), P('stage'), P('stage'), P('stage')),
                         out_specs=(P(('dp', 'stage')), P(('dp', 'stage')), P(('dp', 'stage')), P('dp')),
                         check_vma=False)
```

```python
import functools

import jax
import jax.numpy as jnp
from jax import lax
from jax.experimental import pallas as pl
from jax.experimental.pallas import tpu as pltpu
from jax.sharding import PartitionSpec as P

NORM_EPS = 1e-6
SEG = 8
N_CHUNKS = 4
PIECES = 8
HELP = 2
COLS = 256
HALF = SEG // 2
GROUP = 4
LATE_ROWS = 2
WRITE_PARTS = 4
GELU_C = 0.7978845608028654
GELU_A = 0.044715
MESH = pl.DeviceIdType.MESH
F32 = jnp.float32
BF16 = jnp.bfloat16


def dot_nn(lhs, rhs):
    return lax.dot_general(lhs, rhs, (((1,), (0,)), ((), ())), preferred_element_type=F32)


def dot_nt(lhs, rhs):
    return lax.dot_general(lhs, rhs, (((1,), (1,)), ((), ())), preferred_element_type=F32)


def dot_tn(lhs, rhs):
    return lax.dot_general(lhs, rhs, (((0,), (0,)), ((), ())), preferred_element_type=F32)


def gelu_gate(hidden):
    sq = hidden * hidden
    gate = 0.5 + 0.5 * jnp.tanh(hidden * (GELU_C + (GELU_C * GELU_A) * sq))
    return gate, sq


def gelu_value(hidden):
    return hidden * gelu_gate(hidden)[0]


def gelu_slope(hidden, gate, sq):
    return gate + ((gate * (1.0 - gate)) * hidden) * (2.0 * GELU_C + (6.0 * GELU_C * GELU_A) * sq)


def inv_rms_of(x_float):
    return lax.rsqrt(jnp.mean(x_float * x_float, axis=-1, keepdims=True) + NORM_EPS)


def fold_rows(block):
    rows, cols = block.shape
    return jnp.sum(block.reshape(rows // 8, 8, cols), axis=0)


def step_kernel(n_stages, loss_scale,
                x_hbm, y_hbm, wu_hbm, wd_hbm, gain_ref,
                dwu_hbm, dwd_hbm, sums_hbm,
                wu, wd, help_u, help_d, gains, acts, grads, hiddens, act_stash, grad_stash, value_stash, slope_stash, targets, dwu, dwd_t, dwd, sums,
                dg_part, dg_stash, loss_part, loss_stash, loss_total,
                load_sem, out_sem, x_sem, y_sem, agu_send, agu_recv, agd_send, agd_recv, hu_send, hu_recv, hd_send, hd_recv, gain_send, gain_recv,
                as_send, as_recv, gs_send, gs_recv, fwd_send, fwd_recv, bwd_send, bwd_recv,
                dg_send, dg_recv, lrow_send, lrow_recv, lcol_send, lcol_recv):
    n_rows = n_stages // SEG
    n_chips = SEG // 2
    chunk = acts.shape[2]
    d_model = acts.shape[3]
    d_ff = wu.shape[2]
    me = lax.axis_index('stage')
    row = lax.div(me, SEG)
    r = lax.rem(me, SEG)
    chip = lax.div(r, 2)
    core = lax.rem(r, 2)
    row_base = row * SEG
    left = lax.rem(chip + n_chips - 1, n_chips) * 2 + core
    right = lax.rem(chip + 1, n_chips) * 2 + core
    across = lax.rem(chip + 2, n_chips) * 2 + core
    flip = 1 - 2 * core
    sib = r + flip

    def rcopy(src, dst, send_sem, recv_sem, dev):
        return pltpu.make_async_remote_copy(src_ref=src, dst_ref=dst, send_sem=send_sem, recv_sem=recv_sem,
                                            device_id={'stage': dev}, device_id_type=MESH)

    load_u = pltpu.make_async_copy(wu_hbm.at[0], wu.at[r], load_sem.at[0])
    load_d = pltpu.make_async_copy(wd_hbm.at[0], wd.at[r], load_sem.at[1])
    load_u.start()
    load_d.start()

    def x_load(k):
        first = pl.multiple_of((r * N_CHUNKS + k) * chunk, chunk)
        return pltpu.make_async_copy(x_hbm.at[pl.ds(first, chunk)], acts.at[0, k], x_sem.at[k])

    def y_load(k):
        first = pl.multiple_of((r * N_CHUNKS + k) * chunk, chunk)
        return pltpu.make_async_copy(y_hbm.at[pl.ds(first, chunk)], targets.at[k], y_sem.at[k])

    @pl.when(row == 0)
    def _():
        for k in range(N_CHUNKS):
            x_load(k).start()

    @pl.when(row == n_rows - 1)
    def _():
        for k in range(N_CHUNKS):
            y_load(k).start()

    gains[r] = jnp.broadcast_to(gain_ref[...], (8, d_model))
    dg_part[...] = jnp.zeros_like(dg_part)
    loss_part[...] = jnp.zeros_like(loss_part)

    with jax.named_scope('barrier'):
        barrier = pltpu.get_barrier_semaphore()
        for step in range(1, SEG):
            pl.semaphore_signal(barrier, inc=1, device_id={'stage': row_base + lax.rem(r + step, SEG)}, device_id_type=MESH)
        for step in range(1, n_rows):
            pl.semaphore_signal(barrier, inc=1, device_id={'stage': lax.rem(row + step, n_rows) * SEG + r}, device_id_type=MESH)
        pl.semaphore_wait(barrier, SEG - 1 + n_rows - 1)

    u_rows = d_model // PIECES
    d_rows = d_ff // PIECES
    helped = row < n_rows // 2
    partner = (n_rows - 1 - row) * SEG + r
    n_help = jnp.where((row == 0) | (row == n_rows - 1), HELP, HELP - 1)
    n_direct = PIECES - n_help
    n_ring = jnp.where(helped, n_direct, PIECES)
    chip_left, chip_right, chip_across = lax.div(left, 2), lax.div(right, 2), lax.div(across, 2)

    def each_piece(first, last, fn):
        def body(piece, carry):
            fn(piece)
            return carry
        lax.fori_loop(first, last, body, 0)

    def u_part(slot, piece):
        return wu.at[slot, pl.ds(pl.multiple_of(piece * u_rows, u_rows), u_rows)]

    def d_part(slot, piece):
        return wd.at[slot, pl.ds(pl.multiple_of(piece * d_rows, d_rows), d_rows)]

    def u_copy(slot, piece, dev):
        part = u_part(slot, piece)
        return rcopy(part, part, agu_send, agu_recv.at[slot, piece], row_base + dev)

    def d_copy(slot, piece, dev):
        part = d_part(slot, piece)
        return rcopy(part, part, agd_send, agd_recv.at[slot, piece], row_base + dev)

    def hu_copy(place, piece, dev):
        part = help_u.at[place, piece]
        return rcopy(part, part, hu_send, hu_recv.at[place, piece], row_base + dev)

    def hd_copy(place, piece, dev):
        part = help_d.at[place, piece]
        return rcopy(part, part, hd_send, hd_recv.at[place, piece], row_base + dev)

    def hu_give(piece):
        rcopy(u_part(r, n_direct + piece), help_u.at[chip, piece], agu_send, hu_recv.at[chip, piece], partner).start()

    def hd_give(piece):
        rcopy(d_part(r, n_direct + piece), help_d.at[chip, piece], agd_send, hd_recv.at[chip, piece], partner).start()

    def hu_return(place, piece):
        slot = place * 2 + core
        rcopy(help_u.at[place, piece], u_part(slot, n_direct + piece), hu_send, agu_recv.at[slot, n_direct + piece], partner).start()

    def hd_return(place, piece):
        slot = place * 2 + core
        rcopy(help_d.at[place, piece], d_part(slot, n_direct + piece), hd_send, agd_recv.at[slot, n_direct + piece], partner).start()

    with jax.named_scope('w_load_u'):
        load_u.wait()
    with jax.named_scope('w_load_d'):
        load_d.wait()
    def ring_first(piece):
        u_copy(r, piece, right).start()
        d_copy(r, piece, left).start()

    def ring_second(piece):
        d_copy(r, piece, right).start()
        u_copy(r, piece, left).start()

    def give(piece):
        hu_give(piece)
        hd_give(piece)

    @pl.when(helped)
    def _():
        each_piece(0, n_help, give)
        each_piece(0, n_direct, ring_first)
        each_piece(0, n_direct, ring_second)

    @pl.when(jnp.logical_not(helped))
    def _():
        each_piece(0, PIECES // 2, ring_first)

    def own_to_sib(piece):
        u_copy(r, piece, sib).start()
        d_copy(r, piece, sib).start()
    each_piece(0, PIECES, own_to_sib)
    for step in range(1, SEG):
        rcopy(gains.at[r], gains.at[r], gain_send, gain_recv, row_base + lax.rem(r + step, SEG)).start()

    @pl.when(jnp.logical_not(helped))
    def _():
        def spread(piece):
            hu_copy(chip, piece, r).wait_recv()
            hu_copy(chip, piece, right).start()
            hu_copy(chip, piece, left).start()
            hd_copy(chip, piece, r).wait_recv()
            hd_copy(chip, piece, left).start()
            hd_copy(chip, piece, right).start()

        def relay(piece):
            hu_copy(chip_left, piece, r).wait_recv()
            hu_copy(chip_left, piece, right).start()
            hu_return(chip_left, piece)
            hd_copy(chip_right, piece, r).wait_recv()
            hd_copy(chip_right, piece, left).start()
            hd_return(chip_right, piece)

        def near(piece):
            hd_copy(chip_left, piece, r).wait_recv()
            hd_return(chip_left, piece)
            hu_copy(chip_right, piece, r).wait_recv()
            hu_return(chip_right, piece)

        def far(piece):
            hu_copy(chip_across, piece, r).wait_recv()
            hu_return(chip_across, piece)
            hd_copy(chip_across, piece, r).wait_recv()
            hd_return(chip_across, piece)

        with jax.named_scope('help'):
            each_piece(0, n_help, spread)
            each_piece(0, n_help, relay)
            each_piece(PIECES // 2, PIECES, ring_first)
            each_piece(0, PIECES, ring_second)
            each_piece(0, n_help, near)
            each_piece(0, n_help, far)

    def relay_near(piece):
        u_copy(left, piece, r).wait_recv()
        u_copy(left, piece, right).start()
        u_copy(left, piece, sib).start()
        d_copy(right, piece, r).wait_recv()
        d_copy(right, piece, left).start()
        d_copy(right, piece, sib).start()

    def take_near(piece):
        d_copy(left, piece, r).wait_recv()
        d_copy(left, piece, sib).start()
        u_copy(right, piece, r).wait_recv()
        u_copy(right, piece, sib).start()

    def take_across(piece):
        u_copy(across, piece, r).wait_recv()
        u_copy(across, piece, sib).start()
        d_copy(across, piece, r).wait_recv()
        d_copy(across, piece, sib).start()

    def take_help(piece):
        for slot in (left, right, across):
            u_copy(slot, piece, r).wait_recv()
            u_copy(slot, piece, sib).start()
            d_copy(slot, piece, r).wait_recv()
            d_copy(slot, piece, sib).start()

    def take_sib(piece):
        for slot in (sib, left + flip, right + flip, across + flip):
            u_copy(slot, piece, r).wait_recv()
            d_copy(slot, piece, r).wait_recv()

    with jax.named_scope('ag_first'):
        each_piece(0, n_ring, relay_near)
    with jax.named_scope('ag_second'):
        each_piece(0, n_ring, take_near)
    with jax.named_scope('ag_across'):
        each_piece(0, n_ring, take_across)
    with jax.named_scope('ag_help'):
        each_piece(n_ring, PIECES, take_help)
    with jax.named_scope('ag_sib'):
        each_piece(0, PIECES, take_sib)
    rcopy(gains.at[pl.ds(0, SEG - 1)], gains.at[pl.ds(0, SEG - 1)], gain_send, gain_recv, me).wait_recv()

    def act_ship(layer, k):
        mine = layer == r
        return rcopy(acts.at[layer, k], act_stash.at[k, jnp.where(mine, SEG, r)], as_send, as_recv.at[k],
                     row_base + jnp.where(mine, sib, layer))

    def grad_ship(layer, k):
        mine = layer == r
        return rcopy(grads.at[layer + 1, k], grad_stash.at[k, jnp.where(mine, SEG, r)], gs_send, gs_recv.at[k],
                     row_base + jnp.where(mine, sib, layer))

    def fwd_layer(layer, k):
        x_float = acts[layer, k].astype(F32)
        normed = (x_float * inv_rms_of(x_float) * gains[layer, 0:1, :]).astype(BF16)
        out = x_float
        for part in range(0, d_ff, COLS):
            cols = slice(part, part + COLS)
            hidden = dot_nn(normed, wu[layer, :, cols])
            hiddens[layer, k, :, cols] = hidden
            out += dot_nn(gelu_value(hidden).astype(BF16), wd[layer, cols, :])
        acts[layer + 1, k] = out.astype(BF16)

    def fwd_input_wait(k):
        @pl.when(row == 0)
        def _():
            x_load(k).wait()

        @pl.when(row > 0)
        def _():
            with jax.named_scope('fwd_wait'):
                rcopy(acts.at[0, k], acts.at[0, k], fwd_send, fwd_recv.at[k], me).wait_recv()

    def top_grad(k):
        y_load(k).wait()
        error_val = acts[SEG, k].astype(F32) - targets[k].astype(F32)
        loss_part[...] += fold_rows(error_val * error_val)
        grads[SEG, k] = ((2.0 * loss_scale) * error_val).astype(BF16)

    def fwd_group(group, k):
        for step in range(GROUP):
            fwd_layer(group * GROUP + step, k)
        return k

    def fwd_chunk(k, carry):
        fwd_input_wait(k)
        with jax.named_scope('fwd_layers'):
            lax.fori_loop(0, SEG // GROUP, fwd_group, k)

        @pl.when(row < n_rows - 1)
        def _():
            rcopy(acts.at[SEG, k], acts.at[0, k], fwd_send, fwd_recv.at[k], me + SEG).start()
        for layer in range(SEG):
            act_ship(layer, k).start()

        @pl.when(row == n_rows - 1)
        def _():
            top_grad(k)
        return carry

    lax.fori_loop(0, jnp.where(row == n_rows - 1, 1, N_CHUNKS), fwd_chunk, 0)

    def bwd_layer(step, k):
        layer = SEG - 1 - step
        grad_out = grads[layer + 1, k]
        x_float = acts[layer, k].astype(F32)
        inv_rms = inv_rms_of(x_float)
        x_hat = x_float * inv_rms
        gain = gains[layer, 0:1, :]
        grad_normed = 0.0
        for part in range(0, d_ff, COLS):
            cols = slice(part, part + COLS)
            hidden = hiddens[layer, k, :, cols]
            slope = gelu_slope(hidden, *gelu_gate(hidden))
            grad_gelu = dot_nt(grad_out, wd[layer, cols, :]).astype(BF16).astype(F32)
            grad_hidden = (grad_gelu * slope).astype(BF16)
            grad_normed += dot_nt(grad_hidden, wu[layer, :, cols])
        grad_normed = grad_normed.astype(BF16).astype(F32)
        dg_part[layer] += fold_rows(grad_normed * x_hat)
        grad_hat = grad_normed * gain
        mean_dot = jnp.mean(grad_hat * x_hat, axis=-1, keepdims=True)
        grad_x = inv_rms * (grad_hat - x_hat * mean_dot)
        grads[layer, k] = (grad_out.astype(F32) + grad_x).astype(BF16)

    def bwd_group(group, k):
        for step in range(GROUP):
            bwd_layer(group * GROUP + step, k)

        @pl.when((row > 0) & (group == SEG // GROUP - 1))
        def _():
            rcopy(grads.at[0, k], grads.at[SEG, k], bwd_send, bwd_recv.at[k], me - SEG).start()
        for step in range(GROUP):
            grad_ship(SEG - 1 - group * GROUP - step, k).start()
        return k

    def both_group(group, k):
        for step in range(GROUP):
            fwd_layer(group * GROUP + step, k)
            bwd_layer(group * GROUP + step, k - 1)

        @pl.when((row > 0) & (group == SEG // GROUP - 1))
        def _():
            rcopy(grads.at[0, k - 1], grads.at[SEG, k - 1], bwd_send, bwd_recv.at[k - 1], me - SEG).start()
        for step in range(GROUP):
            grad_ship(SEG - 1 - group * GROUP - step, k - 1).start()
        return k

    def both_chunks(k, carry):
        fwd_input_wait(k)
        with jax.named_scope('both_layers'):
            lax.fori_loop(0, SEG // GROUP, both_group, k)
        top_grad(k)
        for layer in range(SEG):
            act_ship(layer, k).start()
        return carry

    @pl.when(row == n_rows - 1)
    def _():
        lax.fori_loop(1, N_CHUNKS, both_chunks, 0)
        loss_stash[r] = loss_part[...]
        for step in range(1, SEG):
            rcopy(loss_stash.at[r], loss_stash.at[r], lrow_send, lrow_recv, row_base + lax.rem(r + step, SEG)).start()

    rest = act_stash.at[0, pl.ds(0, SEG)]
    all_rest = acts.at[pl.ds(0, SEG)]

    def owner_block(index):
        return lax.div(index, 2), pl.ds(lax.rem(index, 2) * HALF, HALF)

    def value_block(index, carry):
        k, srcs = owner_block(index)

        @pl.when(lax.rem(index, 2) == 0)
        def _():
            with jax.named_scope('as_wait'):
                rcopy(rest, rest, as_send, as_recv.at[k], me).wait_recv()
            act_stash[k, r] = acts[r, k]
        x_float = act_stash[k, srcs].reshape(HALF * chunk, d_model).astype(F32)
        normed = (x_float * inv_rms_of(x_float) * gains[r, 0:1, :]).astype(BF16)
        act_stash[k, srcs] = normed.reshape(HALF, chunk, d_model)
        for part in range(0, d_ff, COLS):
            cols = slice(part, part + COLS)
            hidden = dot_nn(normed, wu[r, :, cols])
            gate, sq = gelu_gate(hidden)
            value_stash[k, srcs, :, cols] = (hidden * gate).astype(BF16).reshape(HALF, chunk, COLS)
            slope_stash[k, srcs, :, cols] = gelu_slope(hidden, gate, sq).reshape(HALF, chunk, COLS)
        return carry

    def sent_own(piece):
        rcopy(u_part(r, 0), u_part(r, 0), agu_send, gain_recv, me).wait_send()
        rcopy(d_part(r, 0), d_part(r, 0), agd_send, gain_recv, me).wait_send()

    def sent_help(piece):
        rcopy(help_u.at[0, 0], help_u.at[0, 0], hu_send, gain_recv, me).wait_send()
        rcopy(help_d.at[0, 0], help_d.at[0, 0], hd_send, gain_recv, me).wait_send()

    def value_phase():
        dwu[...] = jnp.zeros_like(dwu)
        dwd_t[...] = jnp.zeros_like(dwd_t)
        with jax.named_scope('value_blocks'):
            lax.fori_loop(0, 2 * N_CHUNKS, value_block, 0)
        each_piece(0, jnp.where(helped, 3 * n_direct + n_help + 4 * PIECES, 7 * PIECES), sent_own)
        each_piece(0, jnp.where(helped, 0, 6 * n_help), sent_help)
        rest_gain = gains.at[pl.ds(0, SEG - 1)]
        rcopy(rest_gain, rest_gain, gain_send, gain_recv, me).wait_send()
        rcopy(all_rest, all_rest, as_send, dg_recv, me).wait_send()

        @pl.when(row < n_rows - 1)
        def _():
            rcopy(acts.at[0], acts.at[0], fwd_send, dg_recv, me).wait_send()

    @pl.when(row < n_rows - LATE_ROWS)
    def _():
        value_phase()

    def weight_block(k, carry):
        rows = SEG * chunk
        with jax.named_scope('gs_wait'):
            rcopy(rest, rest, gs_send, gs_recv.at[k], me).wait_recv()
        grad_stash[k, r] = grads[r + 1, k]
        normed = act_stash[k, pl.ds(0, SEG)].reshape(rows, d_model)
        grad_out = grad_stash[k, pl.ds(0, SEG)].reshape(rows, d_model)
        for part in range(0, d_ff, COLS):
            cols = slice(part, part + COLS)
            grad_gelu = dot_nt(grad_out, wd[r, cols, :]).astype(BF16).astype(F32)
            grad_hidden = (grad_gelu * slope_stash[k, :, :, cols].reshape(rows, COLS)).astype(BF16)
            dwu[:, cols] += dot_tn(normed, grad_hidden)
            dwd_t[:, cols] += dot_tn(grad_out, value_stash[k, :, :, cols].reshape(rows, COLS))
        return carry

    def bwd_chunk(k, carry):
        @pl.when(row < n_rows - 1)
        def _():
            with jax.named_scope('bwd_wait'):
                rcopy(grads.at[SEG, k], grads.at[SEG, k], bwd_send, bwd_recv.at[k], me).wait_recv()

        with jax.named_scope('bwd_layers'):
            lax.fori_loop(0, SEG // GROUP, bwd_group, k)
        return carry

    lax.fori_loop(jnp.where(row == n_rows - 1, N_CHUNKS - 1, 0), N_CHUNKS, bwd_chunk, 0)

    def dg_ship(layer):
        return rcopy(dg_part.at[layer], dg_stash.at[r], dg_send, dg_recv, row_base + layer)

    for step in range(1, SEG):
        dg_ship(lax.rem(r + step, SEG)).start()
    dg_stash[r] = dg_part[r]

    @pl.when(row >= n_rows - LATE_ROWS)
    def _():
        value_phase()

    with jax.named_scope('weight_blocks'):
        lax.fori_loop(0, N_CHUNKS, weight_block, 0)
    @pl.when(row == n_rows - 1)
    def _():
        rest_row = loss_stash.at[pl.ds(0, SEG - 1)]
        rcopy(rest_row, rest_row, lrow_send, lrow_recv, me).wait_recv()
        loss_total[...] = jnp.sum(loss_stash[...], axis=0)
        for step in range(1, n_rows):
            rcopy(loss_total, loss_total, lcol_send, lcol_recv, me - step * SEG).start()

    with jax.named_scope('turn'):
        up_out = pltpu.make_async_copy(dwu, dwu_hbm.at[0], out_sem.at[0])
        up_out.start()
        dwd[...] = dwd_t[...].T
        down_out = pltpu.make_async_copy(dwd, dwd_hbm.at[0], out_sem.at[1])
        down_out.start()

    rest_dg = dg_stash.at[pl.ds(0, SEG - 1)]
    with jax.named_scope('dg_wait'):
        rcopy(rest_dg, rest_dg, dg_send, dg_recv, me).wait_recv()
    sums[0:8] = jnp.sum(dg_stash[...], axis=0)

    @pl.when(row < n_rows - 1)
    def _():
        rcopy(loss_total, loss_total, lcol_send, lcol_recv, me).wait_recv()
    sums[8:16] = loss_total[...]
    sums_out = pltpu.make_async_copy(sums, sums_hbm, out_sem.at[2])
    sums_out.start()

    rcopy(all_rest, all_rest, gs_send, dg_recv, me).wait_send()
    rcopy(rest_dg, rest_dg, dg_send, dg_recv, me).wait_send()

    @pl.when(row > 0)
    def _():
        rcopy(grads.at[0], grads.at[0], bwd_send, dg_recv, me).wait_send()

    @pl.when(row == n_rows - 1)
    def _():
        rest_row = loss_stash.at[pl.ds(0, SEG - 1)]
        rcopy(rest_row, rest_row, lrow_send, lrow_recv, me).wait_send()
        for step in range(1, n_rows):
            rcopy(loss_total, loss_total, lcol_send, lcol_recv, me).wait_send()
    up_out.wait()
    down_out.wait()
    sums_out.wait()


def write_kernel(n_parts, loss_scale, up_hbm, down_hbm, sums_hbm, up_out, down_out, gain_out, loss_out,
                 up_buf, down_buf, sums_buf, gain_buf, loss_buf, in_sem, out_sem, small_sem):
    pairs = ((up_hbm, up_buf, up_out), (down_hbm, down_buf, down_out))

    def part(ref, index):
        rows = ref.shape[0] // n_parts
        return ref.at[pl.ds(index * rows, rows)]

    sums_read = pltpu.make_async_copy(sums_hbm, sums_buf, small_sem.at[0])
    gain_write = pltpu.make_async_copy(gain_buf, gain_out, small_sem.at[1])
    loss_write = pltpu.make_async_copy(loss_buf, loss_out, small_sem.at[2])
    sums_read.start()
    reads, writes = [], []
    for side, (src, buf, dst) in enumerate(pairs):
        for index in range(n_parts):
            reads.append(pltpu.make_async_copy(part(src.at[0], index), part(buf, index), in_sem.at[side, index]))
            writes.append(pltpu.make_async_copy(part(buf, index), part(dst.at[0], index), out_sem.at[side, index]))
    for read in reads:
        read.start()
    sums_read.wait()
    gain_buf[...] = jnp.sum(sums_buf[0:8], axis=0, keepdims=True)
    loss_buf[0] = jnp.sum(sums_buf[8:16]) * loss_scale
    for read, write in zip(reads, writes):
        read.wait()
        write.start()
    gain_write.start()
    loss_write.start()
    for write in writes:
        write.wait()
    gain_write.wait()
    loss_write.wait()


def solution(mesh):
    n_stages = mesh.shape['stage']

    def stage_body(x_in, y_target, w_up, w_down, norm_gain):
        n_micro, n_tok, d_model = x_in.shape
        d_ff = w_up.shape[2]
        n_rows = n_micro * n_tok
        chunk = n_rows // SEG // N_CHUNKS
        loss_scale = 1.0 / (n_rows * d_model)
        sem = pltpu.SemaphoreType.DMA
        act_shape = (N_CHUNKS, chunk, d_model)
        scratch = [
            pltpu.VMEM((SEG, d_model, d_ff), BF16),
            pltpu.VMEM((SEG, d_ff, d_model), BF16),
            pltpu.VMEM((SEG // 2, HELP, d_model // PIECES, d_ff), BF16),
            pltpu.VMEM((SEG // 2, HELP, d_ff // PIECES, d_model), BF16),
            pltpu.VMEM((SEG, 8, d_model), F32),
            pltpu.VMEM((SEG + 1,) + act_shape, BF16),
            pltpu.VMEM((SEG + 1,) + act_shape, BF16),
            pltpu.VMEM((SEG, N_CHUNKS, chunk, d_ff), F32),
            pltpu.VMEM((N_CHUNKS, SEG + 1, chunk, d_model), BF16),
            pltpu.VMEM((N_CHUNKS, SEG + 1, chunk, d_model), BF16),
            pltpu.VMEM((N_CHUNKS, SEG, chunk, d_ff), BF16),
            pltpu.VMEM((N_CHUNKS, SEG, chunk, d_ff), F32),
            pltpu.VMEM(act_shape, BF16),
            pltpu.VMEM((d_model, d_ff), F32),
            pltpu.VMEM((d_model, d_ff), F32),
            pltpu.VMEM((d_ff, d_model), F32),
            pltpu.VMEM((16, d_model), F32),
            pltpu.VMEM((SEG, 8, d_model), F32),
            pltpu.VMEM((SEG, 8, d_model), F32),
            pltpu.VMEM((8, d_model), F32),
            pltpu.VMEM((SEG, 8, d_model), F32),
            pltpu.VMEM((8, d_model), F32),
            sem((2,)), sem((3,)), sem((N_CHUNKS,)), sem((N_CHUNKS,)),
            sem, sem((SEG, PIECES)), sem, sem((SEG, PIECES)), sem, sem((SEG // 2, HELP)), sem, sem((SEG // 2, HELP)), sem, sem,
            sem, sem((N_CHUNKS,)), sem, sem((N_CHUNKS,)), sem, sem((N_CHUNKS,)), sem, sem((N_CHUNKS,)),
            sem, sem, sem, sem, sem, sem,
        ]
        any_spec = pl.BlockSpec(memory_space=pl.ANY)
        vmem_spec = pl.BlockSpec(memory_space=pltpu.VMEM)
        dw_up, dw_down, sums = pl.pallas_call(
            functools.partial(step_kernel, n_stages, loss_scale),
            out_shape=(jax.ShapeDtypeStruct(w_up.shape, F32), jax.ShapeDtypeStruct(w_down.shape, F32),
                       jax.ShapeDtypeStruct((16, d_model), F32)),
            in_specs=[any_spec, any_spec, any_spec, any_spec, vmem_spec],
            out_specs=(any_spec, any_spec, any_spec),
            scratch_shapes=scratch,
            compiler_params=pltpu.CompilerParams(collective_id=0, has_side_effects=True,
                                                 vmem_limit_bytes=67043328),
        )(x_in.reshape(n_rows, d_model), y_target.reshape(n_rows, d_model), w_up, w_down, norm_gain)
        return pl.pallas_call(
            functools.partial(write_kernel, WRITE_PARTS, loss_scale),
            out_shape=(jax.ShapeDtypeStruct(w_up.shape, F32), jax.ShapeDtypeStruct(w_down.shape, F32),
                       jax.ShapeDtypeStruct(norm_gain.shape, F32), jax.ShapeDtypeStruct((1,), F32)),
            in_specs=[any_spec, any_spec, any_spec],
            out_specs=(any_spec, any_spec, any_spec, any_spec),
            scratch_shapes=[pltpu.VMEM(w_up.shape[1:], F32), pltpu.VMEM(w_down.shape[1:], F32),
                            pltpu.VMEM((16, d_model), F32), pltpu.VMEM((1, d_model), F32), pltpu.SMEM((1,), F32),
                            sem((2, WRITE_PARTS)), sem((2, WRITE_PARTS)), sem((3,))],
        )(dw_up, dw_down, sums)

    return jax.shard_map(stage_body, mesh=mesh,
                         in_specs=(P('dp'), P('dp'), P('stage'), P('stage'), P('stage')),
                         out_specs=(P(('dp', 'stage')), P(('dp', 'stage')), P(('dp', 'stage')), P('dp')),
                         check_vma=False)
```

```python
import functools

import jax
import jax.numpy as jnp
from jax import lax
from jax.experimental import pallas as pl
from jax.experimental.pallas import tpu as pltpu
from jax.sharding import PartitionSpec as P

NORM_EPS = 1e-6
SEG = 8
N_CHUNKS = 4
PIECES = 8
HELP = 2
COLS = 256
BWD_COLS = 128
WEIGHT_COLS = 512
HALF = SEG // 2
GROUP = 4
LATE_ROWS = 2
WRITE_PARTS = 4
GELU_C = 0.7978845608028654
GELU_A = 0.044715
MESH = pl.DeviceIdType.MESH
F32 = jnp.float32
BF16 = jnp.bfloat16


def dot_nn(lhs, rhs):
    return lax.dot_general(lhs, rhs, (((1,), (0,)), ((), ())), preferred_element_type=F32)


def dot_nt(lhs, rhs):
    return lax.dot_general(lhs, rhs, (((1,), (1,)), ((), ())), preferred_element_type=F32)


def dot_tn(lhs, rhs):
    return lax.dot_general(lhs, rhs, (((0,), (0,)), ((), ())), preferred_element_type=F32)


def gelu_gate(hidden):
    sq = hidden * hidden
    gate = 0.5 + 0.5 * jnp.tanh(hidden * (GELU_C + (GELU_C * GELU_A) * sq))
    return gate, sq


def gelu_value(hidden):
    return hidden * gelu_gate(hidden)[0]


def gelu_slope(hidden, gate, sq):
    return gate + ((gate * (1.0 - gate)) * hidden) * (2.0 * GELU_C + (6.0 * GELU_C * GELU_A) * sq)


def inv_rms_of(x_float):
    return lax.rsqrt(jnp.mean(x_float * x_float, axis=-1, keepdims=True) + NORM_EPS)


def fold_rows(block):
    rows, cols = block.shape
    return jnp.sum(block.reshape(rows // 8, 8, cols), axis=0)


def step_kernel(n_stages, loss_scale,
                x_hbm, y_hbm, wu_hbm, wd_hbm, gain_ref,
                dwu_hbm, dwd_hbm, sums_hbm,
                wu, wd, help_u, help_d, gains, acts, grads, hiddens, act_stash, grad_stash, value_stash, slope_stash, targets, dwu, dwd_t, dwd, sums,
                dg_part, dg_stash, loss_part, loss_stash, loss_total,
                load_sem, out_sem, x_sem, y_sem, agu_send, agu_recv, agd_send, agd_recv, hu_send, hu_recv, hd_send, hd_recv, gain_send, gain_recv,
                as_send, as_recv, gs_send, gs_recv, fwd_send, fwd_recv, bwd_send, bwd_recv,
                dg_send, dg_recv, lrow_send, lrow_recv, lcol_send, lcol_recv):
    n_rows = n_stages // SEG
    n_chips = SEG // 2
    chunk = acts.shape[2]
    d_model = acts.shape[3]
    d_ff = wu.shape[2]
    me = lax.axis_index('stage')
    row = lax.div(me, SEG)
    r = lax.rem(me, SEG)
    chip = lax.div(r, 2)
    core = lax.rem(r, 2)
    row_base = row * SEG
    left = lax.rem(chip + n_chips - 1, n_chips) * 2 + core
    right = lax.rem(chip + 1, n_chips) * 2 + core
    across = lax.rem(chip + 2, n_chips) * 2 + core
    flip = 1 - 2 * core
    sib = r + flip

    def rcopy(src, dst, send_sem, recv_sem, dev):
        return pltpu.make_async_remote_copy(src_ref=src, dst_ref=dst, send_sem=send_sem, recv_sem=recv_sem,
                                            device_id={'stage': dev}, device_id_type=MESH)

    load_u = pltpu.make_async_copy(wu_hbm.at[0], wu.at[r], load_sem.at[0])
    load_d = pltpu.make_async_copy(wd_hbm.at[0], wd.at[r], load_sem.at[1])
    load_u.start()
    load_d.start()

    def x_load(k):
        first = pl.multiple_of((r * N_CHUNKS + k) * chunk, chunk)
        return pltpu.make_async_copy(x_hbm.at[pl.ds(first, chunk)], acts.at[0, k], x_sem.at[k])

    def y_load(k):
        first = pl.multiple_of((r * N_CHUNKS + k) * chunk, chunk)
        return pltpu.make_async_copy(y_hbm.at[pl.ds(first, chunk)], targets.at[k], y_sem.at[k])

    @pl.when(row == 0)
    def _():
        for k in range(N_CHUNKS):
            x_load(k).start()

    @pl.when(row == n_rows - 1)
    def _():
        for k in range(N_CHUNKS):
            y_load(k).start()

    gains[r] = jnp.broadcast_to(gain_ref[...], (8, d_model))
    dg_part[...] = jnp.zeros_like(dg_part)
    loss_part[...] = jnp.zeros_like(loss_part)

    with jax.named_scope('barrier'):
        barrier = pltpu.get_barrier_semaphore()
        for step in range(1, SEG):
            pl.semaphore_signal(barrier, inc=1, device_id={'stage': row_base + lax.rem(r + step, SEG)}, device_id_type=MESH)
        for step in range(1, n_rows):
            pl.semaphore_signal(barrier, inc=1, device_id={'stage': lax.rem(row + step, n_rows) * SEG + r}, device_id_type=MESH)
        pl.semaphore_wait(barrier, SEG - 1 + n_rows - 1)

    u_rows = d_model // PIECES
    d_rows = d_ff // PIECES
    helped = row < n_rows // 2
    partner = (n_rows - 1 - row) * SEG + r
    n_help = jnp.where((row == 0) | (row == n_rows - 1), HELP, HELP - 1)
    n_direct = PIECES - n_help
    n_ring = jnp.where(helped, n_direct, PIECES)
    chip_left, chip_right, chip_across = lax.div(left, 2), lax.div(right, 2), lax.div(across, 2)

    def each_piece(first, last, fn):
        def body(piece, carry):
            fn(piece)
            return carry
        lax.fori_loop(first, last, body, 0)

    def u_part(slot, piece):
        return wu.at[slot, pl.ds(pl.multiple_of(piece * u_rows, u_rows), u_rows)]

    def d_part(slot, piece):
        return wd.at[slot, pl.ds(pl.multiple_of(piece * d_rows, d_rows), d_rows)]

    def u_copy(slot, piece, dev):
        part = u_part(slot, piece)
        return rcopy(part, part, agu_send, agu_recv.at[slot, piece], row_base + dev)

    def d_copy(slot, piece, dev):
        part = d_part(slot, piece)
        return rcopy(part, part, agd_send, agd_recv.at[slot, piece], row_base + dev)

    def hu_copy(place, piece, dev):
        part = help_u.at[place, piece]
        return rcopy(part, part, hu_send, hu_recv.at[place, piece], row_base + dev)

    def hd_copy(place, piece, dev):
        part = help_d.at[place, piece]
        return rcopy(part, part, hd_send, hd_recv.at[place, piece], row_base + dev)

    def hu_give(piece):
        rcopy(u_part(r, n_direct + piece), help_u.at[chip, piece], agu_send, hu_recv.at[chip, piece], partner).start()

    def hd_give(piece):
        rcopy(d_part(r, n_direct + piece), help_d.at[chip, piece], agd_send, hd_recv.at[chip, piece], partner).start()

    def hu_return(place, piece):
        slot = place * 2 + core
        rcopy(help_u.at[place, piece], u_part(slot, n_direct + piece), hu_send, agu_recv.at[slot, n_direct + piece], partner).start()

    def hd_return(place, piece):
        slot = place * 2 + core
        rcopy(help_d.at[place, piece], d_part(slot, n_direct + piece), hd_send, agd_recv.at[slot, n_direct + piece], partner).start()

    with jax.named_scope('w_load_u'):
        load_u.wait()
    with jax.named_scope('w_load_d'):
        load_d.wait()
    def ring_first(piece):
        u_copy(r, piece, right).start()
        d_copy(r, piece, left).start()

    def ring_second(piece):
        d_copy(r, piece, right).start()
        u_copy(r, piece, left).start()

    def give(piece):
        hu_give(piece)
        hd_give(piece)

    @pl.when(helped)
    def _():
        each_piece(0, n_help, give)
        each_piece(0, n_direct, ring_first)
        each_piece(0, n_direct, ring_second)

    @pl.when(jnp.logical_not(helped))
    def _():
        each_piece(0, PIECES // 2, ring_first)

    def own_to_sib(piece):
        u_copy(r, piece, sib).start()
        d_copy(r, piece, sib).start()
    each_piece(0, PIECES, own_to_sib)
    for step in range(1, SEG):
        rcopy(gains.at[r], gains.at[r], gain_send, gain_recv, row_base + lax.rem(r + step, SEG)).start()

    @pl.when(jnp.logical_not(helped))
    def _():
        def spread(piece):
            hu_copy(chip, piece, r).wait_recv()
            hu_copy(chip, piece, right).start()
            hu_copy(chip, piece, left).start()
            hd_copy(chip, piece, r).wait_recv()
            hd_copy(chip, piece, left).start()
            hd_copy(chip, piece, right).start()

        def relay(piece):
            hu_copy(chip_left, piece, r).wait_recv()
            hu_copy(chip_left, piece, right).start()
            hu_return(chip_left, piece)
            hd_copy(chip_right, piece, r).wait_recv()
            hd_copy(chip_right, piece, left).start()
            hd_return(chip_right, piece)

        def near(piece):
            hd_copy(chip_left, piece, r).wait_recv()
            hd_return(chip_left, piece)
            hu_copy(chip_right, piece, r).wait_recv()
            hu_return(chip_right, piece)

        def far(piece):
            hu_copy(chip_across, piece, r).wait_recv()
            hu_return(chip_across, piece)
            hd_copy(chip_across, piece, r).wait_recv()
            hd_return(chip_across, piece)

        with jax.named_scope('help'):
            each_piece(0, n_help, spread)
            each_piece(0, n_help, relay)
            each_piece(PIECES // 2, PIECES, ring_first)
            each_piece(0, PIECES, ring_second)
            each_piece(0, n_help, near)
            each_piece(0, n_help, far)

    def relay_near(piece):
        u_copy(left, piece, r).wait_recv()
        u_copy(left, piece, right).start()
        u_copy(left, piece, sib).start()
        d_copy(right, piece, r).wait_recv()
        d_copy(right, piece, left).start()
        d_copy(right, piece, sib).start()

    def take_near(piece):
        d_copy(left, piece, r).wait_recv()
        d_copy(left, piece, sib).start()
        u_copy(right, piece, r).wait_recv()
        u_copy(right, piece, sib).start()

    def take_across(piece):
        u_copy(across, piece, r).wait_recv()
        u_copy(across, piece, sib).start()
        d_copy(across, piece, r).wait_recv()
        d_copy(across, piece, sib).start()

    def take_help(piece):
        for slot in (left, right, across):
            u_copy(slot, piece, r).wait_recv()
            u_copy(slot, piece, sib).start()
            d_copy(slot, piece, r).wait_recv()
            d_copy(slot, piece, sib).start()

    def take_sib(piece):
        for slot in (sib, left + flip, right + flip, across + flip):
            u_copy(slot, piece, r).wait_recv()
            d_copy(slot, piece, r).wait_recv()

    with jax.named_scope('ag_first'):
        each_piece(0, n_ring, relay_near)
    with jax.named_scope('ag_second'):
        each_piece(0, n_ring, take_near)
    with jax.named_scope('ag_across'):
        each_piece(0, n_ring, take_across)
    with jax.named_scope('ag_help'):
        each_piece(n_ring, PIECES, take_help)
    with jax.named_scope('ag_sib'):
        each_piece(0, PIECES, take_sib)
    rcopy(gains.at[pl.ds(0, SEG - 1)], gains.at[pl.ds(0, SEG - 1)], gain_send, gain_recv, me).wait_recv()

    def act_ship(layer, k):
        mine = layer == r
        return rcopy(acts.at[layer, k], act_stash.at[k, jnp.where(mine, SEG, r)], as_send, as_recv.at[k],
                     row_base + jnp.where(mine, sib, layer))

    def grad_ship(layer, k):
        mine = layer == r
        return rcopy(grads.at[layer + 1, k], grad_stash.at[k, jnp.where(mine, SEG, r)], gs_send, gs_recv.at[k],
                     row_base + jnp.where(mine, sib, layer))

    def fwd_layer(layer, k):
        x_float = acts[layer, k].astype(F32)
        normed = (x_float * inv_rms_of(x_float) * gains[layer, 0:1, :]).astype(BF16)
        out = x_float
        for part in range(0, d_ff, COLS):
            cols = slice(part, part + COLS)
            hidden = dot_nn(normed, wu[layer, :, cols])
            hiddens[layer, k, :, cols] = hidden
            out += dot_nn(gelu_value(hidden).astype(BF16), wd[layer, cols, :])
        acts[layer + 1, k] = out.astype(BF16)

    def fwd_input_wait(k):
        @pl.when(row == 0)
        def _():
            x_load(k).wait()

        @pl.when(row > 0)
        def _():
            with jax.named_scope('fwd_wait'):
                rcopy(acts.at[0, k], acts.at[0, k], fwd_send, fwd_recv.at[k], me).wait_recv()

    def top_grad(k):
        y_load(k).wait()
        error_val = acts[SEG, k].astype(F32) - targets[k].astype(F32)
        loss_part[...] += fold_rows(error_val * error_val)
        grads[SEG, k] = ((2.0 * loss_scale) * error_val).astype(BF16)

    def fwd_group(group, k):
        for step in range(GROUP):
            fwd_layer(group * GROUP + step, k)
        return k

    def fwd_chunk(k, carry):
        fwd_input_wait(k)
        with jax.named_scope('fwd_layers'):
            lax.fori_loop(0, SEG // GROUP, fwd_group, k)

        @pl.when(row < n_rows - 1)
        def _():
            rcopy(acts.at[SEG, k], acts.at[0, k], fwd_send, fwd_recv.at[k], me + SEG).start()
        for layer in range(SEG):
            act_ship(layer, k).start()

        @pl.when(row == n_rows - 1)
        def _():
            top_grad(k)
        return carry

    lax.fori_loop(0, jnp.where(row == n_rows - 1, 1, N_CHUNKS), fwd_chunk, 0)

    def bwd_layer(step, k, joined):
        layer = SEG - 1 - step
        grad_out = grads[layer + 1, k]
        x_float = acts[layer, k].astype(F32)
        inv_rms = inv_rms_of(x_float)
        x_hat = x_float * inv_rms
        gain = gains[layer, 0:1, :]
        grad_normed = 0.0
        pieces = []
        for part in range(0, d_ff, BWD_COLS):
            cols = slice(part, part + BWD_COLS)
            hidden = hiddens[layer, k, :, cols]
            slope = gelu_slope(hidden, *gelu_gate(hidden))
            grad_gelu = dot_nt(grad_out, wd[layer, cols, :]).astype(BF16).astype(F32)
            pieces.append((grad_gelu * slope).astype(BF16))
            if not joined:
                grad_normed += dot_nt(pieces[-1], wu[layer, :, cols])
        if joined:
            grad_normed = dot_nt(jnp.concatenate(pieces, axis=1), wu[layer])
        grad_normed = grad_normed.astype(BF16).astype(F32)
        dg_part[layer] += fold_rows(grad_normed * x_hat)
        grad_hat = grad_normed * gain
        mean_dot = jnp.mean(grad_hat * x_hat, axis=-1, keepdims=True)
        grad_x = inv_rms * (grad_hat - x_hat * mean_dot)
        grads[layer, k] = (grad_out.astype(F32) + grad_x).astype(BF16)

    def bwd_group(group, k):
        for step in range(GROUP):
            bwd_layer(group * GROUP + step, k, joined=True)

        @pl.when((row > 0) & (group == SEG // GROUP - 1))
        def _():
            rcopy(grads.at[0, k], grads.at[SEG, k], bwd_send, bwd_recv.at[k], me - SEG).start()
        for step in range(GROUP):
            grad_ship(SEG - 1 - group * GROUP - step, k).start()
        return k

    def both_group(group, k):
        for step in range(GROUP):
            bwd_layer(group * GROUP + step, k - 1, joined=False)
            fwd_layer(group * GROUP + step, k)

        @pl.when((row > 0) & (group == SEG // GROUP - 1))
        def _():
            rcopy(grads.at[0, k - 1], grads.at[SEG, k - 1], bwd_send, bwd_recv.at[k - 1], me - SEG).start()
        for step in range(GROUP):
            grad_ship(SEG - 1 - group * GROUP - step, k - 1).start()
        return k

    def both_chunks(k, carry):
        fwd_input_wait(k)
        with jax.named_scope('both_layers'):
            lax.fori_loop(0, SEG // GROUP, both_group, k)
        top_grad(k)
        for layer in range(SEG):
            act_ship(layer, k).start()
        return carry

    @pl.when(row == n_rows - 1)
    def _():
        lax.fori_loop(1, N_CHUNKS, both_chunks, 0)
        loss_stash[r] = loss_part[...]
        for step in range(1, SEG):
            rcopy(loss_stash.at[r], loss_stash.at[r], lrow_send, lrow_recv, row_base + lax.rem(r + step, SEG)).start()

    rest = act_stash.at[0, pl.ds(0, SEG)]
    all_rest = acts.at[pl.ds(0, SEG)]

    def owner_block(index):
        return lax.div(index, 2), pl.ds(lax.rem(index, 2) * HALF, HALF)

    def value_block(index, carry):
        k, srcs = owner_block(index)

        @pl.when(lax.rem(index, 2) == 0)
        def _():
            with jax.named_scope('as_wait'):
                rcopy(rest, rest, as_send, as_recv.at[k], me).wait_recv()
            act_stash[k, r] = acts[r, k]
        x_float = act_stash[k, srcs].reshape(HALF * chunk, d_model).astype(F32)
        normed = (x_float * inv_rms_of(x_float) * gains[r, 0:1, :]).astype(BF16)
        act_stash[k, srcs] = normed.reshape(HALF, chunk, d_model)
        for part in range(0, d_ff, COLS):
            cols = slice(part, part + COLS)
            hidden = dot_nn(normed, wu[r, :, cols])
            gate, sq = gelu_gate(hidden)
            value_stash[k, srcs, :, cols] = (hidden * gate).astype(BF16).reshape(HALF, chunk, COLS)
            slope_stash[k, srcs, :, cols] = gelu_slope(hidden, gate, sq).reshape(HALF, chunk, COLS)
        return carry

    def sent_own(piece):
        rcopy(u_part(r, 0), u_part(r, 0), agu_send, gain_recv, me).wait_send()
        rcopy(d_part(r, 0), d_part(r, 0), agd_send, gain_recv, me).wait_send()

    def sent_help(piece):
        rcopy(help_u.at[0, 0], help_u.at[0, 0], hu_send, gain_recv, me).wait_send()
        rcopy(help_d.at[0, 0], help_d.at[0, 0], hd_send, gain_recv, me).wait_send()

    def value_phase():
        dwu[...] = jnp.zeros_like(dwu)
        dwd_t[...] = jnp.zeros_like(dwd_t)
        with jax.named_scope('value_blocks'):
            lax.fori_loop(0, 2 * N_CHUNKS, value_block, 0)
        each_piece(0, jnp.where(helped, 3 * n_direct + n_help + 4 * PIECES, 7 * PIECES), sent_own)
        each_piece(0, jnp.where(helped, 0, 6 * n_help), sent_help)
        rest_gain = gains.at[pl.ds(0, SEG - 1)]
        rcopy(rest_gain, rest_gain, gain_send, gain_recv, me).wait_send()
        rcopy(all_rest, all_rest, as_send, dg_recv, me).wait_send()

        @pl.when(row < n_rows - 1)
        def _():
            rcopy(acts.at[0], acts.at[0], fwd_send, dg_recv, me).wait_send()

    @pl.when(row < n_rows - LATE_ROWS)
    def _():
        value_phase()

    def weight_block(k, carry):
        rows = SEG * chunk
        with jax.named_scope('gs_wait'):
            rcopy(rest, rest, gs_send, gs_recv.at[k], me).wait_recv()
        grad_stash[k, r] = grads[r + 1, k]
        normed = act_stash[k, pl.ds(0, SEG)].reshape(rows, d_model)
        grad_out = grad_stash[k, pl.ds(0, SEG)].reshape(rows, d_model)
        for part in range(0, d_ff, WEIGHT_COLS):
            cols = slice(part, part + WEIGHT_COLS)
            dwd_t[:, cols] += dot_tn(grad_out, value_stash[k, :, :, cols].reshape(rows, WEIGHT_COLS))
            grad_gelu = dot_nt(grad_out, wd[r, cols, :]).astype(BF16).astype(F32)
            grad_hidden = (grad_gelu * slope_stash[k, :, :, cols].reshape(rows, WEIGHT_COLS)).astype(BF16)
            dwu[:, cols] += dot_tn(normed, grad_hidden)
        return carry

    def bwd_chunk(k, carry):
        @pl.when(row < n_rows - 1)
        def _():
            with jax.named_scope('bwd_wait'):
                rcopy(grads.at[SEG, k], grads.at[SEG, k], bwd_send, bwd_recv.at[k], me).wait_recv()

        with jax.named_scope('bwd_layers'):
            lax.fori_loop(0, SEG // GROUP, bwd_group, k)
        return carry

    lax.fori_loop(jnp.where(row == n_rows - 1, N_CHUNKS - 1, 0), N_CHUNKS, bwd_chunk, 0)

    def dg_ship(layer):
        return rcopy(dg_part.at[layer], dg_stash.at[r], dg_send, dg_recv, row_base + layer)

    for step in range(1, SEG):
        dg_ship(lax.rem(r + step, SEG)).start()
    dg_stash[r] = dg_part[r]

    @pl.when(row >= n_rows - LATE_ROWS)
    def _():
        value_phase()

    with jax.named_scope('weight_blocks'):
        lax.fori_loop(0, N_CHUNKS, weight_block, 0)
    @pl.when(row == n_rows - 1)
    def _():
        rest_row = loss_stash.at[pl.ds(0, SEG - 1)]
        rcopy(rest_row, rest_row, lrow_send, lrow_recv, me).wait_recv()
        loss_total[...] = jnp.sum(loss_stash[...], axis=0)
        for step in range(1, n_rows):
            rcopy(loss_total, loss_total, lcol_send, lcol_recv, me - step * SEG).start()

    with jax.named_scope('turn'):
        up_out = pltpu.make_async_copy(dwu, dwu_hbm.at[0], out_sem.at[0])
        up_out.start()
        dwd[...] = dwd_t[...].T
        down_out = pltpu.make_async_copy(dwd, dwd_hbm.at[0], out_sem.at[1])
        down_out.start()

    rest_dg = dg_stash.at[pl.ds(0, SEG - 1)]
    with jax.named_scope('dg_wait'):
        rcopy(rest_dg, rest_dg, dg_send, dg_recv, me).wait_recv()
    sums[0:8] = jnp.sum(dg_stash[...], axis=0)

    @pl.when(row < n_rows - 1)
    def _():
        rcopy(loss_total, loss_total, lcol_send, lcol_recv, me).wait_recv()
    sums[8:16] = loss_total[...]
    sums_out = pltpu.make_async_copy(sums, sums_hbm, out_sem.at[2])
    sums_out.start()

    rcopy(all_rest, all_rest, gs_send, dg_recv, me).wait_send()
    rcopy(rest_dg, rest_dg, dg_send, dg_recv, me).wait_send()

    @pl.when(row > 0)
    def _():
        rcopy(grads.at[0], grads.at[0], bwd_send, dg_recv, me).wait_send()

    @pl.when(row == n_rows - 1)
    def _():
        rest_row = loss_stash.at[pl.ds(0, SEG - 1)]
        rcopy(rest_row, rest_row, lrow_send, lrow_recv, me).wait_send()
        for step in range(1, n_rows):
            rcopy(loss_total, loss_total, lcol_send, lcol_recv, me).wait_send()
    up_out.wait()
    down_out.wait()
    sums_out.wait()


def write_kernel(n_parts, loss_scale, up_hbm, down_hbm, sums_hbm, up_out, down_out, gain_out, loss_out,
                 up_buf, down_buf, sums_buf, gain_buf, loss_buf, in_sem, out_sem, small_sem):
    pairs = ((up_hbm, up_buf, up_out), (down_hbm, down_buf, down_out))

    def part(ref, index):
        rows = ref.shape[0] // n_parts
        return ref.at[pl.ds(index * rows, rows)]

    sums_read = pltpu.make_async_copy(sums_hbm, sums_buf, small_sem.at[0])
    gain_write = pltpu.make_async_copy(gain_buf, gain_out, small_sem.at[1])
    loss_write = pltpu.make_async_copy(loss_buf, loss_out, small_sem.at[2])
    sums_read.start()
    reads, writes = [], []
    for side, (src, buf, dst) in enumerate(pairs):
        for index in range(n_parts):
            reads.append(pltpu.make_async_copy(part(src.at[0], index), part(buf, index), in_sem.at[side, index]))
            writes.append(pltpu.make_async_copy(part(buf, index), part(dst.at[0], index), out_sem.at[side, index]))
    for read in reads:
        read.start()
    sums_read.wait()
    gain_buf[...] = jnp.sum(sums_buf[0:8], axis=0, keepdims=True)
    loss_buf[0] = jnp.sum(sums_buf[8:16]) * loss_scale
    for read, write in zip(reads, writes):
        read.wait()
        write.start()
    gain_write.start()
    loss_write.start()
    for write in writes:
        write.wait()
    gain_write.wait()
    loss_write.wait()


def solution(mesh):
    n_stages = mesh.shape['stage']

    def stage_body(x_in, y_target, w_up, w_down, norm_gain):
        n_micro, n_tok, d_model = x_in.shape
        d_ff = w_up.shape[2]
        n_rows = n_micro * n_tok
        chunk = n_rows // SEG // N_CHUNKS
        loss_scale = 1.0 / (n_rows * d_model)
        sem = pltpu.SemaphoreType.DMA
        act_shape = (N_CHUNKS, chunk, d_model)
        scratch = [
            pltpu.VMEM((SEG, d_model, d_ff), BF16),
            pltpu.VMEM((SEG, d_ff, d_model), BF16),
            pltpu.VMEM((SEG // 2, HELP, d_model // PIECES, d_ff), BF16),
            pltpu.VMEM((SEG // 2, HELP, d_ff // PIECES, d_model), BF16),
            pltpu.VMEM((SEG, 8, d_model), F32),
            pltpu.VMEM((SEG + 1,) + act_shape, BF16),
            pltpu.VMEM((SEG + 1,) + act_shape, BF16),
            pltpu.VMEM((SEG, N_CHUNKS, chunk, d_ff), F32),
            pltpu.VMEM((N_CHUNKS, SEG + 1, chunk, d_model), BF16),
            pltpu.VMEM((N_CHUNKS, SEG + 1, chunk, d_model), BF16),
            pltpu.VMEM((N_CHUNKS, SEG, chunk, d_ff), BF16),
            pltpu.VMEM((N_CHUNKS, SEG, chunk, d_ff), F32),
            pltpu.VMEM(act_shape, BF16),
            pltpu.VMEM((d_model, d_ff), F32),
            pltpu.VMEM((d_model, d_ff), F32),
            pltpu.VMEM((d_ff, d_model), F32),
            pltpu.VMEM((16, d_model), F32),
            pltpu.VMEM((SEG, 8, d_model), F32),
            pltpu.VMEM((SEG, 8, d_model), F32),
            pltpu.VMEM((8, d_model), F32),
            pltpu.VMEM((SEG, 8, d_model), F32),
            pltpu.VMEM((8, d_model), F32),
            sem((2,)), sem((3,)), sem((N_CHUNKS,)), sem((N_CHUNKS,)),
            sem, sem((SEG, PIECES)), sem, sem((SEG, PIECES)), sem, sem((SEG // 2, HELP)), sem, sem((SEG // 2, HELP)), sem, sem,
            sem, sem((N_CHUNKS,)), sem, sem((N_CHUNKS,)), sem, sem((N_CHUNKS,)), sem, sem((N_CHUNKS,)),
            sem, sem, sem, sem, sem, sem,
        ]
        any_spec = pl.BlockSpec(memory_space=pl.ANY)
        vmem_spec = pl.BlockSpec(memory_space=pltpu.VMEM)
        dw_up, dw_down, sums = pl.pallas_call(
            functools.partial(step_kernel, n_stages, loss_scale),
            out_shape=(jax.ShapeDtypeStruct(w_up.shape, F32), jax.ShapeDtypeStruct(w_down.shape, F32),
                       jax.ShapeDtypeStruct((16, d_model), F32)),
            in_specs=[any_spec, any_spec, any_spec, any_spec, vmem_spec],
            out_specs=(any_spec, any_spec, any_spec),
            scratch_shapes=scratch,
            compiler_params=pltpu.CompilerParams(collective_id=0, has_side_effects=True,
                                                 vmem_limit_bytes=67043328),
        )(x_in.reshape(n_rows, d_model), y_target.reshape(n_rows, d_model), w_up, w_down, norm_gain)
        return pl.pallas_call(
            functools.partial(write_kernel, WRITE_PARTS, loss_scale),
            out_shape=(jax.ShapeDtypeStruct(w_up.shape, F32), jax.ShapeDtypeStruct(w_down.shape, F32),
                       jax.ShapeDtypeStruct(norm_gain.shape, F32), jax.ShapeDtypeStruct((1,), F32)),
            in_specs=[any_spec, any_spec, any_spec],
            out_specs=(any_spec, any_spec, any_spec, any_spec),
            scratch_shapes=[pltpu.VMEM(w_up.shape[1:], F32), pltpu.VMEM(w_down.shape[1:], F32),
                            pltpu.VMEM((16, d_model), F32), pltpu.VMEM((1, d_model), F32), pltpu.SMEM((1,), F32),
                            sem((2, WRITE_PARTS)), sem((2, WRITE_PARTS)), sem((3,))],
        )(dw_up, dw_down, sums)

    return jax.shard_map(stage_body, mesh=mesh,
                         in_specs=(P('dp'), P('dp'), P('stage'), P('stage'), P('stage')),
                         out_specs=(P(('dp', 'stage')), P(('dp', 'stage')), P(('dp', 'stage')), P('dp')),
                         check_vma=False)
```

```python
import functools

import jax
import jax.numpy as jnp
from jax import lax
from jax.experimental import pallas as pl
from jax.experimental.pallas import tpu as pltpu
from jax.sharding import PartitionSpec as P

NORM_EPS = 1e-6
SEG = 8
N_CHUNKS = 4
PIECES = 8
HELP = 2
COLS = 256
FWD_COLS = 256
BWD_COLS = 128
WEIGHT_COLS = 512
HALF = SEG // 2
GROUP = 4
LATE_ROWS = 2
WRITE_PARTS = 4
GELU_C = 0.7978845608028654
GELU_A = 0.044715
MESH = pl.DeviceIdType.MESH
F32 = jnp.float32
BF16 = jnp.bfloat16


def dot_nn(lhs, rhs):
    return lax.dot_general(lhs, rhs, (((1,), (0,)), ((), ())), preferred_element_type=F32)


def dot_nt(lhs, rhs):
    return lax.dot_general(lhs, rhs, (((1,), (1,)), ((), ())), preferred_element_type=F32)


def dot_tn(lhs, rhs):
    return lax.dot_general(lhs, rhs, (((0,), (0,)), ((), ())), preferred_element_type=F32)


def gelu_gate(hidden):
    sq = hidden * hidden
    gate = 0.5 + 0.5 * jnp.tanh(hidden * (GELU_C + (GELU_C * GELU_A) * sq))
    return gate, sq


def gelu_value(hidden):
    return hidden * gelu_gate(hidden)[0]


def gelu_slope(hidden, gate, sq):
    return gate + ((gate * (1.0 - gate)) * hidden) * (2.0 * GELU_C + (6.0 * GELU_C * GELU_A) * sq)


def inv_rms_of(x_float):
    return lax.rsqrt(jnp.mean(x_float * x_float, axis=-1, keepdims=True) + NORM_EPS)


def fold_rows(block):
    rows, cols = block.shape
    return jnp.sum(block.reshape(rows // 8, 8, cols), axis=0)


def step_kernel(n_stages, loss_scale,
                x_hbm, y_hbm, wu_hbm, wd_hbm, gain_ref,
                dwu_hbm, dwd_hbm, sums_hbm,
                wu, wd, help_u, help_d, gains, acts, grads, hiddens, act_stash, grad_stash, value_stash, slope_stash, targets, dwu, dwd_t, dwd, sums,
                dg_part, dg_stash, loss_part, loss_stash, loss_total,
                load_sem, out_sem, x_sem, y_sem, agu_send, agu_recv, agd_send, agd_recv, hu_send, hu_recv, hd_send, hd_recv, gain_send, gain_recv,
                as_send, as_recv, gs_send, gs_recv, fwd_send, fwd_recv, bwd_send, bwd_recv,
                dg_send, dg_recv, lrow_send, lrow_recv, lcol_send, lcol_recv):
    n_rows = n_stages // SEG
    n_chips = SEG // 2
    chunk = acts.shape[2]
    d_model = acts.shape[3]
    d_ff = wu.shape[2]
    me = lax.axis_index('stage')
    row = lax.div(me, SEG)
    r = lax.rem(me, SEG)
    chip = lax.div(r, 2)
    core = lax.rem(r, 2)
    row_base = row * SEG
    left = lax.rem(chip + n_chips - 1, n_chips) * 2 + core
    right = lax.rem(chip + 1, n_chips) * 2 + core
    across = lax.rem(chip + 2, n_chips) * 2 + core
    flip = 1 - 2 * core
    sib = r + flip

    def rcopy(src, dst, send_sem, recv_sem, dev):
        return pltpu.make_async_remote_copy(src_ref=src, dst_ref=dst, send_sem=send_sem, recv_sem=recv_sem,
                                            device_id={'stage': dev}, device_id_type=MESH)

    load_u = pltpu.make_async_copy(wu_hbm.at[0], wu.at[r], load_sem.at[0])
    load_d = pltpu.make_async_copy(wd_hbm.at[0], wd.at[r], load_sem.at[1])
    load_u.start()
    load_d.start()

    def x_load(k):
        first = pl.multiple_of((r * N_CHUNKS + k) * chunk, chunk)
        return pltpu.make_async_copy(x_hbm.at[pl.ds(first, chunk)], acts.at[0, k], x_sem.at[k])

    def y_load(k):
        first = pl.multiple_of((r * N_CHUNKS + k) * chunk, chunk)
        return pltpu.make_async_copy(y_hbm.at[pl.ds(first, chunk)], targets.at[k], y_sem.at[k])

    @pl.when(row == 0)
    def _():
        for k in range(N_CHUNKS):
            x_load(k).start()

    @pl.when(row == n_rows - 1)
    def _():
        for k in range(N_CHUNKS):
            y_load(k).start()

    gains[r] = jnp.broadcast_to(gain_ref[...], (8, d_model))
    dg_part[...] = jnp.zeros_like(dg_part)
    loss_part[...] = jnp.zeros_like(loss_part)

    with jax.named_scope('barrier'):
        barrier = pltpu.get_barrier_semaphore()
        for step in range(1, SEG):
            pl.semaphore_signal(barrier, inc=1, device_id={'stage': row_base + lax.rem(r + step, SEG)}, device_id_type=MESH)
        for step in range(1, n_rows):
            pl.semaphore_signal(barrier, inc=1, device_id={'stage': lax.rem(row + step, n_rows) * SEG + r}, device_id_type=MESH)
        pl.semaphore_wait(barrier, SEG - 1 + n_rows - 1)

    u_rows = d_model // PIECES
    d_rows = d_ff // PIECES
    helped = row < n_rows // 2
    partner = (n_rows - 1 - row) * SEG + r
    n_help = jnp.where((row == 0) | (row == n_rows - 1), HELP, HELP - 1)
    n_direct = PIECES - n_help
    n_ring = jnp.where(helped, n_direct, PIECES)
    chip_left, chip_right, chip_across = lax.div(left, 2), lax.div(right, 2), lax.div(across, 2)

    def each_piece(first, last, fn):
        def body(piece, carry):
            fn(piece)
            return carry
        lax.fori_loop(first, last, body, 0)

    def u_part(slot, piece):
        return wu.at[slot, pl.ds(pl.multiple_of(piece * u_rows, u_rows), u_rows)]

    def d_part(slot, piece):
        return wd.at[slot, pl.ds(pl.multiple_of(piece * d_rows, d_rows), d_rows)]

    def u_copy(slot, piece, dev):
        part = u_part(slot, piece)
        return rcopy(part, part, agu_send, agu_recv.at[slot, piece], row_base + dev)

    def d_copy(slot, piece, dev):
        part = d_part(slot, piece)
        return rcopy(part, part, agd_send, agd_recv.at[slot, piece], row_base + dev)

    def hu_copy(place, piece, dev):
        part = help_u.at[place, piece]
        return rcopy(part, part, hu_send, hu_recv.at[place, piece], row_base + dev)

    def hd_copy(place, piece, dev):
        part = help_d.at[place, piece]
        return rcopy(part, part, hd_send, hd_recv.at[place, piece], row_base + dev)

    def hu_give(piece):
        rcopy(u_part(r, n_direct + piece), help_u.at[chip, piece], agu_send, hu_recv.at[chip, piece], partner).start()

    def hd_give(piece):
        rcopy(d_part(r, n_direct + piece), help_d.at[chip, piece], agd_send, hd_recv.at[chip, piece], partner).start()

    def hu_return(place, piece):
        slot = place * 2 + core
        rcopy(help_u.at[place, piece], u_part(slot, n_direct + piece), hu_send, agu_recv.at[slot, n_direct + piece], partner).start()

    def hd_return(place, piece):
        slot = place * 2 + core
        rcopy(help_d.at[place, piece], d_part(slot, n_direct + piece), hd_send, agd_recv.at[slot, n_direct + piece], partner).start()

    with jax.named_scope('w_load_u'):
        load_u.wait()
    with jax.named_scope('w_load_d'):
        load_d.wait()
    def ring_first(piece):
        u_copy(r, piece, right).start()
        d_copy(r, piece, left).start()

    def ring_second(piece):
        d_copy(r, piece, right).start()
        u_copy(r, piece, left).start()

    def give(piece):
        hu_give(piece)
        hd_give(piece)

    @pl.when(helped)
    def _():
        each_piece(0, n_help, give)
        each_piece(0, n_direct, ring_first)
        each_piece(0, n_direct, ring_second)

    @pl.when(jnp.logical_not(helped))
    def _():
        each_piece(0, PIECES // 2, ring_first)

    def own_to_sib(piece):
        u_copy(r, piece, sib).start()
        d_copy(r, piece, sib).start()
    each_piece(0, PIECES, own_to_sib)
    for step in range(1, SEG):
        rcopy(gains.at[r], gains.at[r], gain_send, gain_recv, row_base + lax.rem(r + step, SEG)).start()

    @pl.when(jnp.logical_not(helped))
    def _():
        def spread(piece):
            hu_copy(chip, piece, r).wait_recv()
            hu_copy(chip, piece, right).start()
            hu_copy(chip, piece, left).start()
            hd_copy(chip, piece, r).wait_recv()
            hd_copy(chip, piece, left).start()
            hd_copy(chip, piece, right).start()

        def relay(piece):
            hu_copy(chip_left, piece, r).wait_recv()
            hu_copy(chip_left, piece, right).start()
            hu_return(chip_left, piece)
            hd_copy(chip_right, piece, r).wait_recv()
            hd_copy(chip_right, piece, left).start()
            hd_return(chip_right, piece)

        def near(piece):
            hd_copy(chip_left, piece, r).wait_recv()
            hd_return(chip_left, piece)
            hu_copy(chip_right, piece, r).wait_recv()
            hu_return(chip_right, piece)

        def far(piece):
            hu_copy(chip_across, piece, r).wait_recv()
            hu_return(chip_across, piece)
            hd_copy(chip_across, piece, r).wait_recv()
            hd_return(chip_across, piece)

        with jax.named_scope('help'):
            each_piece(0, n_help, spread)
            each_piece(0, n_help, relay)
            each_piece(PIECES // 2, PIECES, ring_first)
            each_piece(0, PIECES, ring_second)
            each_piece(0, n_help, near)
            each_piece(0, n_help, far)

    def relay_near(piece):
        u_copy(left, piece, r).wait_recv()
        u_copy(left, piece, right).start()
        u_copy(left, piece, sib).start()
        d_copy(right, piece, r).wait_recv()
        d_copy(right, piece, left).start()
        d_copy(right, piece, sib).start()

    def take_near(piece):
        d_copy(left, piece, r).wait_recv()
        d_copy(left, piece, sib).start()
        u_copy(right, piece, r).wait_recv()
        u_copy(right, piece, sib).start()

    def take_across(piece):
        u_copy(across, piece, r).wait_recv()
        u_copy(across, piece, sib).start()
        d_copy(across, piece, r).wait_recv()
        d_copy(across, piece, sib).start()

    def take_help(piece):
        for slot in (left, right, across):
            u_copy(slot, piece, r).wait_recv()
            u_copy(slot, piece, sib).start()
            d_copy(slot, piece, r).wait_recv()
            d_copy(slot, piece, sib).start()

    def take_sib(piece):
        for slot in (sib, left + flip, right + flip, across + flip):
            u_copy(slot, piece, r).wait_recv()
            d_copy(slot, piece, r).wait_recv()

    with jax.named_scope('ag_first'):
        each_piece(0, n_ring, relay_near)
    with jax.named_scope('ag_second'):
        each_piece(0, n_ring, take_near)
    with jax.named_scope('ag_across'):
        each_piece(0, n_ring, take_across)
    with jax.named_scope('ag_help'):
        each_piece(n_ring, PIECES, take_help)
    with jax.named_scope('ag_sib'):
        each_piece(0, PIECES, take_sib)
    rcopy(gains.at[pl.ds(0, SEG - 1)], gains.at[pl.ds(0, SEG - 1)], gain_send, gain_recv, me).wait_recv()

    def act_ship(layer, k):
        mine = layer == r
        return rcopy(acts.at[layer, k], act_stash.at[k, jnp.where(mine, SEG, r)], as_send, as_recv.at[k],
                     row_base + jnp.where(mine, sib, layer))

    def grad_ship(layer, k):
        mine = layer == r
        return rcopy(grads.at[layer + 1, k], grad_stash.at[k, jnp.where(mine, SEG, r)], gs_send, gs_recv.at[k],
                     row_base + jnp.where(mine, sib, layer))

    def fwd_layer(layer, k, joined):
        x_float = acts[layer, k].astype(F32)
        normed = (x_float * inv_rms_of(x_float) * gains[layer, 0:1, :]).astype(BF16)
        values = []
        update = 0.0
        for part in range(0, d_ff, FWD_COLS):
            cols = slice(part, part + FWD_COLS)
            hidden = dot_nn(normed, wu[layer, :, cols])
            hiddens[layer, k, :, cols] = hidden
            values.append(gelu_value(hidden).astype(BF16))
            if not joined:
                update += dot_nn(values[-1], wd[layer, cols, :])
        if joined:
            update = dot_nn(jnp.concatenate(values, axis=1), wd[layer])
        acts[layer + 1, k] = (x_float + update).astype(BF16)

    def fwd_input_wait(k):
        @pl.when(row == 0)
        def _():
            x_load(k).wait()

        @pl.when(row > 0)
        def _():
            with jax.named_scope('fwd_wait'):
                rcopy(acts.at[0, k], acts.at[0, k], fwd_send, fwd_recv.at[k], me).wait_recv()

    def top_grad(k):
        y_load(k).wait()
        error_val = acts[SEG, k].astype(F32) - targets[k].astype(F32)
        loss_part[...] += fold_rows(error_val * error_val)
        grads[SEG, k] = ((2.0 * loss_scale) * error_val).astype(BF16)

    def fwd_group(group, k):
        for step in range(GROUP):
            fwd_layer(group * GROUP + step, k, joined=True)
        return k

    def fwd_chunk(k, carry):
        fwd_input_wait(k)
        with jax.named_scope('fwd_layers'):
            lax.fori_loop(0, SEG // GROUP, fwd_group, k)

        @pl.when(row < n_rows - 1)
        def _():
            rcopy(acts.at[SEG, k], acts.at[0, k], fwd_send, fwd_recv.at[k], me + SEG).start()
        for layer in range(SEG):
            act_ship(layer, k).start()

        @pl.when(row == n_rows - 1)
        def _():
            top_grad(k)
        return carry

    lax.fori_loop(0, jnp.where(row == n_rows - 1, 1, N_CHUNKS), fwd_chunk, 0)

    def bwd_layer(step, k, joined):
        layer = SEG - 1 - step
        grad_out = grads[layer + 1, k]
        x_float = acts[layer, k].astype(F32)
        inv_rms = inv_rms_of(x_float)
        x_hat = x_float * inv_rms
        gain = gains[layer, 0:1, :]
        grad_normed = 0.0
        pieces = []
        for part in range(0, d_ff, BWD_COLS):
            cols = slice(part, part + BWD_COLS)
            hidden = hiddens[layer, k, :, cols]
            slope = gelu_slope(hidden, *gelu_gate(hidden))
            grad_gelu = dot_nt(grad_out, wd[layer, cols, :]).astype(BF16).astype(F32)
            pieces.append((grad_gelu * slope).astype(BF16))
            if not joined:
                grad_normed += dot_nt(pieces[-1], wu[layer, :, cols])
        if joined:
            grad_normed = dot_nt(jnp.concatenate(pieces, axis=1), wu[layer])
        grad_normed = grad_normed.astype(BF16).astype(F32)
        dg_part[layer] += fold_rows(grad_normed * x_hat)
        grad_hat = grad_normed * gain
        mean_dot = jnp.mean(grad_hat * x_hat, axis=-1, keepdims=True)
        grad_x = inv_rms * (grad_hat - x_hat * mean_dot)
        grads[layer, k] = (grad_out.astype(F32) + grad_x).astype(BF16)

    def bwd_group(group, k):
        for step in range(GROUP):
            bwd_layer(group * GROUP + step, k, joined=True)

        @pl.when((row > 0) & (group == SEG // GROUP - 1))
        def _():
            rcopy(grads.at[0, k], grads.at[SEG, k], bwd_send, bwd_recv.at[k], me - SEG).start()
        for step in range(GROUP):
            grad_ship(SEG - 1 - group * GROUP - step, k).start()
        return k

    def both_group(group, k):
        for step in range(GROUP):
            bwd_layer(group * GROUP + step, k - 1, joined=False)
            fwd_layer(group * GROUP + step, k, joined=False)

        @pl.when((row > 0) & (group == SEG // GROUP - 1))
        def _():
            rcopy(grads.at[0, k - 1], grads.at[SEG, k - 1], bwd_send, bwd_recv.at[k - 1], me - SEG).start()
        for step in range(GROUP):
            grad_ship(SEG - 1 - group * GROUP - step, k - 1).start()
        return k

    def both_chunks(k, carry):
        fwd_input_wait(k)
        with jax.named_scope('both_layers'):
            lax.fori_loop(0, SEG // GROUP, both_group, k)
        top_grad(k)
        for layer in range(SEG):
            act_ship(layer, k).start()
        return carry

    @pl.when(row == n_rows - 1)
    def _():
        lax.fori_loop(1, N_CHUNKS, both_chunks, 0)
        loss_stash[r] = loss_part[...]
        for step in range(1, SEG):
            rcopy(loss_stash.at[r], loss_stash.at[r], lrow_send, lrow_recv, row_base + lax.rem(r + step, SEG)).start()

    rest = act_stash.at[0, pl.ds(0, SEG)]
    all_rest = acts.at[pl.ds(0, SEG)]

    def owner_block(index):
        return lax.div(index, 2), pl.ds(lax.rem(index, 2) * HALF, HALF)

    def value_block(index, carry):
        k, srcs = owner_block(index)

        @pl.when(lax.rem(index, 2) == 0)
        def _():
            with jax.named_scope('as_wait'):
                rcopy(rest, rest, as_send, as_recv.at[k], me).wait_recv()
            act_stash[k, r] = acts[r, k]
        x_float = act_stash[k, srcs].reshape(HALF * chunk, d_model).astype(F32)
        normed = (x_float * inv_rms_of(x_float) * gains[r, 0:1, :]).astype(BF16)
        act_stash[k, srcs] = normed.reshape(HALF, chunk, d_model)
        for part in range(0, d_ff, COLS):
            cols = slice(part, part + COLS)
            hidden = dot_nn(normed, wu[r, :, cols])
            gate, sq = gelu_gate(hidden)
            value_stash[k, srcs, :, cols] = (hidden * gate).astype(BF16).reshape(HALF, chunk, COLS)
            slope_stash[k, srcs, :, cols] = gelu_slope(hidden, gate, sq).reshape(HALF, chunk, COLS)
        return carry

    def sent_own(piece):
        rcopy(u_part(r, 0), u_part(r, 0), agu_send, gain_recv, me).wait_send()
        rcopy(d_part(r, 0), d_part(r, 0), agd_send, gain_recv, me).wait_send()

    def sent_help(piece):
        rcopy(help_u.at[0, 0], help_u.at[0, 0], hu_send, gain_recv, me).wait_send()
        rcopy(help_d.at[0, 0], help_d.at[0, 0], hd_send, gain_recv, me).wait_send()

    def value_phase():
        dwu[...] = jnp.zeros_like(dwu)
        dwd_t[...] = jnp.zeros_like(dwd_t)
        with jax.named_scope('value_blocks'):
            lax.fori_loop(0, 2 * N_CHUNKS, value_block, 0)
        each_piece(0, jnp.where(helped, 3 * n_direct + n_help + 4 * PIECES, 7 * PIECES), sent_own)
        each_piece(0, jnp.where(helped, 0, 6 * n_help), sent_help)
        rest_gain = gains.at[pl.ds(0, SEG - 1)]
        rcopy(rest_gain, rest_gain, gain_send, gain_recv, me).wait_send()
        rcopy(all_rest, all_rest, as_send, dg_recv, me).wait_send()

        @pl.when(row < n_rows - 1)
        def _():
            rcopy(acts.at[0], acts.at[0], fwd_send, dg_recv, me).wait_send()

    @pl.when(row < n_rows - LATE_ROWS)
    def _():
        value_phase()

    def weight_block(k, carry):
        rows = SEG * chunk
        with jax.named_scope('gs_wait'):
            rcopy(rest, rest, gs_send, gs_recv.at[k], me).wait_recv()
        grad_stash[k, r] = grads[r + 1, k]
        normed = act_stash[k, pl.ds(0, SEG)].reshape(rows, d_model)
        grad_out = grad_stash[k, pl.ds(0, SEG)].reshape(rows, d_model)
        for part in range(0, d_ff, WEIGHT_COLS):
            cols = slice(part, part + WEIGHT_COLS)
            dwd_t[:, cols] += dot_tn(grad_out, value_stash[k, :, :, cols].reshape(rows, WEIGHT_COLS))
            grad_gelu = dot_nt(grad_out, wd[r, cols, :]).astype(BF16).astype(F32)
            grad_hidden = (grad_gelu * slope_stash[k, :, :, cols].reshape(rows, WEIGHT_COLS)).astype(BF16)
            dwu[:, cols] += dot_tn(normed, grad_hidden)
        return carry

    def bwd_chunk(k, carry):
        @pl.when(row < n_rows - 1)
        def _():
            with jax.named_scope('bwd_wait'):
                rcopy(grads.at[SEG, k], grads.at[SEG, k], bwd_send, bwd_recv.at[k], me).wait_recv()

        with jax.named_scope('bwd_layers'):
            lax.fori_loop(0, SEG // GROUP, bwd_group, k)
        return carry

    lax.fori_loop(jnp.where(row == n_rows - 1, N_CHUNKS - 1, 0), N_CHUNKS, bwd_chunk, 0)

    def dg_ship(layer):
        return rcopy(dg_part.at[layer], dg_stash.at[r], dg_send, dg_recv, row_base + layer)

    for step in range(1, SEG):
        dg_ship(lax.rem(r + step, SEG)).start()
    dg_stash[r] = dg_part[r]

    @pl.when(row >= n_rows - LATE_ROWS)
    def _():
        value_phase()

    with jax.named_scope('weight_blocks'):
        lax.fori_loop(0, N_CHUNKS, weight_block, 0)
    @pl.when(row == n_rows - 1)
    def _():
        rest_row = loss_stash.at[pl.ds(0, SEG - 1)]
        rcopy(rest_row, rest_row, lrow_send, lrow_recv, me).wait_recv()
        loss_total[...] = jnp.sum(loss_stash[...], axis=0)
        for step in range(1, n_rows):
            rcopy(loss_total, loss_total, lcol_send, lcol_recv, me - step * SEG).start()

    with jax.named_scope('turn'):
        up_out = pltpu.make_async_copy(dwu, dwu_hbm.at[0], out_sem.at[0])
        up_out.start()
        dwd[...] = dwd_t[...].T
        down_out = pltpu.make_async_copy(dwd, dwd_hbm.at[0], out_sem.at[1])
        down_out.start()

    rest_dg = dg_stash.at[pl.ds(0, SEG - 1)]
    with jax.named_scope('dg_wait'):
        rcopy(rest_dg, rest_dg, dg_send, dg_recv, me).wait_recv()
    sums[0:8] = jnp.sum(dg_stash[...], axis=0)

    @pl.when(row < n_rows - 1)
    def _():
        rcopy(loss_total, loss_total, lcol_send, lcol_recv, me).wait_recv()
    sums[8:16] = loss_total[...]
    sums_out = pltpu.make_async_copy(sums, sums_hbm, out_sem.at[2])
    sums_out.start()

    rcopy(all_rest, all_rest, gs_send, dg_recv, me).wait_send()
    rcopy(rest_dg, rest_dg, dg_send, dg_recv, me).wait_send()

    @pl.when(row > 0)
    def _():
        rcopy(grads.at[0], grads.at[0], bwd_send, dg_recv, me).wait_send()

    @pl.when(row == n_rows - 1)
    def _():
        rest_row = loss_stash.at[pl.ds(0, SEG - 1)]
        rcopy(rest_row, rest_row, lrow_send, lrow_recv, me).wait_send()
        for step in range(1, n_rows):
            rcopy(loss_total, loss_total, lcol_send, lcol_recv, me).wait_send()
    up_out.wait()
    down_out.wait()
    sums_out.wait()


def write_kernel(n_parts, loss_scale, up_hbm, down_hbm, sums_hbm, up_out, down_out, gain_out, loss_out,
                 up_buf, down_buf, sums_buf, gain_buf, loss_buf, in_sem, out_sem, small_sem):
    pairs = ((up_hbm, up_buf, up_out), (down_hbm, down_buf, down_out))

    def part(ref, index):
        rows = ref.shape[0] // n_parts
        return ref.at[pl.ds(index * rows, rows)]

    sums_read = pltpu.make_async_copy(sums_hbm, sums_buf, small_sem.at[0])
    gain_write = pltpu.make_async_copy(gain_buf, gain_out, small_sem.at[1])
    loss_write = pltpu.make_async_copy(loss_buf, loss_out, small_sem.at[2])
    sums_read.start()
    reads, writes = [], []
    for side, (src, buf, dst) in enumerate(pairs):
        for index in range(n_parts):
            reads.append(pltpu.make_async_copy(part(src.at[0], index), part(buf, index), in_sem.at[side, index]))
            writes.append(pltpu.make_async_copy(part(buf, index), part(dst.at[0], index), out_sem.at[side, index]))
    for read in reads:
        read.start()
    sums_read.wait()
    gain_buf[...] = jnp.sum(sums_buf[0:8], axis=0, keepdims=True)
    loss_buf[0] = jnp.sum(sums_buf[8:16]) * loss_scale
    for read, write in zip(reads, writes):
        read.wait()
        write.start()
    gain_write.start()
    loss_write.start()
    for write in writes:
        write.wait()
    gain_write.wait()
    loss_write.wait()


def solution(mesh):
    n_stages = mesh.shape['stage']

    def stage_body(x_in, y_target, w_up, w_down, norm_gain):
        n_micro, n_tok, d_model = x_in.shape
        d_ff = w_up.shape[2]
        n_rows = n_micro * n_tok
        chunk = n_rows // SEG // N_CHUNKS
        loss_scale = 1.0 / (n_rows * d_model)
        sem = pltpu.SemaphoreType.DMA
        act_shape = (N_CHUNKS, chunk, d_model)
        scratch = [
            pltpu.VMEM((SEG, d_model, d_ff), BF16),
            pltpu.VMEM((SEG, d_ff, d_model), BF16),
            pltpu.VMEM((SEG // 2, HELP, d_model // PIECES, d_ff), BF16),
            pltpu.VMEM((SEG // 2, HELP, d_ff // PIECES, d_model), BF16),
            pltpu.VMEM((SEG, 8, d_model), F32),
            pltpu.VMEM((SEG + 1,) + act_shape, BF16),
            pltpu.VMEM((SEG + 1,) + act_shape, BF16),
            pltpu.VMEM((SEG, N_CHUNKS, chunk, d_ff), F32),
            pltpu.VMEM((N_CHUNKS, SEG + 1, chunk, d_model), BF16),
            pltpu.VMEM((N_CHUNKS, SEG + 1, chunk, d_model), BF16),
            pltpu.VMEM((N_CHUNKS, SEG, chunk, d_ff), BF16),
            pltpu.VMEM((N_CHUNKS, SEG, chunk, d_ff), F32),
            pltpu.VMEM(act_shape, BF16),
            pltpu.VMEM((d_model, d_ff), F32),
            pltpu.VMEM((d_model, d_ff), F32),
            pltpu.VMEM((d_ff, d_model), F32),
            pltpu.VMEM((16, d_model), F32),
            pltpu.VMEM((SEG, 8, d_model), F32),
            pltpu.VMEM((SEG, 8, d_model), F32),
            pltpu.VMEM((8, d_model), F32),
            pltpu.VMEM((SEG, 8, d_model), F32),
            pltpu.VMEM((8, d_model), F32),
            sem((2,)), sem((3,)), sem((N_CHUNKS,)), sem((N_CHUNKS,)),
            sem, sem((SEG, PIECES)), sem, sem((SEG, PIECES)), sem, sem((SEG // 2, HELP)), sem, sem((SEG // 2, HELP)), sem, sem,
            sem, sem((N_CHUNKS,)), sem, sem((N_CHUNKS,)), sem, sem((N_CHUNKS,)), sem, sem((N_CHUNKS,)),
            sem, sem, sem, sem, sem, sem,
        ]
        any_spec = pl.BlockSpec(memory_space=pl.ANY)
        vmem_spec = pl.BlockSpec(memory_space=pltpu.VMEM)
        dw_up, dw_down, sums = pl.pallas_call(
            functools.partial(step_kernel, n_stages, loss_scale),
            out_shape=(jax.ShapeDtypeStruct(w_up.shape, F32), jax.ShapeDtypeStruct(w_down.shape, F32),
                       jax.ShapeDtypeStruct((16, d_model), F32)),
            in_specs=[any_spec, any_spec, any_spec, any_spec, vmem_spec],
            out_specs=(any_spec, any_spec, any_spec),
            scratch_shapes=scratch,
            compiler_params=pltpu.CompilerParams(collective_id=0, has_side_effects=True,
                                                 vmem_limit_bytes=67043328),
        )(x_in.reshape(n_rows, d_model), y_target.reshape(n_rows, d_model), w_up, w_down, norm_gain)
        return pl.pallas_call(
            functools.partial(write_kernel, WRITE_PARTS, loss_scale),
            out_shape=(jax.ShapeDtypeStruct(w_up.shape, F32), jax.ShapeDtypeStruct(w_down.shape, F32),
                       jax.ShapeDtypeStruct(norm_gain.shape, F32), jax.ShapeDtypeStruct((1,), F32)),
            in_specs=[any_spec, any_spec, any_spec],
            out_specs=(any_spec, any_spec, any_spec, any_spec),
            scratch_shapes=[pltpu.VMEM(w_up.shape[1:], F32), pltpu.VMEM(w_down.shape[1:], F32),
                            pltpu.VMEM((16, d_model), F32), pltpu.VMEM((1, d_model), F32), pltpu.SMEM((1,), F32),
                            sem((2, WRITE_PARTS)), sem((2, WRITE_PARTS)), sem((3,))],
        )(dw_up, dw_down, sums)

    return jax.shard_map(stage_body, mesh=mesh,
                         in_specs=(P('dp'), P('dp'), P('stage'), P('stage'), P('stage')),
                         out_specs=(P(('dp', 'stage')), P(('dp', 'stage')), P(('dp', 'stage')), P('dp')),
                         check_vma=False)
```
